32 devices in a mesh: ga: 8 (over y, x, core), band: 4 (over z).
Axes of the slice: x: 2, y: 2, z: 4, core: 2. Of those that a mesh axis runs over, the one named last changes fastest.
Arguments:
- psi: bfloat16 [2, 8, 96, 2048], P(None, 'band', None, 'ga'), may hold values from -6 to 6
- vloc: float32 [96, 9216], P('ga'), may hold values from 0.5 to 1.5
- dv: float32 [96, 9216], P('ga'), may hold values from -6 to 6
- beta: float32 [2, 128, 96, 2048], P(None, None, None, 'ga'), may hold values from -0.02734375 to 0.02734375
- dij: float32 [2, 4, 4], replicated, may hold values from -1 to 1.5, as said below
- atom_type: int32 [32], replicated, may hold values from 0 to 1
- stick_xy: int32 [2048], replicated, may hold values from 0 to 9215, as said below
- band_shift: float32 [8], P('band'), may hold values from 0.3 to 3
Outputs:
- response: float32 [2, 8, 96, 2048], P(None, 'band', None, 'ga')
- density: float32 [96, 9216], P('ga', 'band')
The draws below stay inside these ranges and needn't reach their ends.
Inputs may be any that keep to these rules, and one draw needn't show every extreme that they name: `stick_xy`: 2048 distinct columns, each with both frequencies f(y) and f(x) in -(32) to 31. `dij`: each of the 2 matrices is symmetric positive definite with diagonal at least 0.5.
All inputs are finite; a program needn't handle non-finite values.
Results may differ from the reference program's by a relative error of at most 0.0003.
Values may be sent and summed in bfloat16 or wider, within the bound.
A program may use at most 128 MiB of HBM per device.

```python
import math
import jax
import jax.numpy as jnp
from jax import lax

GRID = 96
STICKS = 2048
NATOM = 32
NBETA = 4
NTYPE = 2
ITERS = 2
NPROJ = 128
BANDS = 8


def draw_stick_xy(key, part):
    radius_cells = GRID // 3
    square_side = 2 * radius_cells
    chosen = jax.random.permutation(key, square_side * square_side)[:STICKS]
    freq_y = chosen // square_side - radius_cells
    freq_x = chosen % square_side - radius_cells
    return (freq_y % GRID * GRID + freq_x % GRID).astype(jnp.int32)


def draw_dij(key, part):
    factor = jax.random.uniform(key, (NTYPE, NBETA, NBETA), jnp.float32, -1.0, 1.0)
    product = jnp.einsum('tij,tkj->tik', factor, factor) / NBETA
    return product + 0.5 * jnp.eye(NBETA, dtype=jnp.float32)[None]


def with_ends(values, key, least, largest):
    dims = values.shape
    spot = [jax.random.randint(jax.random.fold_in(key, axis), (), 0, dims[axis]) for axis in range(len(dims))]
    values = values.at[tuple(spot)].set(least)
    longest = dims.index(max(dims))
    spot[longest] = (spot[longest] + 1) % dims[longest]
    return values.at[tuple(spot)].set(largest)


def level_of(key, dims, cuts, low, high):
    gain = 1.0
    for dim, parts in cuts:
        draws = jax.random.uniform(jax.random.fold_in(jax.random.fold_in(key, 6), dim), (parts,), jnp.float32, low / len(cuts), high / len(cuts))
        gain = gain * jnp.repeat(jnp.exp(draws), dims[dim] // parts).reshape((-1,) + (1,) * (len(dims) - 1 - dim))
    return gain


def noise(rng, dims, width, reach, shards=(), kind=jnp.bfloat16):
    entries = jax.random.normal(rng, dims, jnp.float32) * width
    if len(shards) > 0:
        entries = level_of(rng, dims, shards, -0.22, 0.18) * entries
    return jnp.clip(entries, min=-reach, max=reach).astype(kind)


def setup_inputs(seed: int = 0) -> dict:
    streams_of = jax.random.split(jax.random.key(seed), 9)
    return {
        "psi": noise(streams_of[0], (2, BANDS, GRID, STICKS), 1.0, 6.0, ((1, 4), (3, 8))),
        "vloc": jnp.clip(0.5 + 1.0 * jax.random.uniform(streams_of[1], (GRID, GRID * GRID), jnp.float32) ** level_of(streams_of[1], (GRID, GRID * GRID), ((0, 8),), -0.2, 0.2), 0.5, 1.5),
        "dv": noise(streams_of[2], (GRID, GRID * GRID), 1.0, 6.0, ((0, 8),), jnp.float32),
        "beta": noise(streams_of[3], (2, NPROJ, GRID, STICKS), (GRID * STICKS // 4) ** -0.5, 0.02734375, ((3, 8),), jnp.float32),
        "dij": draw_dij(jax.random.fold_in(streams_of[8], 71), 0),
        "atom_type": with_ends(jax.random.randint(streams_of[5], (NATOM,), 0, NTYPE), jax.random.fold_in(streams_of[5], 1), 0, NTYPE - 1).astype(jnp.int32),
        "stick_xy": draw_stick_xy(jax.random.fold_in(streams_of[8], 71), 0),
        "band_shift": jnp.clip(jnp.exp(math.log(3.0) - 2.3025851 * jax.random.uniform(streams_of[7], (BANDS,), jnp.float32) ** level_of(streams_of[7], (BANDS,), ((0, 4),), -0.2, 0.2)), 0.3, 3.0),
    }


highest = lax.Precision.HIGHEST


def frequency(index):
    return (index + GRID // 2) % GRID - GRID // 2


def kinetic_table(stick_xy):
    freq_z = frequency(jnp.arange(GRID, dtype=jnp.int32))
    freq_y = frequency(stick_xy // GRID)
    freq_x = frequency(stick_xy % GRID)
    summed = freq_z[:, None] ** 2 + (freq_y ** 2 + freq_x ** 2)[None, :]
    return summed.astype(jnp.float32) * (4.0 / (GRID * GRID))


def to_real(coef, stick_xy):
    values = coef[0] + 1j * coef[1]
    grid = jnp.zeros((GRID, GRID * GRID), values.dtype).at[:, stick_xy].set(values)
    field = jnp.fft.ifftn(grid.reshape(GRID, GRID, GRID)) * (GRID ** 1.5)
    field = field.reshape(GRID, GRID * GRID)
    return jnp.stack([jnp.real(field), jnp.imag(field)])


def to_recip(field, stick_xy):
    values = (field[0] + 1j * field[1]).reshape(GRID, GRID, GRID)
    spectrum = jnp.fft.fftn(values).reshape(GRID, GRID * GRID) / (GRID ** 1.5)
    picked = spectrum[:, stick_xy]
    return jnp.stack([jnp.real(picked), jnp.imag(picked)])


def reference(psi, vloc, dv, beta, dij, atom_type, stick_xy, band_shift):
    occupied = jnp.moveaxis(psi.astype(jnp.float32), 1, 0)
    kinetic = kinetic_table(stick_xy)
    inv_norm = 1.0 / (2.0 * GRID * STICKS)

    def dv_image(coef):
        return to_recip(dv[None] * to_real(coef, stick_xy), stick_xy)

    image = lax.map(dv_image, occupied)
    intersect_re = jnp.einsum('mczs,nczs->mn', occupied, image, precision=highest) * inv_norm
    intersect_im = (jnp.einsum('mzs,nzs->mn', occupied[:, 0], image[:, 1], precision=highest) - jnp.einsum('mzs,nzs->mn', occupied[:, 1], image[:, 0], precision=highest)) * inv_norm
    corr_re = jnp.einsum('mn,mzs->nzs', intersect_re, occupied[:, 0], precision=highest) - jnp.einsum('mn,mzs->nzs', intersect_im, occupied[:, 1], precision=highest)
    corr_im = jnp.einsum('mn,mzs->nzs', intersect_im, occupied[:, 0], precision=highest) + jnp.einsum('mn,mzs->nzs', intersect_re, occupied[:, 1], precision=highest)
    rhs = jnp.stack([corr_re, corr_im], axis=1) - image
    selected = dij[atom_type]
    diagonal = kinetic[None] + band_shift[:, None, None]

    def local_image(coef):
        return to_recip(vloc[None] * to_real(coef, stick_xy), stick_xy)

    def apply_operator(vector):
        local = lax.map(local_image, vector)
        proj_re = jnp.einsum('jzs,bzs->bj', beta[0], vector[:, 0], precision=highest) + jnp.einsum('jzs,bzs->bj', beta[1], vector[:, 1], precision=highest)
        proj_im = jnp.einsum('jzs,bzs->bj', beta[0], vector[:, 1], precision=highest) - jnp.einsum('jzs,bzs->bj', beta[1], vector[:, 0], precision=highest)
        shaped_re = proj_re.reshape(BANDS, NATOM, NBETA)
        shaped_im = proj_im.reshape(BANDS, NATOM, NBETA)
        coup_re = jnp.einsum('aij,baj->bai', selected, shaped_re, precision=highest).reshape(BANDS, NPROJ)
        coup_im = jnp.einsum('aij,baj->bai', selected, shaped_im, precision=highest).reshape(BANDS, NPROJ)
        back_re = jnp.einsum('jzs,bj->bzs', beta[0], coup_re, precision=highest) - jnp.einsum('jzs,bj->bzs', beta[1], coup_im, precision=highest)
        back_im = jnp.einsum('jzs,bj->bzs', beta[0], coup_im, precision=highest) + jnp.einsum('jzs,bj->bzs', beta[1], coup_re, precision=highest)
        return diagonal[:, None] * vector + local + jnp.stack([back_re, back_im], axis=1)

    def band_sum(first, second):
        return jnp.sum(first * second, axis=(1, 2, 3))

    solution = jnp.zeros_like(rhs)
    residual = rhs
    direction = rhs
    norm_now = band_sum(rhs, rhs)
    for iteration in range(ITERS):
        image_now = apply_operator(direction)
        alpha = (norm_now / band_sum(direction, image_now))[:, None, None, None]
        solution = solution + alpha * direction
        residual = residual - alpha * image_now
        if iteration + 1 < ITERS:
            norm_next = band_sum(residual, residual)
            direction = residual + (norm_next / norm_now)[:, None, None, None] * direction
            norm_now = norm_next

    def accumulate(carry, pair):
        psi_field = to_real(pair[0], stick_xy)
        resp_field = to_real(pair[1], stick_xy)
        return carry + 4.0 * jnp.sum(psi_field * resp_field, axis=0), None

    density, unused = lax.scan(accumulate, jnp.zeros((GRID, GRID * GRID), jnp.float32), (occupied, solution))
    return jnp.moveaxis(solution, 0, 1), density
```

```python
import math

import jax
import jax.numpy as jnp
import ml_dtypes
import numpy as np
from jax import lax
from jax.experimental import pallas as pl
from jax.experimental.pallas import tpu as pltpu
from jax.sharding import PartitionSpec as P

LANES = 128
PER = 4
f32, bf16 = jnp.float32, jnp.bfloat16
VMEM = pl.BlockSpec(memory_space=pltpu.VMEM)


def frequency(index, grid):
    return (index + grid // 2) % grid - grid // 2


def phase(rows, cols, grid, sign):
    angle = 2.0 * math.pi * ((rows[:, None] * cols[None, :]) % grid) / grid
    return np.exp(1j * sign * angle) / math.sqrt(grid)


def parts_of(table):
    return np.stack(
        [np.stack([table.real, -table.imag], 1), np.stack([table.imag, table.real], 1)]
    )


def halves_of(table):
    table = table.astype(np.float32)
    hi = table.astype(ml_dtypes.bfloat16)
    lo = (table - hi.astype(np.float32)).astype(ml_dtypes.bfloat16)
    return hi, lo


class Plan:
    def __init__(self, bands, grid, own, planes, shards, sticks):
        self.bands, self.grid, self.own, self.planes = bands, grid, own, planes
        self.shards, self.sticks = shards, sticks
        self.side = 2 * (grid // 3)
        self.q = 2 * planes
        self.rows = -(-bands * self.q // 16) * 16
        self.images = bands * planes
        self.groups = self.side // PER
        self.fold = LANES // self.side
        self.tiles = PER // self.fold
        self.wide = PER * self.side
        side, fold, tiles, groups = self.side, self.fold, self.tiles, self.groups
        cells = np.arange(grid)
        freqs = np.arange(side) - grid // 3
        z = parts_of(phase(cells, cells, grid, 1.0))
        z = z.reshape(2, shards, planes, 2 * grid).transpose(1, 0, 2, 3)
        self.z_inv = np.stack(halves_of(z.reshape(shards * self.q, 2 * grid)))
        z = parts_of(phase(cells, cells, grid, -1.0))
        z = z.reshape(2, grid, 2, shards, planes).transpose(0, 1, 3, 2, 4)
        self.z_fwd = np.stack(halves_of(z.reshape(2 * grid, shards * self.q)))
        y = parts_of(phase(cells, freqs, grid, 1.0))
        y = y.reshape(2, grid, 2, groups, tiles, fold).transpose(0, 5, 1, 2, 4, 3)
        hi, lo = halves_of(y.reshape(2 * fold * grid, 2 * tiles * groups))
        self.y_inv = np.concatenate([hi, hi, lo], axis=1)
        x = parts_of(phase(freqs, cells, grid, 1.0).T).transpose(2, 3, 0, 1)
        x = np.repeat(x[:, None], fold, axis=1)
        x = np.pad(x, ((0, 0),) * 4 + ((0, LANES - grid),))
        self.x_inv = np.stack(halves_of(x.reshape(2 * LANES, 2 * LANES)))
        x = parts_of(phase(cells, freqs, grid, -1.0).T).transpose(2, 3, 0, 1)
        x = np.repeat(x[:, :, :, None], fold, axis=3)
        x = np.pad(x, ((0, 0), (0, LANES - grid)) + ((0, 0),) * 3)
        self.x_fwd = np.stack(halves_of(x.reshape(2 * LANES, 2 * LANES)))
        y = parts_of(phase(freqs, cells, grid, -1.0))
        y = y.reshape(2, groups, tiles, fold, 2 * grid).transpose(0, 3, 2, 1, 4)
        self.y_fwd = np.stack(halves_of(y.reshape(2 * side, 2 * grid)))


def dot(a, b):
    return jnp.dot(a, b, preferred_element_type=f32)


def dot_t(a, b):
    return lax.dot_general(a, b, (((1,), (1,)), ((), ())), preferred_element_type=f32)


def split(x):
    hi = x.astype(bf16)
    return hi, (x - hi.astype(f32)).astype(bf16)


def split3(x):
    hi = x.astype(bf16)
    rest = x - hi.astype(f32)
    mid = rest.astype(bf16)
    return hi, mid, (rest - mid.astype(f32)).astype(bf16)


def aligned(at, size):
    return pl.ds(pl.multiple_of(at * size, math.gcd(size, LANES)), size)


def spec_of(shape, dtype=f32):
    return jax.ShapeDtypeStruct(shape, dtype)


def lines_to_rows(p, held, oh, mask, left, sq):
    def spread(src, carry):
        at = aligned(src, p.own)
        hi, lo = split(held[src])
        for g in range(p.groups):
            keep = mask[g, :, at]
            for r in range(0, p.rows, 16):
                to = pl.ds(g * p.rows + r, 16)
                left[0, to, at] = hi[r : r + 16] * keep
                left[1, to, at] = lo[r : r + 16] * keep
        return carry

    lax.fori_loop(0, p.shards, spread, 0)
    made = dot(left[0], oh[...]) + dot(left[1], oh[...])
    for t in range(p.tiles):
        sq[t] = made[:, t * LANES : (t + 1) * LANES]


def rows_to_mixed(p, sq, y_inv, mixed):
    low = lax.broadcasted_iota(jnp.int32, (1, 2 * LANES), 1) % LANES < p.side

    def pair(at, carry):
        for b in range(p.bands):
            tiles = []
            for k in range(2):
                pieces = []
                for c in range(2):
                    n = b * p.q + c * p.planes + 2 * at + k
                    for t in range(p.tiles):
                        pieces.append(sq[t, pl.ds(n, p.groups, stride=p.rows), :])
                tiles.append(jnp.concatenate(pieces, axis=0))
            hi, lo = split(jnp.concatenate(tiles, axis=1))
            out = dot(y_inv[...], jnp.concatenate([hi, lo, hi], axis=0))
            both = [
                jnp.where(
                    low,
                    out[2 * c * p.grid : (2 * c + 1) * p.grid],
                    out[(2 * c + 1) * p.grid : (2 * c + 2) * p.grid],
                )
                for c in range(2)
            ]
            for k in range(2):
                lane = slice(k * LANES, (k + 1) * LANES)
                hi, lo = split(jnp.concatenate([both[0][:, lane], both[1][:, lane]], axis=1))
                to = aligned(b * p.planes + 2 * at + k, p.grid)
                mixed[0, to, :] = hi
                mixed[1, to, :] = lo
        return carry

    lax.fori_loop(0, p.planes // 2, pair, 0)


def mixed_to_field(p, mixed, x_inv, x_fwd, pot, field, spectrum, stat):
    some = math.gcd(p.planes, 4)
    size = some * p.grid

    for b in range(p.bands):

        def block(at, total, b=b):
            to = aligned(b * (p.planes // some) + at, size)
            hi, lo = mixed[0, to, :], mixed[1, to, :]
            one = dot(hi, x_inv[0]) + dot(lo, x_inv[0]) + dot(hi, x_inv[1])
            field[to, :] = one
            wide = pot[aligned(at, size), :]
            used = one * jnp.concatenate([wide, wide], axis=1)
            if spectrum is not None:
                hi, lo = split(used)
                spectrum[to, :] = dot(hi, x_fwd[0]) + dot(lo, x_fwd[0]) + dot(hi, x_fwd[1])
            if stat is not None:
                made = jnp.sum((used * one).reshape(size // 8, 8, 2 * LANES), axis=0)
                total = total + made[:, :LANES] + made[:, LANES:]
            return total

        total = lax.fori_loop(0, p.planes // some, block, jnp.zeros((8, LANES), f32))
        if stat is not None:
            stat[b] = total


def spectrum_to_lines(p, spectrum, y_fwd, oh_t, group_of, sq, left, lines):
    low = lax.broadcasted_iota(jnp.int32, (1, 2 * LANES), 1) % LANES < p.side
    half = p.side // p.fold

    def pair(at, carry):
        for b in range(p.bands):
            tiles = []
            for k in range(2):
                one = spectrum[aligned(b * p.planes + 2 * at + k, p.grid), :]
                tiles.append(jnp.concatenate([one[:, :LANES], one[:, LANES:]], axis=0))
            hi, lo = split(jnp.concatenate(tiles, axis=1))
            out = dot(y_fwd[0], hi) + dot(y_fwd[0], lo) + dot(y_fwd[1], hi)
            for c in range(2):
                from_ = c * p.side
                both = jnp.where(
                    low, out[from_ : from_ + half], out[from_ + half : from_ + 2 * half]
                )
                for k in range(2):
                    to = aligned(b * p.q + c * p.planes + 2 * at + k, p.groups)
                    for t in range(p.tiles):
                        sq[t, to, :] = both[
                            t * p.groups : (t + 1) * p.groups, k * LANES : (k + 1) * LANES
                        ]
        return carry

    lax.fori_loop(0, p.planes // 2, pair, 0)
    for g in range(p.groups):
        to = pl.ds(g * p.rows, p.rows)
        for t in range(p.tiles):
            hi, lo = split(sq[t, pl.ds(g, p.rows, stride=p.groups), :])
            left[0, to, t * LANES : (t + 1) * LANES] = hi
            left[1, to, t * LANES : (t + 1) * LANES] = lo

    def gather(dest, carry):
        at = aligned(dest, p.own)
        weights = oh_t[:, at]
        got = dot(left[0, :, : p.wide], weights) + dot(left[1, :, : p.wide], weights)
        kind = group_of[0:1, at]
        kept = got[: p.rows]
        for g in range(1, p.groups):
            kept = jnp.where(kind == g, got[g * p.rows : (g + 1) * p.rows], kept)
        lines[dest] = kept
        return carry

    lax.fori_loop(0, p.shards, gather, 0)


def planes_call(p, held, tables, pot, back, want_stat, name):
    oh, oh_t, mask, group_of = tables
    outs = [spec_of((p.images * p.grid, 2 * LANES))]
    if back:
        outs.append(spec_of((p.shards, p.rows, p.own)))
    if want_stat:
        outs.append(spec_of((p.bands, 8, LANES)))
    ins = [held, oh, mask, p.y_inv, p.x_inv, pot]
    if back:
        ins += [oh_t, group_of, p.x_fwd, p.y_fwd]
    many = p.groups * p.rows
    scratch = [
        pltpu.VMEM((2, many, p.sticks), bf16),
        pltpu.VMEM((p.tiles, many, LANES), f32),
        pltpu.VMEM((2, p.images * p.grid, 2 * LANES), bf16),
    ]
    if back:
        scratch.append(pltpu.VMEM((p.images * p.grid, 2 * LANES), f32))

    def kernel(*refs):
        refs = list(refs)
        held_r, oh_r, mask_r, y_inv_r, x_inv_r, pot_r = refs[:6]
        refs = refs[6:]
        if back:
            oh_t_r, group_r, x_fwd_r, y_fwd_r = refs[:4]
            refs = refs[4:]
        field_r = refs.pop(0)
        lines_r = refs.pop(0) if back else None
        stat_r = refs.pop(0) if want_stat else None
        left, sq, mixed = refs[:3]
        spectrum = refs[3] if back else None
        lines_to_rows(p, held_r, oh_r, mask_r, left, sq)
        rows_to_mixed(p, sq, y_inv_r, mixed)
        mixed_to_field(
            p, mixed, x_inv_r, x_fwd_r if back else None, pot_r, field_r, spectrum, stat_r
        )
        if back:
            spectrum_to_lines(p, spectrum, y_fwd_r, oh_t_r, group_r, sq, left, lines_r)

    return pl.pallas_call(
        kernel,
        out_shape=outs,
        in_specs=[VMEM] * len(ins),
        out_specs=[VMEM] * len(outs),
        scratch_shapes=scratch,
        name=name,
    )(*ins)


def greet(axis, count):
    me = lax.axis_index(axis)
    barrier = pltpu.get_barrier_semaphore()
    for hop in range(1, count):
        peer = lax.rem(me + hop, count)
        pl.semaphore_signal(
            barrier, inc=1, device_id={axis: peer}, device_id_type=pl.DeviceIdType.MESH
        )


def met(count):
    pl.semaphore_wait(pltpu.get_barrier_semaphore(), count - 1)


def pushes(axis, count, source, held, send_sem, recv_sem, scatter):
    me = lax.axis_index(axis)
    copies = []
    for hop in range(1, count):
        peer = lax.rem(me + hop, count)
        copies.append(
            pltpu.make_async_remote_copy(
                src_ref=source.at[peer] if scatter else source,
                dst_ref=held.at[me],
                send_sem=send_sem.at[hop - 1],
                recv_sem=recv_sem.at[hop - 1],
                device_id={axis: peer},
                device_id_type=pl.DeviceIdType.MESH,
            )
        )
    return copies


def sems(count):
    return [pltpu.SemaphoreType.DMA((count - 1,)), pltpu.SemaphoreType.DMA((count - 1,))]


def collect(p, held, out_r):
    me = lax.axis_index("ga")
    for hop in range(1, p.shards):
        src = lax.rem(me + hop, p.shards)
        out_r[src] = held[src]


def to_lines(p, values, z_inv, chunks, exact):
    for b in range(p.bands):
        value = values(b)
        if exact:
            hi = value
            out = dot(z_inv[0], hi) + dot(z_inv[1], hi)
        else:
            hi, lo = split(value)
            out = dot(z_inv[0], hi) + dot(z_inv[0], lo) + dot(z_inv[1], hi)
        for d in range(p.shards):
            chunks[d, b * p.q : (b + 1) * p.q, :] = out[d * p.q : (d + 1) * p.q]


def from_lines(p, held, joined, z_fwd, result):
    for b in range(p.bands):
        for src in range(p.shards):
            joined[src * p.q : (src + 1) * p.q, :] = held[src, b * p.q : (b + 1) * p.q, :]
        hi, lo = split(joined[...])
        out = dot(z_fwd[0], hi) + dot(z_fwd[0], lo) + dot(z_fwd[1], hi)
        result[0, b] = out[: p.grid]
        result[1, b] = out[p.grid :]


def first_call(p, psi):
    def kernel(psi_r, z_inv_r, out_r, chunks, held, send, recv):
        greet("ga", p.shards)
        me = lax.axis_index("ga")
        to_lines(
            p, lambda b: jnp.concatenate([psi_r[0, b], psi_r[1, b]], axis=0), z_inv_r, chunks, True
        )
        met(p.shards)
        copies = pushes("ga", p.shards, chunks, held, send, recv, True)
        for copy in copies:
            copy.start()
        out_r[me] = chunks[me]
        for copy in copies:
            copy.wait()
        collect(p, held, out_r)

    shape = (p.shards, p.rows, p.own)
    return pl.pallas_call(
        kernel,
        out_shape=spec_of(shape),
        in_specs=[VMEM] * 2,
        out_specs=VMEM,
        scratch_shapes=[pltpu.VMEM(shape, f32), pltpu.VMEM(shape, f32)] + sems(p.shards),
        compiler_params=pltpu.CompilerParams(collective_id=0, has_side_effects=True),
        name="first_exchange",
    )(psi, p.z_inv)


def rhs_call(p, lines, gathered, diag):
    many = gathered.shape[1]
    count = p.bands * many * 2
    tall = 16
    inv_norm = 1.0 / (2.0 * p.grid * p.sticks)

    def kernel(
        lines_r, psi_r, diag_r, z_fwd_r, z_inv_r, rhs_r, chunks_r, stat_r,
        held, joined, image, part, sums, send0, recv0, send1, recv1,
    ):
        greet("ga", p.shards)
        me = lax.axis_index("ga")
        met(p.shards)
        copies = pushes("ga", p.shards, lines_r, held, send0, recv0, True)
        for copy in copies:
            copy.start()
        held[me] = lines_r[me]
        for copy in copies:
            copy.wait()
        from_lines(p, held, joined, z_fwd_r, image)

        for n in range(p.bands):

            def overlap(t, acc, n=n):
                z = aligned(t, tall)
                acc = list(acc)
                for lane in range(0, p.own, LANES):
                    cut = pl.ds(lane, LANES)
                    i_re, i_im = image[0, n, z, cut], image[1, n, z, cut]
                    for m in range(many):
                        p_re = psi_r[0, m, z, cut].astype(f32)
                        p_im = psi_r[1, m, z, cut].astype(f32)
                        acc[2 * m] = acc[2 * m] + (p_re * i_re + p_im * i_im)
                        acc[2 * m + 1] = acc[2 * m + 1] + (p_re * i_im - p_im * i_re)
                return tuple(acc)

            zero = jnp.zeros((tall, LANES), f32)
            acc = lax.fori_loop(0, p.grid // tall, overlap, (zero,) * (2 * many))
            for m in range(2 * many):
                part[pl.ds(n * 2 * many + m, 1), :] = jnp.sum(acc[m], axis=0, keepdims=True)
        part[...] = jnp.broadcast_to(
            jnp.sum(part[...], axis=1, keepdims=True) * inv_norm, part.shape
        )
        copies = pushes("ga", p.shards, part, sums, send1, recv1, False)
        for copy in copies:
            copy.start()
        sums[me] = part[...]
        for copy in copies:
            copy.wait()
        inter = sums[0]
        for at in range(1, p.shards):
            inter = inter + sums[at]
        sums[0] = inter

        for n in range(p.bands):

            def right(t, acc, n=n):
                z = aligned(t, tall)
                norm, curve = acc
                for lane in range(0, p.own, LANES):
                    cut = pl.ds(lane, LANES)
                    re, im = -image[0, n, z, cut], -image[1, n, z, cut]
                    for m in range(many):
                        p_re = psi_r[0, m, z, cut].astype(f32)
                        p_im = psi_r[1, m, z, cut].astype(f32)
                        row = n * 2 * many + 2 * m
                        c_re = sums[0, row : row + 1, :]
                        c_im = sums[0, row + 1 : row + 2, :]
                        re = re + (c_re * p_re - c_im * p_im)
                        im = im + (c_im * p_re + c_re * p_im)
                    rhs_r[0, n, z, cut] = re
                    rhs_r[1, n, z, cut] = im
                    square = re * re + im * im
                    norm = norm + square
                    curve = curve + square * diag_r[n, z, cut]
                return norm, curve

            zero = jnp.zeros((tall, LANES), f32)
            norm, curve = lax.fori_loop(0, p.grid // tall, right, (zero, zero))
            stat_r[0, n] = norm[:8] + norm[8:]
            stat_r[1, n] = curve[:8] + curve[8:]
        to_lines(
            p, lambda b: jnp.concatenate([rhs_r[0, b], rhs_r[1, b]], axis=0), z_inv_r, chunks_r, False
        )

    shape = (p.shards, p.rows, p.own)
    mine = (2, p.bands, p.grid, p.own)
    return pl.pallas_call(
        kernel,
        out_shape=[spec_of(mine), spec_of(shape), spec_of((2, p.bands, 8, LANES))],
        in_specs=[VMEM] * 5,
        out_specs=[VMEM] * 3,
        scratch_shapes=[
            pltpu.VMEM(shape, f32),
            pltpu.VMEM((p.shards * p.q, p.own), f32),
            pltpu.VMEM(mine, f32),
            pltpu.VMEM((count, LANES), f32),
            pltpu.VMEM((p.shards, count, LANES), f32),
        ]
        + sems(p.shards)
        + sems(p.shards),
        compiler_params=pltpu.CompilerParams(collective_id=1, has_side_effects=True),
        name="right_side",
    )(lines, gathered, diag, p.z_fwd, p.z_inv)


def project_block(p, beta_r, vec_r, sums_r, base, group, unroll):
    _, some, grid, lanes = beta_r.shape
    for first in range(0, some, group):

        def body(t, sums, first=first):
            z = aligned(t, 8)
            sums = list(sums)
            for lane in range(0, lanes, LANES):
                cut = pl.ds(lane, LANES)
                v_re = [vec_r[0, b, z, cut] for b in range(p.bands)]
                v_im = [vec_r[1, b, z, cut] for b in range(p.bands)]
                for j in range(group):
                    b_re = beta_r[0, first + j, z, cut]
                    b_im = beta_r[1, first + j, z, cut]
                    for b in range(p.bands):
                        to = (j * p.bands + b) * 2
                        sums[to] = sums[to] + (b_re * v_re[b] + b_im * v_im[b])
                        sums[to + 1] = sums[to + 1] + (b_re * v_im[b] - b_im * v_re[b])
            return tuple(sums)

        zero = jnp.zeros((8, LANES), f32)
        sums = lax.fori_loop(0, grid // 8, body, (zero,) * (group * p.bands * 2), unroll=unroll)
        for j in range(group):
            for n in range(2 * p.bands):
                sums_r[n, pl.ds(base + first + j, 1), :] = jnp.sum(
                    sums[j * p.bands * 2 + n], axis=0, keepdims=True
                )


def lane_totals(p, sums_r, out_r):
    ones = jnp.ones((8, LANES), bf16)
    for n in range(2 * p.bands):
        hi, mid, lo = split3(sums_r[n])
        out_r[n : n + 1, :] = (dot_t(ones, hi) + dot_t(ones, mid) + dot_t(ones, lo))[0:1]


def project_call(p, beta, vec, chunks, number):
    parts, count, grid, own = beta.shape
    some = math.gcd(count, 32)
    steps = count // some

    def kernel(beta_r, vec_r, chunks_r, out_r, proj_r, sums, held, send, recv):
        step = pl.program_id(0)
        me = lax.axis_index("ga")
        copies = pushes("ga", p.shards, chunks_r, held, send, recv, True)

        @pl.when(step == 0)
        def _():
            greet("ga", p.shards)
            met(p.shards)
            for copy in copies:
                copy.start()
            out_r[me] = chunks_r[me]

        project_block(p, beta_r, vec_r, sums, step * some, 4, 3)

        @pl.when(step == steps - 1)
        def _():
            lane_totals(p, sums, proj_r)
            for copy in copies:
                copy.wait()
            collect(p, held, out_r)

    whole = lambda shape: pl.BlockSpec(shape, lambda i: (0,) * len(shape))
    return pl.pallas_call(
        kernel,
        grid=(steps,),
        out_shape=[spec_of(chunks.shape), spec_of((2 * p.bands, count))],
        in_specs=[
            pl.BlockSpec((parts, some, grid, own), lambda i: (0, i, 0, 0)),
            whole(vec.shape),
            VMEM,
        ],
        out_specs=[VMEM, whole((2 * p.bands, count))],
        scratch_shapes=[
            pltpu.VMEM((2 * p.bands, count, LANES), f32),
            pltpu.VMEM(chunks.shape, f32),
        ]
        + sems(p.shards),
        compiler_params=pltpu.CompilerParams(collective_id=number, has_side_effects=True),
        cost_estimate=pl.CostEstimate(
            flops=4 * beta.size * p.bands, bytes_accessed=4 * beta.size, transcendentals=0
        ),
        name=f"project_{number}",
    )(beta, vec, chunks)


def payload_of(p, proj_r, stat_r, field_stat_r, pay):
    pay[0 : 2 * p.bands, :] = proj_r[...]
    for b in range(p.bands):
        norm = jnp.sum(stat_r[0, b], axis=0, keepdims=True)
        curve = jnp.sum(stat_r[1, b] + field_stat_r[b], axis=0, keepdims=True)
        both = jnp.concatenate([norm, curve], axis=0)
        both = jnp.broadcast_to(jnp.sum(both, axis=1, keepdims=True), both.shape)
        pay[2 * p.bands + b : 2 * p.bands + b + 1, :] = both[0:1]
        pay[3 * p.bands + b : 3 * p.bands + b + 1, :] = both[1:2]


def couple_rows(p, total, pair_r, coef_r):
    ones = jnp.ones((LANES, LANES), bf16)
    energy = []
    for b in range(p.bands):
        made = 0.0
        for n in (2 * b, 2 * b + 1):
            row = total[n : n + 1]
            product = pair_r[...] * row
            hi, mid, lo = split3(product)
            coef = dot(hi, ones) + dot(mid, ones) + dot(lo, ones)
            if coef_r is not None:
                coef_r[n] = coef
            eye = (
                lax.broadcasted_iota(jnp.int32, coef.shape, 0)
                == lax.broadcasted_iota(jnp.int32, coef.shape, 1)
            )
            on_lanes = jnp.sum(jnp.where(eye, coef, 0.0), axis=0, keepdims=True)
            made = made + jnp.sum(on_lanes * row, axis=1, keepdims=True)
        energy.append(made)
    return energy


def spread_block(p, beta_r, coef_r, out_r, base, group):
    _, some, grid, lanes = beta_r.shape
    for lane in range(0, lanes, LANES):
        cut = pl.ds(lane, LANES)
        for first in range(0, some, group):
            coef = [
                [
                    jnp.broadcast_to(coef_r[n, pl.ds(base + first + j, 1), :], (8, LANES))
                    for n in range(2 * p.bands)
                ]
                for j in range(group)
            ]

            def body(t, carry, first=first, coef=coef, cut=cut):
                z = aligned(t, 8)
                re = [out_r[0, b, z, cut] for b in range(p.bands)]
                im = [out_r[1, b, z, cut] for b in range(p.bands)]
                for j in range(group):
                    b_re = beta_r[0, first + j, z, cut]
                    b_im = beta_r[1, first + j, z, cut]
                    for b in range(p.bands):
                        c_re, c_im = coef[j][2 * b], coef[j][2 * b + 1]
                        re[b] = re[b] + (b_re * c_re - b_im * c_im)
                        im[b] = im[b] + (b_re * c_im + b_im * c_re)
                for b in range(p.bands):
                    out_r[0, b, z, cut] = re[b]
                    out_r[1, b, z, cut] = im[b]
                return carry

            lax.fori_loop(0, grid // 8, body, 0, unroll=2)


def residual_call(p, beta, lines, rhs, diag, pair, proj, stat, field_stat, number):
    parts, count, grid, own = beta.shape
    some = math.gcd(count, 32)
    steps = count // some
    tall = 8
    payload = -(-4 * p.bands // 8) * 8

    def kernel(
        beta_r, lines_r, rhs_r, diag_r, pair_r, proj_r, stat_r, field_stat_r, z_fwd_r, z_inv_r,
        res_r, chunks_r, new_stat_r, step_r,
        held, joined, image, back, pay, sums, coef, send0, recv0, send1, recv1,
    ):
        step = pl.program_id(0)
        me = lax.axis_index("ga")
        copies = pushes("ga", p.shards, lines_r, held, send0, recv0, True)
        small = pushes("ga", p.shards, pay, sums, send1, recv1, False)

        @pl.when(step == 0)
        def _():
            greet("ga", p.shards)
            payload_of(p, proj_r, stat_r, field_stat_r, pay)
            met(p.shards)
            for copy in small:
                copy.start()
            for copy in copies:
                copy.start()
            sums[me] = pay[...]
            held[me] = lines_r[me]
            back[...] = jnp.zeros_like(back)
            for copy in small:
                copy.wait()
            total = sums[0]
            for at in range(1, p.shards):
                total = total + sums[at]
            energy = couple_rows(p, total, pair_r, coef)
            for b in range(p.bands):
                norm = total[2 * p.bands + b : 2 * p.bands + b + 1]
                curve = total[3 * p.bands + b : 3 * p.bands + b + 1] + energy[b]
                step_r[b : b + 1, :] = norm
                step_r[p.bands + b : p.bands + b + 1, :] = norm / curve

        spread_block(p, beta_r, coef, back, step * some, 8)

        @pl.when(step == steps - 1)
        def _():
            for copy in copies:
                copy.wait()
            from_lines(p, held, joined, z_fwd_r, image)
            for b in range(p.bands):
                alpha = step_r[p.bands + b : p.bands + b + 1, :]

                def fresh(t, acc, b=b, alpha=alpha):
                    z = aligned(t, tall)
                    norm, curve = acc
                    for lane in range(0, own, LANES):
                        cut = pl.ds(lane, LANES)
                        scale = diag_r[b, z, cut]
                        square = 0.0
                        for c in range(2):
                            r = rhs_r[c, b, z, cut]
                            made = scale * r + image[c, b, z, cut] + back[c, b, z, cut]
                            new = r - alpha * made
                            res_r[c, b, z, cut] = new
                            square = square + new * new
                        norm = norm + square
                        curve = curve + square * scale
                    return norm, curve

                zero = jnp.zeros((tall, LANES), f32)
                norm, curve = lax.fori_loop(0, grid // tall, fresh, (zero, zero))
                new_stat_r[0, b] = norm
                new_stat_r[1, b] = curve
            to_lines(
                p,
                lambda b: jnp.concatenate([res_r[0, b], res_r[1, b]], axis=0),
                z_inv_r,
                chunks_r,
                False,
            )

    shape = (p.shards, p.rows, p.own)
    mine = (2, p.bands, p.grid, p.own)
    return pl.pallas_call(
        kernel,
        grid=(steps,),
        out_shape=[
            spec_of(mine), spec_of(shape), spec_of((2, p.bands, 8, LANES)),
            spec_of((2 * p.bands, LANES)),
        ],
        in_specs=[pl.BlockSpec((parts, some, grid, own), lambda i: (0, i, 0, 0))] + [VMEM] * 9,
        out_specs=[VMEM] * 4,
        scratch_shapes=[
            pltpu.VMEM(shape, f32),
            pltpu.VMEM((p.shards * p.q, p.own), f32),
            pltpu.VMEM(mine, f32),
            pltpu.VMEM(mine, f32),
            pltpu.VMEM((payload, LANES), f32),
            pltpu.VMEM((p.shards, payload, LANES), f32),
            pltpu.VMEM((2 * p.bands, count, LANES), f32),
        ]
        + sems(p.shards)
        + sems(p.shards),
        compiler_params=pltpu.CompilerParams(collective_id=number, has_side_effects=True),
        cost_estimate=pl.CostEstimate(
            flops=4 * beta.size * p.bands, bytes_accessed=4 * beta.size, transcendentals=0
        ),
        name=f"residual_{number}",
    )(beta, lines, rhs, diag, pair, proj, stat, field_stat, p.z_fwd, p.z_inv)


def last_call(p, groups, rhs, res, pair, proj, stat, field_stat, step, fields, number):
    payload = -(-4 * p.bands // 8) * 8
    wide = p.grid // groups
    dense = p.planes % 4 == 0 and LANES - p.grid == p.grid // 3
    thick = p.planes * 3 // 4 if dense else p.planes
    rest = LANES - p.grid

    def kernel(
        rhs_r, res_r, pair_r, proj_r, stat_r, field_stat_r, step_r, psi_r, f0_r, f1_r,
        resp_r, dens_r,
        pay, sums, chunks, got, send0, recv0, send1, recv1,
    ):
        greet("ga", p.shards)
        greet("band", groups)
        payload_of(p, proj_r, stat_r, field_stat_r, pay)
        met(p.shards + groups - 1)
        me = lax.axis_index("ga")
        copies = pushes("ga", p.shards, pay, sums, send0, recv0, False)
        for copy in copies:
            copy.start()
        sums[me] = pay[...]
        for copy in copies:
            copy.wait()
        total = sums[0]
        for at in range(1, p.shards):
            total = total + sums[at]
        energy = couple_rows(p, total, pair_r, None)
        keep, alpha1 = [], []
        for b in range(p.bands):
            norm0 = step_r[b : b + 1, :]
            alpha0 = step_r[p.bands + b : p.bands + b + 1, :]
            norm1 = total[2 * p.bands + b : 2 * p.bands + b + 1]
            curve = total[3 * p.bands + b : 3 * p.bands + b + 1] + energy[b]
            ratio = norm1 / norm0
            alpha = norm1 / (curve - ratio * norm1 / alpha0)
            alpha1.append(alpha)
            keep.append(alpha0 + alpha * ratio)

        def plane(zp):
            made = 0.0
            for b in range(p.bands):
                at = aligned(b * p.planes + zp, p.grid)
                k2 = jnp.concatenate([keep[b], keep[b]], axis=1)
                a2 = jnp.concatenate([alpha1[b], alpha1[b]], axis=1)
                made = made + psi_r[at, :] * (k2 * f0_r[at, :] + a2 * f1_r[at, :])
            return 4.0 * (made[:, :LANES] + made[:, LANES:])

        lane = lax.broadcasted_iota(jnp.int32, (1, LANES), 1)

        def put(at, value):
            for g in range(groups):
                chunks[g, at] = value[g * wide : (g + 1) * wide]

        if dense:

            def four(i, carry):
                last = plane(4 * i + 3)
                for k in range(3):
                    moved = pltpu.roll(last, p.grid - k * rest, 1)
                    put(3 * i + k, jnp.where(lane < p.grid, plane(4 * i + k), moved))
                return carry

            lax.fori_loop(0, p.planes // 4, four, 0)
        else:

            def single(i, carry):
                put(i, plane(i))
                return carry

            lax.fori_loop(0, p.planes, single, 0)

        mine = lax.axis_index("band")
        copies = pushes("band", groups, chunks, got, send1, recv1, True)
        for copy in copies:
            copy.start()
        got[mine] = chunks[mine]
        for b in range(p.bands):

            def answer(t, carry, b=b):
                z = aligned(t, 8)
                for lane_at in range(0, p.own, LANES):
                    cut = pl.ds(lane_at, LANES)
                    for c in range(2):
                        resp_r[c, b, z, cut] = (
                            keep[b] * rhs_r[c, b, z, cut] + alpha1[b] * res_r[c, b, z, cut]
                        )
                return carry

            lax.fori_loop(0, p.grid // 8, answer, 0)
        for copy in copies:
            copy.wait()
        for at in range(thick):
            value = got[0, at]
            for g in range(1, groups):
                value = value + got[g, at]
            got[0, at] = value
        if dense:
            for i in range(p.planes // 4):
                last = jnp.zeros((wide, LANES), f32)
                for k in range(3):
                    value = got[0, 3 * i + k]
                    dens_r[4 * i + k] = value
                    moved = pltpu.roll(value, LANES - p.grid + k * rest, 1)
                    inside = (lane >= k * rest) & (lane < (k + 1) * rest)
                    last = jnp.where(inside, moved, last)
                dens_r[4 * i + 3] = last
        else:
            for at in range(p.planes):
                dens_r[at] = got[0, at]

    mine = (2, p.bands, p.grid, p.own)
    return pl.pallas_call(
        kernel,
        out_shape=[spec_of(mine), spec_of((p.planes, wide, LANES))],
        in_specs=[VMEM] * 10,
        out_specs=[VMEM] * 2,
        scratch_shapes=[
            pltpu.VMEM((payload, LANES), f32),
            pltpu.VMEM((p.shards, payload, LANES), f32),
            pltpu.VMEM((groups, thick, wide, LANES), f32),
            pltpu.VMEM((groups, thick, wide, LANES), f32),
        ]
        + sems(p.shards)
        + sems(groups),
        compiler_params=pltpu.CompilerParams(collective_id=number, has_side_effects=True),
        name="finish",
    )(rhs, res, pair, proj, stat, field_stat, step, *fields)


def per_device(groups, shards, psi, vloc, dv, beta, dij, atom_type, stick_xy, band_shift):
    _, bands, grid, own = psi.shape
    planes = vloc.shape[0]
    sticks = stick_xy.shape[0]
    p = Plan(bands, grid, own, planes, shards, sticks)
    radius = grid // 3
    per_atom = dij.shape[1]
    count = beta.shape[1]

    ky = frequency(stick_xy // grid, grid) + radius
    kx = frequency(stick_xy % grid, grid) + radius
    group = ky // PER
    slot = (ky % PER) * p.side + kx
    places = jnp.arange(p.wide, dtype=jnp.int32)
    oh = (slot[:, None] == places[None, :]).astype(bf16)
    oh_t = (slot[None, :] == places[:, None]).astype(bf16)
    kinds = jnp.arange(p.groups, dtype=jnp.int32)
    mask = jnp.broadcast_to(
        (group[None, None, :] == kinds[:, None, None]), (p.groups, 16, sticks)
    ).astype(bf16)
    group_of = jnp.broadcast_to(group[None, :], (8, sticks))
    tables = (oh, oh_t, mask, group_of)

    def widen(field):
        shaped = jnp.pad(field.reshape(planes, grid, grid), ((0, 0), (0, 0), (0, LANES - grid)))
        return shaped.reshape(planes * grid, LANES)

    start = lax.axis_index("ga") * own
    own_xy = lax.dynamic_slice_in_dim(stick_xy, start, own)
    freq_z = frequency(jnp.arange(grid, dtype=jnp.int32), grid)
    summed = (
        freq_z[:, None] ** 2
        + (frequency(own_xy // grid, grid) ** 2 + frequency(own_xy % grid, grid) ** 2)[None, :]
    )
    kinetic = summed.astype(f32) * (4.0 / (grid * grid))
    diag = kinetic[None] + band_shift[:, None, None]

    index = jnp.arange(count, dtype=jnp.int32)
    kind = jnp.arange(dij.shape[0], dtype=jnp.int32)
    chosen = (atom_type[:, None] == kind[None, :]).astype(f32)
    selected = jnp.sum(chosen[:, :, None, None] * dij[None], axis=1).reshape(count, per_atom)
    pair = jnp.where(
        (index // per_atom)[:, None] == (index // per_atom)[None, :],
        jnp.tile(selected, (1, count // per_atom)),
        0.0,
    )

    others = [
        lax.ppermute(psi, "band", [(src, (src + hop) % groups) for src in range(groups)])
        for hop in range(1, groups)
    ]
    gathered = jnp.concatenate([psi] + others, axis=1)

    held = first_call(p, psi)
    psi_real, lines = planes_call(p, held, tables, widen(dv), True, False, "planes_dv")
    rhs, chunks, stat0 = rhs_call(p, lines, gathered, diag)
    held, proj0 = project_call(p, beta, rhs, chunks, 2)
    pot = widen(vloc)
    field0, lines, plane0 = planes_call(p, held, tables, pot, True, True, "planes_rhs")
    res, chunks, stat1, step = residual_call(
        p, beta, lines, rhs, diag, pair, proj0, stat0, plane0, 3
    )
    held, proj1 = project_call(p, beta, res, chunks, 4)
    field1, plane1 = planes_call(p, held, tables, pot, False, True, "planes_res")
    response, density = last_call(
        p, groups, rhs, res, pair, proj1, stat1, plane1, step, (psi_real, field0, field1), 5
    )
    density = density[:, :, :grid].reshape(planes, grid * grid // groups)
    return (response, density)


def solution(mesh):
    placed = (
        P(None, "band", None, "ga"),
        P("ga", None),
        P("ga", None),
        P(None, None, None, "ga"),
        P(),
        P(),
        P(),
        P("band"),
    )
    groups, shards = mesh.shape["band"], mesh.shape["ga"]

    def body(*args):
        return per_device(groups, shards, *args)

    return jax.shard_map(
        body,
        mesh=mesh,
        in_specs=placed,
        out_specs=(P(None, "band", None, "ga"), P("ga", "band")),
        check_vma=False,
    )
```

```python
import math

import jax
import jax.numpy as jnp
import ml_dtypes
import numpy as np
from jax import lax
from jax.experimental import pallas as pl
from jax.experimental.pallas import tpu as pltpu
from jax.sharding import PartitionSpec as P

LANES = 128
PER = 4
f32, bf16 = jnp.float32, jnp.bfloat16
VMEM = pl.BlockSpec(memory_space=pltpu.VMEM)


def frequency(index, grid):
    return (index + grid // 2) % grid - grid // 2


def phase(rows, cols, grid, sign):
    angle = 2.0 * math.pi * ((rows[:, None] * cols[None, :]) % grid) / grid
    return np.exp(1j * sign * angle) / math.sqrt(grid)


def parts_of(table):
    return np.stack(
        [np.stack([table.real, -table.imag], 1), np.stack([table.imag, table.real], 1)]
    )


def halves_of(table):
    table = table.astype(np.float32)
    hi = table.astype(ml_dtypes.bfloat16)
    lo = (table - hi.astype(np.float32)).astype(ml_dtypes.bfloat16)
    return hi, lo


class Plan:
    def __init__(self, bands, grid, own, planes, shards, sticks, count):
        self.bands, self.grid, self.own, self.planes = bands, grid, own, planes
        self.shards, self.sticks, self.count = shards, sticks, count
        self.side = 2 * (grid // 3)
        self.q = 2 * planes
        self.rows = -(-bands * self.q // 16) * 16
        self.images = bands * planes
        self.groups = self.side // PER
        self.fold = LANES // self.side
        self.tiles = PER // self.fold
        self.wide = PER * self.side
        side, fold, tiles, groups = self.side, self.fold, self.tiles, self.groups
        cells = np.arange(grid)
        freqs = np.arange(side) - grid // 3
        z = parts_of(phase(cells, cells, grid, 1.0))
        z = z.reshape(2, shards, planes, 2 * grid).transpose(1, 0, 2, 3)
        self.z_inv = np.stack(halves_of(z.reshape(shards * self.q, 2 * grid)))
        z = parts_of(phase(cells, cells, grid, -1.0))
        z = z.reshape(2, grid, 2, shards, planes).transpose(0, 1, 3, 2, 4)
        self.z_fwd = np.stack(halves_of(z.reshape(2 * grid, shards * self.q)))
        y = parts_of(phase(cells, freqs, grid, 1.0))
        y = y.reshape(2, grid, 2, groups, tiles, fold).transpose(0, 5, 1, 2, 4, 3)
        hi, lo = halves_of(y.reshape(2 * fold * grid, 2 * tiles * groups))
        self.y_inv = np.concatenate([hi, hi, lo], axis=1)
        x = parts_of(phase(freqs, cells, grid, 1.0).T).transpose(2, 3, 0, 1)
        x = np.repeat(x[:, None], fold, axis=1)
        x = np.pad(x, ((0, 0),) * 4 + ((0, LANES - grid),))
        self.x_inv = np.stack(halves_of(x.reshape(2 * LANES, 2 * LANES)))
        x = parts_of(phase(cells, freqs, grid, -1.0).T).transpose(2, 3, 0, 1)
        x = np.repeat(x[:, :, :, None], fold, axis=3)
        x = np.pad(x, ((0, 0), (0, LANES - grid)) + ((0, 0),) * 3)
        self.x_fwd = np.stack(halves_of(x.reshape(2 * LANES, 2 * LANES)))
        y = parts_of(phase(freqs, cells, grid, -1.0))
        y = y.reshape(2, groups, tiles, fold, 2 * grid).transpose(0, 3, 2, 1, 4)
        self.y_fwd = np.stack(halves_of(y.reshape(2 * side, 2 * grid)))


def dot(a, b):
    return jnp.dot(a, b, preferred_element_type=f32)


def dot_t(a, b):
    return lax.dot_general(a, b, (((1,), (1,)), ((), ())), preferred_element_type=f32)


def split(x):
    hi = x.astype(bf16)
    return hi, (x - hi.astype(f32)).astype(bf16)


def split3(x):
    hi = x.astype(bf16)
    rest = x - hi.astype(f32)
    mid = rest.astype(bf16)
    return hi, mid, (rest - mid.astype(f32)).astype(bf16)


def aligned(at, size):
    return pl.ds(pl.multiple_of(at * size, math.gcd(size, LANES)), size)


def spec_of(shape, dtype=f32):
    return jax.ShapeDtypeStruct(shape, dtype)


def lines_to_rows(p, held, oh_t, mask, left, sq):
    def spread(src, carry):
        at = aligned(src, p.own)
        hi, lo = split(held[src])
        for g in range(p.groups):
            keep = mask[g, :, at]
            for r in range(0, p.rows, 16):
                to = pl.ds(g * p.rows + r, 16)
                left[0, to, at] = hi[r : r + 16] * keep
                left[1, to, at] = lo[r : r + 16] * keep
        return carry

    lax.fori_loop(0, p.shards, spread, 0)
    made = dot_t(left[0], oh_t[...]) + dot_t(left[1], oh_t[...])
    for t in range(p.tiles):
        sq[t] = made[:, t * LANES : (t + 1) * LANES]


def rows_to_mixed(p, sq, y_inv, mixed):
    low = lax.broadcasted_iota(jnp.int32, (1, 2 * LANES), 1) % LANES < p.side

    def pair(at, carry):
        for b in range(p.bands):
            tiles = []
            for k in range(2):
                pieces = []
                for c in range(2):
                    n = b * p.q + c * p.planes + 2 * at + k
                    for t in range(p.tiles):
                        pieces.append(sq[t, pl.ds(n, p.groups, stride=p.rows), :])
                tiles.append(jnp.concatenate(pieces, axis=0))
            hi, lo = split(jnp.concatenate(tiles, axis=1))
            out = dot(y_inv[...], jnp.concatenate([hi, lo, hi], axis=0))
            both = [
                jnp.where(
                    low,
                    out[2 * c * p.grid : (2 * c + 1) * p.grid],
                    out[(2 * c + 1) * p.grid : (2 * c + 2) * p.grid],
                )
                for c in range(2)
            ]
            for k in range(2):
                lane = slice(k * LANES, (k + 1) * LANES)
                hi, lo = split(jnp.concatenate([both[0][:, lane], both[1][:, lane]], axis=1))
                to = aligned(b * p.planes + 2 * at + k, p.grid)
                mixed[0, to, :] = hi
                mixed[1, to, :] = lo
        return carry

    lax.fori_loop(0, p.planes // 2, pair, 0)


def mixed_to_field(p, mixed, x_inv, x_fwd, pot, field, spectrum, stat):
    some = math.gcd(p.planes, 4)
    size = some * p.grid

    for b in range(p.bands):

        def block(at, total, b=b):
            to = aligned(b * (p.planes // some) + at, size)
            hi, lo = mixed[0, to, :], mixed[1, to, :]
            one = dot(hi, x_inv[0]) + dot(lo, x_inv[0]) + dot(hi, x_inv[1])
            field[to, :] = one
            wide = pot[aligned(at, size), :]
            used = one * jnp.concatenate([wide, wide], axis=1)
            if spectrum is not None:
                hi, lo = split(used)
                spectrum[to, :] = dot(hi, x_fwd[0]) + dot(lo, x_fwd[0]) + dot(hi, x_fwd[1])
            if stat is not None:
                made = jnp.sum((used * one).reshape(size // 8, 8, 2 * LANES), axis=0)
                total = total + made[:, :LANES] + made[:, LANES:]
            return total

        total = lax.fori_loop(0, p.planes // some, block, jnp.zeros((8, LANES), f32))
        if stat is not None:
            stat[b] = total


def spectrum_to_lines(p, spectrum, y_fwd, oh_t, rows_of, sq, left, lines, held, push):
    low = lax.broadcasted_iota(jnp.int32, (1, 2 * LANES), 1) % LANES < p.side
    half = p.side // p.fold

    def pair(at, carry):
        for b in range(p.bands):
            tiles = []
            for k in range(2):
                one = spectrum[aligned(b * p.planes + 2 * at + k, p.grid), :]
                tiles.append(jnp.concatenate([one[:, :LANES], one[:, LANES:]], axis=0))
            hi, lo = split(jnp.concatenate(tiles, axis=1))
            out = dot(y_fwd[0], hi) + dot(y_fwd[0], lo) + dot(y_fwd[1], hi)
            for c in range(2):
                from_ = c * p.side
                both = jnp.where(
                    low, out[from_ : from_ + half], out[from_ + half : from_ + 2 * half]
                )
                for k in range(2):
                    to = aligned(b * p.q + c * p.planes + 2 * at + k, p.groups)
                    for t in range(p.tiles):
                        sq[t, to, :] = both[
                            t * p.groups : (t + 1) * p.groups, k * LANES : (k + 1) * LANES
                        ]
        return carry

    lax.fori_loop(0, p.planes // 2, pair, 0)
    for g in range(p.groups):
        to = pl.ds(g * p.rows, p.rows)
        for t in range(p.tiles):
            hi, lo = split(sq[t, pl.ds(g, p.rows, stride=p.groups), :])
            left[0, to, t * LANES : (t + 1) * LANES] = hi
            left[1, to, t * LANES : (t + 1) * LANES] = lo

    def gather(dest):
        at = aligned(dest, p.own)
        weights = oh_t[:, at]
        got = dot(left[0, :, : p.wide], weights) + dot(left[1, :, : p.wide], weights)
        kind = rows_of[1:2, at]
        kept = got[: p.rows]
        for g in range(1, p.groups):
            kept = jnp.where(kind == g, got[g * p.rows : (g + 1) * p.rows], kept)
        return kept

    me = lax.axis_index("ga")

    def each(hop, carry):
        dest = lax.rem(me + hop, p.shards)
        lines[dest] = gather(dest)

        @pl.when(hop > 1)
        def _():
            push(hop - 1).start()

        return carry

    lax.fori_loop(1, p.shards, each, 0)
    held[me] = gather(me)
    push(p.shards - 1).start()


def greet(axis, count):
    me = lax.axis_index(axis)
    barrier = pltpu.get_barrier_semaphore()
    for hop in range(1, count):
        peer = lax.rem(me + hop, count)
        pl.semaphore_signal(
            barrier, inc=1, device_id={axis: peer}, device_id_type=pl.DeviceIdType.MESH
        )


def pusher(axis, count, source, held, sends, recvs, which, scatter):
    me = lax.axis_index(axis)

    def push(hop):
        peer = lax.rem(me + hop, count)
        return pltpu.make_async_remote_copy(
            src_ref=source.at[peer] if scatter else source,
            dst_ref=held.at[me],
            send_sem=sends.at[which, hop - 1],
            recv_sem=recvs.at[which, hop - 1],
            device_id={axis: peer},
            device_id_type=pl.DeviceIdType.MESH,
        )

    return push


def start_all(push, count):
    for hop in range(1, count):
        push(hop).start()


def wait_all(push, count):
    for hop in range(1, count):
        push(hop).wait()


def total_of(sums, count):
    total = sums[0]
    for at in range(1, count):
        total = total + sums[at]
    return total


def to_lines(p, value_of, z_inv, chunks, exact):
    for b in range(p.bands):
        value = value_of(b)
        if exact:
            out = dot(z_inv[0], value) + dot(z_inv[1], value)
        else:
            hi, lo = split(value)
            out = dot(z_inv[0], hi) + dot(z_inv[0], lo) + dot(z_inv[1], hi)
        for d in range(p.shards):
            chunks[d, b * p.q : (b + 1) * p.q, :] = out[d * p.q : (d + 1) * p.q]


def from_lines(p, held, joined, z_fwd, result):
    for b in range(p.bands):
        for src in range(p.shards):
            joined[src * p.q : (src + 1) * p.q, :] = held[src, b * p.q : (b + 1) * p.q, :]
        hi, lo = split(joined[...])
        out = dot(z_fwd[0], hi) + dot(z_fwd[0], lo) + dot(z_fwd[1], hi)
        result[0, b] = out[: p.grid]
        result[1, b] = out[p.grid :]


TALL = 16
JB = 4
SLOTS = 4


def fetch(p, beta_hbm, staged, sem, at):
    return pltpu.make_async_copy(
        beta_hbm.at[:, pl.ds(at * JB, JB)], staged.at[at % SLOTS], sem.at[at % SLOTS]
    )


def convert(p, beta_hbm, staged, sem, beta, first, last):
    chunks = p.count // JB
    for at in range(first, last):
        fetch(p, beta_hbm, staged, sem, at).wait()
        slot = at % SLOTS

        def one(j, carry, at=at, slot=slot):
            for c in range(2):
                hi, lo = split(staged[slot, c, j])
                beta[0, c, at * JB + j] = hi
                beta[1, c, at * JB + j] = lo
            return carry

        lax.fori_loop(0, JB, one, 0)
        if at + SLOTS < chunks:
            fetch(p, beta_hbm, staged, sem, at + SLOTS).start()


def stack_vector(p, vec, stacked):
    for zt in range(p.grid // TALL):
        for b in range(p.bands):
            for c in range(2):
                hi, lo = split(vec[c, b, zt * TALL : (zt + 1) * TALL, :])
                at = (2 * b + c) * 2 * TALL
                stacked[zt, at : at + TALL, :] = hi
                stacked[zt, at + TALL : at + 2 * TALL, :] = lo


def project(p, beta, stacked, acc, pay):
    cols = 4 * p.bands * TALL
    keep = (
        lax.broadcasted_iota(jnp.int32, (TALL, cols), 0)
        == lax.broadcasted_iota(jnp.int32, (TALL, cols), 1) % TALL
    )
    some = math.gcd(p.count, 32)
    acc[...] = jnp.zeros_like(acc)

    def tile(at, carry):
        zt = at // (p.count // some)
        first = lax.rem(at, p.count // some) * some
        z = aligned(zt, TALL)
        right = stacked[zt]
        for c in range(2):
            hi = beta[0, c, pl.ds(first, some), z, :].reshape(some * TALL, p.own)
            lo = beta[1, c, pl.ds(first, some), z, :].reshape(some * TALL, p.own)
            out = (dot_t(hi, right) + dot_t(lo, right)).reshape(some, TALL, cols)
            out = jnp.where(keep[None], out, 0.0)
            acc[c, pl.ds(first, some)] += out[:, :8] + out[:, 8:]
        return carry

    lax.fori_loop(0, (p.grid // TALL) * (p.count // some), tile, 0)
    row = lax.broadcasted_iota(jnp.int32, (8, cols), 0)
    kind = lax.broadcasted_iota(jnp.int32, (8, cols), 1) // (2 * TALL)
    same = (row // 2 == kind // 2) & (row < 2 * p.bands)
    plain = jnp.where(same & (row % 2 == kind % 2), 1.0, 0.0).astype(bf16)
    cross = jnp.where(
        same & (row % 2 != kind % 2), jnp.where(row % 2 == 0, 1.0, -1.0), 0.0
    ).astype(bf16)
    made = 0.0
    for c, pick in ((0, plain), (1, cross)):
        for piece in split3(jnp.sum(acc[c], axis=1)):
            made = made + dot_t(pick, piece)
    pay[0 : 2 * p.bands, :] = made[: 2 * p.bands]


def couple(p, total, pair):
    hi, mid, lo = split3(total)
    p_hi, p_mid, p_lo = split3(pair[...])
    made = (
        dot_t(hi, p_hi) + dot_t(hi, p_mid) + dot_t(mid, p_hi)
        + dot_t(hi, p_lo) + dot_t(mid, p_mid) + dot_t(lo, p_hi)
    )
    product = jnp.sum(made * total, axis=1, keepdims=True)
    energy = [product[2 * b : 2 * b + 1] + product[2 * b + 1 : 2 * b + 2] for b in range(p.bands)]
    return made, energy


def build_coefs(p, made, coefs):
    blocks = p.count // TALL
    wide = TALL * TALL
    lane = lax.broadcasted_iota(jnp.int32, (TALL, wide), 1) // TALL
    source = lax.broadcasted_iota(jnp.int32, (TALL, wide), 0)
    repeat = jnp.where(lane == source, 1.0, 0.0).astype(bf16)
    keep = (
        lax.broadcasted_iota(jnp.int32, (TALL, wide), 0)
        == lax.broadcasted_iota(jnp.int32, (TALL, wide), 1) % TALL
    )
    hi, mid, lo = split3(made)
    for jb in range(blocks):
        cut = slice(jb * TALL, (jb + 1) * TALL)
        full = dot(hi[:, cut], repeat) + dot(mid[:, cut], repeat) + dot(lo[:, cut], repeat)
        for b in range(p.bands):
            re, im = full[2 * b : 2 * b + 1], full[2 * b + 1 : 2 * b + 2]
            for part, rows in ((0, (re, im)), (1, (-im, re))):
                for c in range(2):
                    one, two = split(jnp.where(keep, rows[c], 0.0))
                    to = slice((2 * b + c) * TALL, (2 * b + c + 1) * TALL)
                    at = slice((2 * jb + part) * wide, (2 * jb + part + 1) * wide)
                    coefs[0, to, at] = one
                    coefs[1, to, at] = two


def back_project(p, beta, coefs, back):
    blocks = p.count // TALL
    wide = TALL * TALL
    many = 2 * p.bands * TALL

    def tile(zt, carry):
        z = aligned(zt, TALL)
        made = jnp.zeros((many, p.own), f32)
        for jb in range(blocks):
            for part in range(2):
                js = slice(jb * TALL, (jb + 1) * TALL)
                hi = beta[0, part, js, z, :].reshape(wide, p.own)
                lo = beta[1, part, js, z, :].reshape(wide, p.own)
                at = slice((2 * jb + part) * wide, (2 * jb + part + 1) * wide)
                c_hi, c_lo = coefs[0, :, at], coefs[1, :, at]
                made = made + dot(c_hi, hi) + dot(c_lo, hi) + dot(c_hi, lo)
        for b in range(p.bands):
            for c in range(2):
                at = (2 * b + c) * TALL
                back[c, b, z, :] = made[at : at + TALL]
        return carry

    lax.fori_loop(0, p.grid // TALL, tile, 0)


def intersect(p, groups, gath, image, part):
    many = groups * p.bands
    inv_norm = 1.0 / (2.0 * p.grid * p.sticks)
    for n in range(p.bands):

        def overlap(t, acc, n=n):
            z = aligned(t, TALL)
            acc = list(acc)
            for lane in range(0, p.own, LANES):
                cut = pl.ds(lane, LANES)
                i_re, i_im = image[0, n, z, cut], image[1, n, z, cut]
                for m in range(many):
                    p_re = gath[m // p.bands, 0, m % p.bands, z, cut].astype(f32)
                    p_im = gath[m // p.bands, 1, m % p.bands, z, cut].astype(f32)
                    re = p_re * i_re + p_im * i_im
                    im = p_re * i_im - p_im * i_re
                    acc[2 * m] = acc[2 * m] + (re[:8] + re[8:])
                    acc[2 * m + 1] = acc[2 * m + 1] + (im[:8] + im[8:])
            return tuple(acc)

        zero = jnp.zeros((8, LANES), f32)
        acc = lax.fori_loop(0, p.grid // TALL, overlap, (zero,) * (2 * many))
        for m in range(2 * many):
            part[pl.ds(n * 2 * many + m, 1), :] = jnp.sum(acc[m], axis=0, keepdims=True)
    part[...] = jnp.broadcast_to(
        jnp.sum(part[...], axis=1, keepdims=True) * inv_norm, part.shape
    )


def right_side(p, groups, gath, image, inter, diag, rhs):
    many = groups * p.bands
    stats = []
    for n in range(p.bands):

        def right(t, acc, n=n):
            z = aligned(t, TALL)
            norm, curve = acc
            for lane in range(0, p.own, LANES):
                cut = pl.ds(lane, LANES)
                re, im = -image[0, n, z, cut], -image[1, n, z, cut]
                for m in range(many):
                    p_re = gath[m // p.bands, 0, m % p.bands, z, cut].astype(f32)
                    p_im = gath[m // p.bands, 1, m % p.bands, z, cut].astype(f32)
                    row = n * 2 * many + 2 * m
                    c_re = inter[row : row + 1, :]
                    c_im = inter[row + 1 : row + 2, :]
                    re = re + (c_re * p_re - c_im * p_im)
                    im = im + (c_im * p_re + c_re * p_im)
                rhs[0, n, z, cut] = re
                rhs[1, n, z, cut] = im
                square = re * re + im * im
                norm = norm + square
                curve = curve + square * diag[n, z, cut]
            return norm, curve

        zero = jnp.zeros((TALL, LANES), f32)
        norm, curve = lax.fori_loop(0, p.grid // TALL, right, (zero, zero))
        stats.append((norm, curve))
    return stats


def fresh(p, rhs, image, back, diag, alpha, res):
    stats = []
    for b in range(p.bands):

        def one(t, acc, b=b):
            z = aligned(t, 8)
            norm, curve = acc
            for lane in range(0, p.own, LANES):
                cut = pl.ds(lane, LANES)
                scale = diag[b, z, cut]
                square = 0.0
                for c in range(2):
                    r = rhs[c, b, z, cut]
                    made = scale * r + image[c, b, z, cut] + back[c, b, z, cut]
                    new = r - alpha[b] * made
                    res[c, b, z, cut] = new
                    square = square + new * new
                norm = norm + square
                curve = curve + square * scale
            return norm, curve

        zero = jnp.zeros((8, LANES), f32)
        stats.append(lax.fori_loop(0, p.grid // 8, one, (zero, zero)))
    return stats


def everywhere(x):
    x = jnp.sum(x, axis=0, keepdims=True)
    return jnp.broadcast_to(jnp.sum(x, axis=1, keepdims=True), x.shape)


def pay_stats(p, stats, pay):
    for b in range(p.bands):
        at = 2 * p.bands + b
        pay[at : at + 1, :] = everywhere(stats[b][0])
        at = 3 * p.bands + b
        pay[at : at + 1, :] = everywhere(stats[b][1])


def program(p, groups, psi, pot_dv, pot_v, beta_hbm_array, rows_of, shift, pair):
    payload = -(-4 * p.bands // 8) * 8
    few = -(-p.bands // 8) * 8
    many = groups * p.bands
    inters = p.bands * many * 2
    wide_y = p.grid // groups
    dense = p.planes % 4 == 0 and LANES - p.grid == p.grid // 3
    thick = p.planes * 3 // 4 if dense else p.planes
    rest = LANES - p.grid
    chunk = (p.shards, p.rows, p.own)
    mine = (2, p.bands, p.grid, p.own)
    cells = p.images * p.grid
    many_rows = p.groups * p.rows
    n_chunks = p.count // JB

    def kernel(
        psi_r, pot_dv_r, pot_v_r, beta_hbm, rows_r, shift_r, pair_r,
        z_inv, z_fwd, y_inv, x_inv, x_fwd, y_fwd,
        resp_r, dens_r,
        oh_t, mask, left, sq, mixed, spectrum, field_p, field_0, field_1,
        chunk_a, chunk_b, held_a, held_b, held_c, held_d, held_e,
        gath, joined, image, rhs, res, diag, stat,
        part, sums_i, pay_a, sums_a, pay_b, sums_b, pay_c, sums_c, pay_d, sums_d,
        staged, beta, stacked, acc, coefs,
        dens_send, dens_got,
        beta_sem, sends, recvs, band_sends, band_recvs,
    ):
        me = lax.axis_index("ga")
        mine_band = lax.axis_index("band")

        def over(source, held, which, scatter):
            return pusher("ga", p.shards, source, held, sends, recvs, which, scatter)

        greet("ga", p.shards)
        greet("band", groups)
        for at in range(SLOTS):
            fetch(p, beta_hbm, staged, beta_sem, at).start()
        to_lines(
            p, lambda b: jnp.concatenate([psi_r[0, b], psi_r[1, b]], axis=0), z_inv, chunk_a, True
        )
        pl.semaphore_wait(pltpu.get_barrier_semaphore(), p.shards + groups - 2)
        push_a = over(chunk_a, held_a, 0, True)
        start_all(push_a, p.shards)
        push_psi = pusher("band", groups, psi_r, gath, band_sends, band_recvs, 0, False)
        start_all(push_psi, groups)
        held_a[me] = chunk_a[me]
        gath[mine_band] = psi_r[...]

        def table(at, carry):
            cut = aligned(at, LANES)
            slot = rows_r[0:1, cut]
            rows = lax.broadcasted_iota(jnp.int32, (p.wide, LANES), 0)
            oh_t[:, cut] = jnp.where(rows == slot, 1.0, 0.0).astype(bf16)
            kind = jnp.broadcast_to(rows_r[1:2, cut], (16, LANES))
            for g in range(p.groups):
                mask[g, :, cut] = jnp.where(kind == g, 1.0, 0.0).astype(bf16)
            return carry

        lax.fori_loop(0, p.sticks // LANES, table, 0)
        flat = rows_r[2:3, pl.ds(pl.multiple_of(me * p.own, LANES), p.own)]
        z = lax.broadcasted_iota(jnp.int32, (p.grid, p.own), 0)
        z = jnp.where(z < p.grid // 2, z, z - p.grid)
        kinetic = (z * z + flat).astype(f32) * (4.0 / (p.grid * p.grid))
        for b in range(p.bands):
            diag[b] = kinetic + shift_r[b]
        early = n_chunks // 2
        convert(p, beta_hbm, staged, beta_sem, beta, 0, early)
        wait_all(push_a, p.shards)

        lines_to_rows(p, held_a, oh_t, mask, left, sq)
        rows_to_mixed(p, sq, y_inv, mixed)
        mixed_to_field(p, mixed, x_inv, x_fwd, pot_dv_r, field_p, spectrum, None)
        push_b = over(chunk_b, held_b, 1, True)
        spectrum_to_lines(p, spectrum, y_fwd, oh_t, rows_r, sq, left, chunk_b, held_b, push_b)
        convert(p, beta_hbm, staged, beta_sem, beta, early, n_chunks)
        wait_all(push_psi, groups)
        wait_all(push_b, p.shards)

        from_lines(p, held_b, joined, z_fwd, image)
        intersect(p, groups, gath, image, part)
        push_i = over(part, sums_i, 2, False)
        start_all(push_i, p.shards)
        sums_i[me] = part[...]
        wait_all(push_i, p.shards)
        part[...] = total_of(sums_i, p.shards)
        stats = right_side(p, groups, gath, image, part, diag, rhs)
        to_lines(
            p, lambda b: jnp.concatenate([rhs[0, b], rhs[1, b]], axis=0), z_inv, chunk_a, False
        )
        stack_vector(p, rhs, stacked)
        push_c = over(chunk_a, held_c, 3, True)
        start_all(push_c, p.shards)
        held_c[me] = chunk_a[me]
        pay_stats(p, stats, pay_a)
        project(p, beta, stacked, acc, pay_a)
        push_pa = over(pay_a, sums_a, 4, False)
        start_all(push_pa, p.shards)
        sums_a[me] = pay_a[...]
        wait_all(push_c, p.shards)

        lines_to_rows(p, held_c, oh_t, mask, left, sq)
        rows_to_mixed(p, sq, y_inv, mixed)
        mixed_to_field(p, mixed, x_inv, x_fwd, pot_v_r, field_0, spectrum, stat)
        for b in range(p.bands):
            pay_b[b : b + 1, :] = everywhere(stat[b])
        push_pb = over(pay_b, sums_b, 5, False)
        start_all(push_pb, p.shards)
        sums_b[me] = pay_b[...]
        push_d = over(chunk_b, held_d, 6, True)
        spectrum_to_lines(p, spectrum, y_fwd, oh_t, rows_r, sq, left, chunk_b, held_d, push_d)
        wait_all(push_pa, p.shards)
        total = total_of(sums_a, p.shards)
        made, energy = couple(p, total, pair_r)
        build_coefs(p, made, coefs)
        back_project(p, beta, coefs, res)
        wait_all(push_pb, p.shards)
        planes = total_of(sums_b, p.shards)
        norm0, alpha0 = [], []
        for b in range(p.bands):
            norm0.append(total[2 * p.bands + b : 2 * p.bands + b + 1])
            curve = total[3 * p.bands + b : 3 * p.bands + b + 1] + planes[b : b + 1] + energy[b]
            alpha0.append(norm0[b] / curve)
        wait_all(push_d, p.shards)
        from_lines(p, held_d, joined, z_fwd, image)
        stats = fresh(p, rhs, image, res, diag, alpha0, res)
        to_lines(
            p, lambda b: jnp.concatenate([res[0, b], res[1, b]], axis=0), z_inv, chunk_a, False
        )
        stack_vector(p, res, stacked)
        push_e = over(chunk_a, held_e, 7, True)
        start_all(push_e, p.shards)
        held_e[me] = chunk_a[me]
        pay_stats(p, stats, pay_c)
        project(p, beta, stacked, acc, pay_c)
        push_pc = over(pay_c, sums_c, 8, False)
        start_all(push_pc, p.shards)
        sums_c[me] = pay_c[...]
        wait_all(push_e, p.shards)

        lines_to_rows(p, held_e, oh_t, mask, left, sq)
        rows_to_mixed(p, sq, y_inv, mixed)
        mixed_to_field(p, mixed, x_inv, None, pot_v_r, field_1, None, stat)
        for b in range(p.bands):
            pay_d[b : b + 1, :] = everywhere(stat[b])
        push_pd = over(pay_d, sums_d, 9, False)
        start_all(push_pd, p.shards)
        sums_d[me] = pay_d[...]
        wait_all(push_pc, p.shards)
        total = total_of(sums_c, p.shards)
        made, energy = couple(p, total, pair_r)
        wait_all(push_pd, p.shards)
        planes = total_of(sums_d, p.shards)
        keep, alpha1 = [], []
        for b in range(p.bands):
            norm1 = total[2 * p.bands + b : 2 * p.bands + b + 1]
            curve = total[3 * p.bands + b : 3 * p.bands + b + 1] + planes[b : b + 1] + energy[b]
            ratio = norm1 / norm0[b]
            alpha = norm1 / (curve - ratio * norm1 / alpha0[b])
            alpha1.append(alpha)
            keep.append(alpha0[b] + alpha * ratio)

        def plane(zp):
            made = 0.0
            for b in range(p.bands):
                at = aligned(b * p.planes + zp, p.grid)
                k2 = jnp.concatenate([keep[b], keep[b]], axis=1)
                a2 = jnp.concatenate([alpha1[b], alpha1[b]], axis=1)
                made = made + field_p[at, :] * (k2 * field_0[at, :] + a2 * field_1[at, :])
            return 4.0 * (made[:, :LANES] + made[:, LANES:])

        lane = lax.broadcasted_iota(jnp.int32, (1, LANES), 1)

        def put(at, value):
            for g in range(groups):
                dens_send[g, at] = value[g * wide_y : (g + 1) * wide_y]

        if dense:

            def four(i, carry):
                last = plane(4 * i + 3)
                for k in range(3):
                    moved = pltpu.roll(last, p.grid - k * rest, 1)
                    put(3 * i + k, jnp.where(lane < p.grid, plane(4 * i + k), moved))
                return carry

            lax.fori_loop(0, p.planes // 4, four, 0)
        else:

            def single(i, carry):
                put(i, plane(i))
                return carry

            lax.fori_loop(0, p.planes, single, 0)

        push_z = pusher("band", groups, dens_send, dens_got, band_sends, band_recvs, 1, True)
        start_all(push_z, groups)
        dens_got[mine_band] = dens_send[mine_band]
        for b in range(p.bands):

            def answer(t, carry, b=b):
                z = aligned(t, 8)
                for lane_at in range(0, p.own, LANES):
                    cut = pl.ds(lane_at, LANES)
                    for c in range(2):
                        resp_r[c, b, z, cut] = (
                            keep[b] * rhs[c, b, z, cut] + alpha1[b] * res[c, b, z, cut]
                        )
                return carry

            lax.fori_loop(0, p.grid // 8, answer, 0)
        wait_all(push_z, groups)

        def summed(at):
            value = dens_got[0, at]
            for g in range(1, groups):
                value = value + dens_got[g, at]
            return value

        if dense:
            for i in range(p.planes // 4):
                last = jnp.zeros((wide_y, LANES), f32)
                for k in range(3):
                    value = summed(3 * i + k)
                    dens_r[4 * i + k] = value
                    moved = pltpu.roll(value, LANES - p.grid + k * rest, 1)
                    inside = (lane >= k * rest) & (lane < (k + 1) * rest)
                    last = jnp.where(inside, moved, last)
                dens_r[4 * i + 3] = last
        else:
            for at in range(p.planes):
                dens_r[at] = summed(at)

    small = (p.shards, payload, LANES)
    tiny = (p.shards, few, LANES)
    scratch = [
        pltpu.VMEM((p.wide, p.sticks), bf16),
        pltpu.VMEM((p.groups, 16, p.sticks), bf16),
        pltpu.VMEM((2, many_rows, p.sticks), bf16),
        pltpu.VMEM((p.tiles, many_rows, LANES), f32),
        pltpu.VMEM((2, cells, 2 * LANES), bf16),
        pltpu.VMEM((cells, 2 * LANES), f32),
        pltpu.VMEM((cells, 2 * LANES), f32),
        pltpu.VMEM((cells, 2 * LANES), f32),
        pltpu.VMEM((cells, 2 * LANES), f32),
        pltpu.VMEM(chunk, f32),
        pltpu.VMEM(chunk, f32),
        pltpu.VMEM(chunk, f32),
        pltpu.VMEM(chunk, f32),
        pltpu.VMEM(chunk, f32),
        pltpu.VMEM(chunk, f32),
        pltpu.VMEM(chunk, f32),
        pltpu.VMEM((groups,) + mine, bf16),
        pltpu.VMEM((p.shards * p.q, p.own), f32),
        pltpu.VMEM(mine, f32),
        pltpu.VMEM(mine, f32),
        pltpu.VMEM(mine, f32),
        pltpu.VMEM((p.bands, p.grid, p.own), f32),
        pltpu.VMEM((p.bands, 8, LANES), f32),
        pltpu.VMEM((inters, LANES), f32),
        pltpu.VMEM((p.shards, inters, LANES), f32),
        pltpu.VMEM((payload, LANES), f32),
        pltpu.VMEM(small, f32),
        pltpu.VMEM((few, LANES), f32),
        pltpu.VMEM(tiny, f32),
        pltpu.VMEM((payload, LANES), f32),
        pltpu.VMEM(small, f32),
        pltpu.VMEM((few, LANES), f32),
        pltpu.VMEM(tiny, f32),
        pltpu.VMEM((SLOTS, 2, JB, p.grid, p.own), f32),
        pltpu.VMEM((2, 2, p.count, p.grid, p.own), bf16),
        pltpu.VMEM((p.grid // TALL, 4 * p.bands * TALL, p.own), bf16),
        pltpu.VMEM((2, p.count, 8, 4 * p.bands * TALL), f32),
        pltpu.VMEM((2, 2 * p.bands * TALL, 2 * p.count * TALL), bf16),
        pltpu.VMEM((groups, thick, wide_y, LANES), f32),
        pltpu.VMEM((groups, thick, wide_y, LANES), f32),
        pltpu.SemaphoreType.DMA((SLOTS,)),
        pltpu.SemaphoreType.DMA((10, p.shards - 1)),
        pltpu.SemaphoreType.DMA((10, p.shards - 1)),
        pltpu.SemaphoreType.DMA((2, groups - 1)),
        pltpu.SemaphoreType.DMA((2, groups - 1)),
    ]
    return pl.pallas_call(
        kernel,
        out_shape=[spec_of(mine), spec_of((p.planes, wide_y, LANES))],
        in_specs=[VMEM] * 3
        + [pl.BlockSpec(memory_space=pl.ANY), VMEM, pl.BlockSpec(memory_space=pltpu.SMEM)]
        + [VMEM] * 7,
        out_specs=[VMEM] * 2,
        scratch_shapes=scratch,
        compiler_params=pltpu.CompilerParams(
            collective_id=0, has_side_effects=True, vmem_limit_bytes=67_043_328
        ),
        name="response",
    )(
        psi, pot_dv, pot_v, beta_hbm_array, rows_of, shift, pair,
        p.z_inv, p.z_fwd, p.y_inv, p.x_inv, p.x_fwd, p.y_fwd,
    )


def per_device(groups, shards, psi, vloc, dv, beta, dij, atom_type, stick_xy, band_shift):
    _, bands, grid, own = psi.shape
    planes = vloc.shape[0]
    sticks = stick_xy.shape[0]
    count = beta.shape[1]
    p = Plan(bands, grid, own, planes, shards, sticks, count)
    radius = grid // 3
    per_atom = dij.shape[1]

    fy = frequency(stick_xy // grid, grid)
    fx = frequency(stick_xy % grid, grid)
    ky, kx = fy + radius, fx + radius
    rows_of = jnp.stack(
        [(ky % PER) * p.side + kx, ky // PER, fy * fy + fx * fx] + [jnp.zeros_like(fy)] * 5
    )

    def widen(field):
        shaped = jnp.pad(field.reshape(planes, grid, grid), ((0, 0), (0, 0), (0, LANES - grid)))
        return shaped.reshape(planes * grid, LANES)

    index = jnp.arange(count, dtype=jnp.int32)
    kind = jnp.arange(dij.shape[0], dtype=jnp.int32)
    chosen = (atom_type[:, None] == kind[None, :]).astype(f32)
    selected = jnp.sum(chosen[:, :, None, None] * dij[None], axis=1).reshape(count, per_atom)
    pair = jnp.where(
        (index // per_atom)[:, None] == (index // per_atom)[None, :],
        jnp.tile(selected, (1, count // per_atom)),
        0.0,
    )
    response, density = program(
        p, groups, psi, widen(dv), widen(vloc), beta, rows_of, band_shift, pair
    )
    density = density[:, :, :grid].reshape(planes, grid * grid // groups)
    return (response, density)


def solution(mesh):
    placed = (
        P(None, "band", None, "ga"),
        P("ga", None),
        P("ga", None),
        P(None, None, None, "ga"),
        P(),
        P(),
        P(),
        P("band"),
    )
    groups, shards = mesh.shape["band"], mesh.shape["ga"]

    def body(*args):
        return per_device(groups, shards, *args)

    return jax.shard_map(
        body,
        mesh=mesh,
        in_specs=placed,
        out_specs=(P(None, "band", None, "ga"), P("ga", "band")),
        check_vma=False,
    )
```

```python
import math

import jax
import jax.numpy as jnp
import ml_dtypes
import numpy as np
from jax import lax
from jax.experimental import pallas as pl
from jax.experimental.pallas import tpu as pltpu
from jax.sharding import PartitionSpec as P

LANES = 128
PER = 4
f32, bf16 = jnp.float32, jnp.bfloat16
VMEM = pl.BlockSpec(memory_space=pltpu.VMEM)


def frequency(index, grid):
    return (index + grid // 2) % grid - grid // 2


def phase(rows, cols, grid, sign):
    angle = 2.0 * math.pi * ((rows[:, None] * cols[None, :]) % grid) / grid
    return np.exp(1j * sign * angle) / math.sqrt(grid)


def parts_of(table):
    return np.stack(
        [np.stack([table.real, -table.imag], 1), np.stack([table.imag, table.real], 1)]
    )


def halves_of(table):
    table = table.astype(np.float32)
    hi = table.astype(ml_dtypes.bfloat16)
    lo = (table - hi.astype(np.float32)).astype(ml_dtypes.bfloat16)
    return hi, lo


class Plan:
    def __init__(self, bands, grid, own, planes, shards, sticks, count):
        self.bands, self.grid, self.own, self.planes = bands, grid, own, planes
        self.shards, self.sticks, self.count = shards, sticks, count
        self.side = 2 * (grid // 3)
        self.q = 2 * planes
        self.rows = -(-bands * self.q // 16) * 16
        self.images = bands * planes
        self.groups = self.side // PER
        self.fold = LANES // self.side
        self.tiles = PER // self.fold
        self.wide = PER * self.side
        self.row_step = self.rows + 8
        self.group_step = self.groups + 8
        self.pot_step = grid + 8
        side, fold, tiles, groups = self.side, self.fold, self.tiles, self.groups
        cells = np.arange(grid)
        freqs = np.arange(side) - grid // 3
        z = parts_of(phase(cells, cells, grid, 1.0))
        z = z.reshape(2, shards, planes, 2 * grid).transpose(1, 0, 2, 3)
        self.z_inv = np.stack(halves_of(z.reshape(shards * self.q, 2 * grid)))
        z = parts_of(phase(cells, cells, grid, -1.0))
        z = z.reshape(2, grid, 2, shards, planes).transpose(0, 1, 3, 2, 4)
        self.z_fwd = np.stack(halves_of(z.reshape(2 * grid, shards * self.q)))
        y = parts_of(phase(cells, freqs, grid, 1.0))
        y = y.reshape(2, grid, 2, groups, tiles, fold).transpose(0, 5, 1, 2, 4, 3)
        hi, lo = halves_of(y.reshape(2 * fold * grid, 2 * tiles * groups))
        self.y_inv = np.concatenate([hi, hi, lo], axis=1)
        x = parts_of(phase(freqs, cells, grid, 1.0).T).transpose(2, 3, 0, 1)
        x = np.repeat(x[:, None], fold, axis=1)
        x = np.pad(x, ((0, 0),) * 4 + ((0, LANES - grid),))
        self.x_inv = np.stack(halves_of(x.reshape(2 * LANES, 2 * LANES)))
        x = parts_of(phase(cells, freqs, grid, -1.0).T).transpose(2, 3, 0, 1)
        x = np.repeat(x[:, :, :, None], fold, axis=3)
        x = np.pad(x, ((0, 0), (0, LANES - grid)) + ((0, 0),) * 3)
        self.x_fwd = np.stack(halves_of(x.reshape(2 * LANES, 2 * LANES)))
        y = parts_of(phase(freqs, cells, grid, -1.0))
        y = y.reshape(2, groups, tiles, fold, 2 * grid).transpose(0, 3, 2, 1, 4)
        self.y_fwd = np.stack(halves_of(y.reshape(2 * side, 2 * grid)))


def dot(a, b):
    return jnp.dot(a, b, preferred_element_type=f32)


def dot_t(a, b):
    return lax.dot_general(a, b, (((1,), (1,)), ((), ())), preferred_element_type=f32)


def split(x):
    hi = x.astype(bf16)
    return hi, (x - hi.astype(f32)).astype(bf16)


def split3(x):
    hi = x.astype(bf16)
    rest = x - hi.astype(f32)
    mid = rest.astype(bf16)
    return hi, mid, (rest - mid.astype(f32)).astype(bf16)


def aligned(at, size):
    return pl.ds(pl.multiple_of(at * size, math.gcd(size, LANES)), size)


def spec_of(shape, dtype=f32):
    return jax.ShapeDtypeStruct(shape, dtype)


def lines_to_rows(p, held, oh_t, mask, left, sq):
    def spread(src, carry):
        at = aligned(src, p.own)
        hi, lo = split(held[src])
        for g in range(p.groups):
            keep = mask[g, :, at]
            for r in range(0, p.rows, 16):
                to = pl.ds(g * p.rows + r, 16)
                left[0, to, at] = hi[r : r + 16] * keep
                left[1, to, at] = lo[r : r + 16] * keep
        return carry

    lax.fori_loop(0, p.shards, spread, 0)
    made = dot_t(left[0], oh_t[...]) + dot_t(left[1], oh_t[...])
    for g in range(p.groups):
        for t in range(p.tiles):
            sq[t, pl.ds(g * p.row_step, p.rows), :] = made[
                g * p.rows : (g + 1) * p.rows, t * LANES : (t + 1) * LANES
            ]


def rows_to_mixed(p, sq, y_inv, mixed):
    low = lax.broadcasted_iota(jnp.int32, (1, 2 * LANES), 1) % LANES < p.side

    def pair(at, carry):
        for b in range(p.bands):
            tiles = []
            for k in range(2):
                pieces = []
                for c in range(2):
                    n = b * p.q + c * p.planes + 2 * at + k
                    for t in range(p.tiles):
                        pieces.append(sq[t, pl.ds(n, p.groups, stride=p.row_step), :])
                tiles.append(jnp.concatenate(pieces, axis=0))
            hi, lo = split(jnp.concatenate(tiles, axis=1))
            out = dot(y_inv[...], jnp.concatenate([hi, lo, hi], axis=0))
            both = [
                jnp.where(
                    low,
                    out[2 * c * p.grid : (2 * c + 1) * p.grid],
                    out[(2 * c + 1) * p.grid : (2 * c + 2) * p.grid],
                )
                for c in range(2)
            ]
            for k in range(2):
                lane = slice(k * LANES, (k + 1) * LANES)
                hi, lo = split(jnp.concatenate([both[0][:, lane], both[1][:, lane]], axis=1))
                to = aligned(b * p.planes + 2 * at + k, p.grid)
                mixed[0, to, :] = hi
                mixed[1, to, :] = lo
        return carry

    lax.fori_loop(0, p.planes // 2, pair, 0)


def mixed_to_field(p, mixed, x_inv, x_fwd, pot, field, spectrum, stat):
    some = math.gcd(p.planes, 4)
    size = some * p.grid

    for b in range(p.bands):

        def block(at, total, b=b):
            to = aligned(b * (p.planes // some) + at, size)
            hi, lo = mixed[0, to, :], mixed[1, to, :]
            one = dot(hi, x_inv[0]) + dot(lo, x_inv[0]) + dot(hi, x_inv[1])
            field[to, :] = one
            wide = jnp.concatenate(
                [
                    pot[pl.ds(pl.multiple_of((at * some + k) * p.pot_step, 8), p.grid), :]
                    for k in range(some)
                ],
                axis=0,
            )
            used = one * jnp.concatenate([wide, wide], axis=1)
            if spectrum is not None:
                hi, lo = split(used)
                spectrum[to, :] = dot(hi, x_fwd[0]) + dot(lo, x_fwd[0]) + dot(hi, x_fwd[1])
            if stat is not None:
                made = jnp.sum((used * one).reshape(size // 8, 8, 2 * LANES), axis=0)
                total = total + made[:, :LANES] + made[:, LANES:]
            return total

        total = lax.fori_loop(0, p.planes // some, block, jnp.zeros((8, LANES), f32))
        if stat is not None:
            stat[b] = total


def spectrum_to_lines(p, spectrum, y_fwd, oh_t, rows_of, sq, left, lines, held, push):
    low = lax.broadcasted_iota(jnp.int32, (1, 2 * LANES), 1) % LANES < p.side
    half = p.side // p.fold

    def pair(at, carry):
        for b in range(p.bands):
            tiles = []
            for k in range(2):
                one = spectrum[aligned(b * p.planes + 2 * at + k, p.grid), :]
                tiles.append(jnp.concatenate([one[:, :LANES], one[:, LANES:]], axis=0))
            hi, lo = split(jnp.concatenate(tiles, axis=1))
            out = dot(y_fwd[0], hi) + dot(y_fwd[0], lo) + dot(y_fwd[1], hi)
            for c in range(2):
                from_ = c * p.side
                both = jnp.where(
                    low, out[from_ : from_ + half], out[from_ + half : from_ + 2 * half]
                )
                for k in range(2):
                    n = b * p.q + c * p.planes + 2 * at + k
                    to = pl.ds(pl.multiple_of(n * p.group_step, 8), p.groups)
                    for t in range(p.tiles):
                        sq[t, to, :] = both[
                            t * p.groups : (t + 1) * p.groups, k * LANES : (k + 1) * LANES
                        ]
        return carry

    lax.fori_loop(0, p.planes // 2, pair, 0)
    for g in range(p.groups):
        to = pl.ds(g * p.rows, p.rows)
        for t in range(p.tiles):
            hi, lo = split(sq[t, pl.ds(g, p.rows, stride=p.group_step), :])
            left[0, to, t * LANES : (t + 1) * LANES] = hi
            left[1, to, t * LANES : (t + 1) * LANES] = lo

    def gather(dest):
        at = aligned(dest, p.own)
        weights = oh_t[:, at]
        got = dot(left[0, :, : p.wide], weights) + dot(left[1, :, : p.wide], weights)
        kind = rows_of[0:1, at]
        kept = got[: p.rows]
        for g in range(1, p.groups):
            kept = jnp.where(kind == g, got[g * p.rows : (g + 1) * p.rows], kept)
        return kept

    me = lax.axis_index("ga")

    def each(hop, carry):
        dest = lax.rem(me + hop, p.shards)
        lines[dest] = gather(dest)

        @pl.when(hop > 1)
        def _():
            push(hop - 1).start()

        return carry

    lax.fori_loop(1, p.shards, each, 0)
    held[me] = gather(me)
    push(p.shards - 1).start()


def greet(axis, count):
    me = lax.axis_index(axis)
    barrier = pltpu.get_barrier_semaphore()
    for hop in range(1, count):
        peer = lax.rem(me + hop, count)
        pl.semaphore_signal(
            barrier, inc=1, device_id={axis: peer}, device_id_type=pl.DeviceIdType.MESH
        )


def pusher(axis, count, source, held, sends, recvs, which, scatter):
    me = lax.axis_index(axis)

    def push(hop):
        peer = lax.rem(me + hop, count)
        return pltpu.make_async_remote_copy(
            src_ref=source.at[peer] if scatter else source,
            dst_ref=held.at[me],
            send_sem=sends.at[which, hop - 1],
            recv_sem=recvs.at[which, hop - 1],
            device_id={axis: peer},
            device_id_type=pl.DeviceIdType.MESH,
        )

    return push


def start_all(push, count):
    for hop in range(1, count):
        push(hop).start()


def wait_all(push, count):
    for hop in range(1, count):
        push(hop).wait()


def total_of(sums, count):
    total = sums[0]
    for at in range(1, count):
        total = total + sums[at]
    return total


def to_lines(p, value_of, z_inv, chunks, exact):
    for b in range(p.bands):
        value = value_of(b)
        if exact:
            out = dot(z_inv[0], value) + dot(z_inv[1], value)
        else:
            hi, lo = split(value)
            out = dot(z_inv[0], hi) + dot(z_inv[0], lo) + dot(z_inv[1], hi)
        for d in range(p.shards):
            chunks[d, b * p.q : (b + 1) * p.q, :] = out[d * p.q : (d + 1) * p.q]


def from_lines(p, held, joined, z_fwd, result):
    for b in range(p.bands):
        for src in range(p.shards):
            joined[src * p.q : (src + 1) * p.q, :] = held[src, b * p.q : (b + 1) * p.q, :]
        hi, lo = split(joined[...])
        out = dot(z_fwd[0], hi) + dot(z_fwd[0], lo) + dot(z_fwd[1], hi)
        result[0, b] = out[: p.grid]
        result[1, b] = out[p.grid :]


TALL = 16
JB = 4
SLOTS = 4


def fetch(p, beta_hbm, staged, sem, at):
    return pltpu.make_async_copy(
        beta_hbm.at[:, pl.ds(at * JB, JB)], staged.at[at % SLOTS], sem.at[at % SLOTS]
    )


def convert(p, beta_hbm, staged, sem, beta, first, last):
    chunks = p.count // JB
    for at in range(first, last):
        fetch(p, beta_hbm, staged, sem, at).wait()
        slot = at % SLOTS

        def one(j, carry, at=at, slot=slot):
            for c in range(2):
                hi, lo = split(staged[slot, c, j])
                beta[0, c, at * JB + j] = hi
                beta[1, c, at * JB + j] = lo
            return carry

        lax.fori_loop(0, JB, one, 0)
        if at + SLOTS < chunks:
            fetch(p, beta_hbm, staged, sem, at + SLOTS).start()


def stack_vector(p, vec, stacked):
    for zt in range(p.grid // TALL):
        for b in range(p.bands):
            for c in range(2):
                hi, lo = split(vec[c, b, zt * TALL : (zt + 1) * TALL, :])
                at = (2 * b + c) * 2 * TALL
                stacked[zt, at : at + TALL, :] = hi
                stacked[zt, at + TALL : at + 2 * TALL, :] = lo


def project(p, beta, stacked, acc, pay):
    cols = 4 * p.bands * TALL
    keep = (
        lax.broadcasted_iota(jnp.int32, (TALL, cols), 0)
        == lax.broadcasted_iota(jnp.int32, (TALL, cols), 1) % TALL
    )
    some = p.count
    acc[...] = jnp.zeros_like(acc)

    def tile(at, carry):
        zt = at // (p.count // some)
        first = lax.rem(at, p.count // some) * some
        z = aligned(zt, TALL)
        right = stacked[zt]
        for c in range(2):
            hi = beta[0, c, pl.ds(first, some), z, :].reshape(some * TALL, p.own)
            lo = beta[1, c, pl.ds(first, some), z, :].reshape(some * TALL, p.own)
            out = (dot_t(hi, right) + dot_t(lo, right)).reshape(some, TALL, cols)
            out = jnp.where(keep[None], out, 0.0)
            acc[c, pl.ds(first, some)] += out[:, :8] + out[:, 8:]
        return carry

    lax.fori_loop(0, (p.grid // TALL) * (p.count // some), tile, 0)
    row = lax.broadcasted_iota(jnp.int32, (8, cols), 0)
    kind = lax.broadcasted_iota(jnp.int32, (8, cols), 1) // (2 * TALL)
    same = (row // 2 == kind // 2) & (row < 2 * p.bands)
    plain = jnp.where(same & (row % 2 == kind % 2), 1.0, 0.0).astype(bf16)
    cross = jnp.where(
        same & (row % 2 != kind % 2), jnp.where(row % 2 == 0, 1.0, -1.0), 0.0
    ).astype(bf16)
    made = 0.0
    for c, pick in ((0, plain), (1, cross)):
        for piece in split3(jnp.sum(acc[c], axis=1)):
            made = made + dot_t(pick, piece)
    pay[0 : 2 * p.bands, :] = made[: 2 * p.bands]


def couple(p, total, pair):
    hi, mid, lo = split3(total)
    p_hi, p_mid, p_lo = split3(pair[...])
    made = (
        dot_t(hi, p_hi) + dot_t(hi, p_mid) + dot_t(mid, p_hi)
        + dot_t(hi, p_lo) + dot_t(mid, p_mid) + dot_t(lo, p_hi)
    )
    product = jnp.sum(made * total, axis=1, keepdims=True)
    energy = [product[2 * b : 2 * b + 1] + product[2 * b + 1 : 2 * b + 2] for b in range(p.bands)]
    return made, energy


def build_coefs(p, made, coefs):
    blocks = p.count // TALL
    wide = TALL * TALL
    lane = lax.broadcasted_iota(jnp.int32, (TALL, wide), 1) // TALL
    source = lax.broadcasted_iota(jnp.int32, (TALL, wide), 0)
    repeat = jnp.where(lane == source, 1.0, 0.0).astype(bf16)
    keep = (
        lax.broadcasted_iota(jnp.int32, (TALL, wide), 0)
        == lax.broadcasted_iota(jnp.int32, (TALL, wide), 1) % TALL
    )
    hi, mid, lo = split3(made)
    for jb in range(blocks):
        cut = slice(jb * TALL, (jb + 1) * TALL)
        full = dot(hi[:, cut], repeat) + dot(mid[:, cut], repeat) + dot(lo[:, cut], repeat)
        for b in range(p.bands):
            re, im = full[2 * b : 2 * b + 1], full[2 * b + 1 : 2 * b + 2]
            for part, rows in ((0, (re, im)), (1, (-im, re))):
                for c in range(2):
                    one, two = split(jnp.where(keep, rows[c], 0.0))
                    to = slice((2 * b + c) * TALL, (2 * b + c + 1) * TALL)
                    at = slice((2 * jb + part) * wide, (2 * jb + part + 1) * wide)
                    coefs[0, to, at] = one
                    coefs[1, to, at] = two


def back_project(p, beta, coefs, back):
    blocks = p.count // TALL
    wide = TALL * TALL
    many = 2 * p.bands * TALL

    def tile(zt, carry):
        z = aligned(zt, TALL)
        made = jnp.zeros((many, p.own), f32)
        for jb in range(blocks):
            for part in range(2):
                js = slice(jb * TALL, (jb + 1) * TALL)
                hi = beta[0, part, js, z, :].reshape(wide, p.own)
                lo = beta[1, part, js, z, :].reshape(wide, p.own)
                at = slice((2 * jb + part) * wide, (2 * jb + part + 1) * wide)
                c_hi, c_lo = coefs[0, :, at], coefs[1, :, at]
                made = made + dot(c_hi, hi) + dot(c_lo, hi) + dot(c_hi, lo)
        for b in range(p.bands):
            for c in range(2):
                at = (2 * b + c) * TALL
                back[c, b, z, :] = made[at : at + TALL]
        return carry

    lax.fori_loop(0, p.grid // TALL, tile, 0)


TOP = 32767.0


def tables(p, xy_r, shift_r, rows_s, oh_t, mask, diag):
    radius = p.grid // 3

    def centred(k):
        return jnp.where(k < p.grid // 2, k, k - p.grid)

    def table(at, carry):
        cut = aligned(at, LANES)
        xy = xy_r[pl.ds(at, 1), :]
        y = ((xy.astype(f32) + 0.5) * (1.0 / p.grid)).astype(jnp.int32)
        fy, fx = centred(y), centred(xy - y * p.grid)
        group = (fy + radius) // PER
        slot = (fy + radius - group * PER) * p.side + fx + radius
        rows_s[0:1, cut] = group
        rows_s[1:2, cut] = fy * fy + fx * fx
        rows = lax.broadcasted_iota(jnp.int32, (p.wide, LANES), 0)
        oh_t[:, cut] = jnp.where(rows == slot, 1.0, 0.0).astype(bf16)
        kind = jnp.broadcast_to(group, (16, LANES))
        for g in range(p.groups):
            mask[g, :, cut] = jnp.where(kind == g, 1.0, 0.0).astype(bf16)
        return carry

    lax.fori_loop(0, p.sticks // LANES, table, 0)
    me = lax.axis_index("ga")
    flat = rows_s[1:2, pl.ds(pl.multiple_of(me * p.own, LANES), p.own)]
    z = centred(lax.broadcasted_iota(jnp.int32, (p.grid, p.own), 0))
    kinetic = (z * z + flat).astype(f32) * (4.0 / (p.grid * p.grid))
    for b in range(p.bands):
        diag[b] = kinetic + shift_r[b]


def widen(p, raw, pot):
    lane = lax.broadcasted_iota(jnp.int32, (1, LANES), 1)
    for y in range(p.grid):
        tile, off = divmod(y * p.grid, LANES)
        value = raw[:, tile * LANES : (tile + 1) * LANES]
        if off:
            value = pltpu.roll(value, LANES - off, 1)
        if off + p.grid > LANES:
            more = raw[:, (tile + 1) * LANES : (tile + 2) * LANES]
            value = jnp.where(lane < LANES - off, value, pltpu.roll(more, LANES - off, 1))
        pot[pl.ds(y, p.planes, stride=p.pot_step), :] = value


def narrow(p, wide_y, rows, out):
    lane = lax.broadcasted_iota(jnp.int32, (1, LANES), 1)
    made = None
    for y in range(wide_y):
        tile, off = divmod(y * p.grid, LANES)
        value = rows[pl.ds(y, p.planes, stride=wide_y), :]
        if off:
            value = pltpu.roll(value, off, 1)
        made = value if off == 0 else jnp.where(lane < off, made, value)
        if off + p.grid >= LANES:
            out[:, tile * LANES : (tile + 1) * LANES] = made
            made = value
    if wide_y * p.grid % LANES:
        tile = wide_y * p.grid // LANES
        out[:, tile * LANES :] = made[:, : wide_y * p.grid - tile * LANES]


def build_pair(p, dij_r, type_r, pair):
    kinds, per, _ = dij_r.shape
    shape = (8, p.count)
    row = lax.broadcasted_iota(jnp.int32, shape, 0)
    col = lax.broadcasted_iota(jnp.int32, shape, 1)
    for first in range(0, p.count, 8):
        kind = jnp.zeros(shape, jnp.int32)
        for a in range(first // per, (first + 8) // per):
            kind = jnp.where((row + first) // per == a, type_r[a], kind)
        value = jnp.zeros(shape, f32)
        for t in range(kinds):
            for i in range(per):
                here = (kind == t) & (row % per == i)
                for k in range(per):
                    value = jnp.where(here & (col % per == k), dij_r[t, i, k], value)
        value = jnp.where((row + first) // per == col // per, value, 0.0)
        pair[pl.ds(first, 8), :] = value


def intersect(p, groups, gath, image, part):
    many = groups * p.bands
    inv_norm = 1.0 / (2.0 * p.grid * p.sticks)
    for n in range(p.bands):

        def overlap(t, acc, n=n):
            z = aligned(t, TALL)
            acc = list(acc)
            for lane in range(0, p.own, LANES):
                cut = pl.ds(lane, LANES)
                i_re, i_im = image[0, n, z, cut], image[1, n, z, cut]
                for m in range(many):
                    p_re = gath[m // p.bands, 0, m % p.bands, z, cut].astype(f32)
                    p_im = gath[m // p.bands, 1, m % p.bands, z, cut].astype(f32)
                    re = p_re * i_re + p_im * i_im
                    im = p_re * i_im - p_im * i_re
                    acc[2 * m] = acc[2 * m] + (re[:8] + re[8:])
                    acc[2 * m + 1] = acc[2 * m + 1] + (im[:8] + im[8:])
            return tuple(acc)

        zero = jnp.zeros((8, LANES), f32)
        acc = lax.fori_loop(0, p.grid // TALL, overlap, (zero,) * (2 * many))
        for m in range(2 * many):
            part[pl.ds(n * 2 * many + m, 1), :] = jnp.sum(acc[m], axis=0, keepdims=True)
    part[...] = jnp.broadcast_to(
        jnp.sum(part[...], axis=1, keepdims=True) * inv_norm, part.shape
    )


def right_side(p, groups, gath, image, inter, diag, rhs):
    many = groups * p.bands
    stats = []
    for n in range(p.bands):

        def right(t, acc, n=n):
            z = aligned(t, TALL)
            norm, curve = acc
            for lane in range(0, p.own, LANES):
                cut = pl.ds(lane, LANES)
                re, im = -image[0, n, z, cut], -image[1, n, z, cut]
                for m in range(many):
                    p_re = gath[m // p.bands, 0, m % p.bands, z, cut].astype(f32)
                    p_im = gath[m // p.bands, 1, m % p.bands, z, cut].astype(f32)
                    row = n * 2 * many + 2 * m
                    c_re = inter[row : row + 1, :]
                    c_im = inter[row + 1 : row + 2, :]
                    re = re + (c_re * p_re - c_im * p_im)
                    im = im + (c_im * p_re + c_re * p_im)
                rhs[0, n, z, cut] = re
                rhs[1, n, z, cut] = im
                square = re * re + im * im
                norm = norm + square
                curve = curve + square * diag[n, z, cut]
            return norm, curve

        zero = jnp.zeros((TALL, LANES), f32)
        norm, curve = lax.fori_loop(0, p.grid // TALL, right, (zero, zero))
        stats.append((norm, curve))
    return stats


def fresh(p, rhs, image, back, diag, alpha, res):
    stats = []
    for b in range(p.bands):

        def one(t, acc, b=b):
            z = aligned(t, 8)
            norm, curve = acc
            for lane in range(0, p.own, LANES):
                cut = pl.ds(lane, LANES)
                scale = diag[b, z, cut]
                square = 0.0
                for c in range(2):
                    r = rhs[c, b, z, cut]
                    made = scale * r + image[c, b, z, cut] + back[c, b, z, cut]
                    new = r - alpha[b] * made
                    res[c, b, z, cut] = new
                    square = square + new * new
                norm = norm + square
                curve = curve + square * scale
            return norm, curve

        zero = jnp.zeros((8, LANES), f32)
        stats.append(lax.fori_loop(0, p.grid // 8, one, (zero, zero)))
    return stats


def answers(p, keep, alpha, rhs, res, out):
    for b in range(p.bands):

        def answer(t, carry, b=b):
            z = aligned(t, 8)
            for lane_at in range(0, p.own, LANES):
                cut = pl.ds(lane_at, LANES)
                for c in range(2):
                    out[c, b, z, cut] = keep[b] * rhs[c, b, z, cut] + alpha[b] * res[c, b, z, cut]
            return carry

        lax.fori_loop(0, p.grid // 8, answer, 0)


def settle(*arrays):
    def kernel(*refs):
        for source, target in zip(refs[: len(arrays)], refs[len(arrays) :]):
            target[...] = source[...]

    return pl.pallas_call(
        kernel,
        out_shape=[spec_of(x.shape) for x in arrays],
        in_specs=[VMEM] * len(arrays),
        out_specs=[VMEM] * len(arrays),
        name="settle",
    )(*arrays)


def everywhere(x):
    x = jnp.sum(x, axis=0, keepdims=True)
    return jnp.broadcast_to(jnp.sum(x, axis=1, keepdims=True), x.shape)


def pay_stats(p, stats, pay):
    for b in range(p.bands):
        at = 2 * p.bands + b
        pay[at : at + 1, :] = everywhere(stats[b][0])
        at = 3 * p.bands + b
        pay[at : at + 1, :] = everywhere(stats[b][1])


def program(p, groups, psi, dv, vloc, beta_array, xy, shift, dij, atom_type):
    payload = -(-4 * p.bands // 8) * 8
    few = -(-p.bands // 8) * 8
    many = groups * p.bands
    inters = p.bands * many * 2
    wide_y = p.grid // groups
    dense = p.planes % 4 == 0 and LANES - p.grid == p.grid // 3
    thick = p.planes * 3 // 4 if dense else p.planes
    rest = LANES - p.grid
    coded = dense and wide_y % 8 == 0
    dense_rows = -(-thick * wide_y // 16) * 16
    chunk = (p.shards, p.rows, p.own)
    mine = (2, p.bands, p.grid, p.own)
    cells = p.images * p.grid
    many_rows = p.groups * p.rows
    n_chunks = p.count // JB

    def kernel(
        psi_r, dv_r, vloc_r, beta_hbm, xy_r, shift_r, dij_r, type_r,
        z_inv, z_fwd, y_inv, x_inv, x_fwd, y_fwd,
        resp_o, dens_r,
        rows_s, pot_dv, pot_v, pair, oh_t, mask, left, sq, mixed, spectrum, field_p, field_0, field_1,
        chunk_a, chunk_b, held_a, held_b, held_c, held_d, held_e,
        gath, joined, image, rhs, res, diag, stat,
        part, sums_i, pay_a, sums_a, pay_b, sums_b, pay_c, sums_c, pay_d, sums_d,
        staged, beta, stacked, acc, coefs,
        dens_f, dens_q, dens_send, dens_got, scale_send, scale_got, dens_sum,
        beta_sem, sends, recvs, band_sends, band_recvs, out_sem,
    ):
        me = lax.axis_index("ga")
        mine_band = lax.axis_index("band")

        def over(source, held, which, scatter):
            return pusher("ga", p.shards, source, held, sends, recvs, which, scatter)

        greet("ga", p.shards)
        greet("band", groups)
        for at in range(SLOTS):
            fetch(p, beta_hbm, staged, beta_sem, at).start()
        to_lines(
            p, lambda b: jnp.concatenate([psi_r[0, b], psi_r[1, b]], axis=0), z_inv, chunk_a, True
        )
        tables(p, xy_r, shift_r, rows_s, oh_t, mask, diag)
        widen(p, dv_r, pot_dv)
        pl.semaphore_wait(pltpu.get_barrier_semaphore(), p.shards + groups - 2)
        push_a = over(chunk_a, held_a, 0, True)
        start_all(push_a, p.shards)
        push_psi = pusher("band", groups, psi_r, gath, band_sends, band_recvs, 0, False)
        start_all(push_psi, groups)
        held_a[me] = chunk_a[me]
        gath[mine_band] = psi_r[...]

        early, middle = n_chunks * 5 // 8, n_chunks * 13 // 16
        convert(p, beta_hbm, staged, beta_sem, beta, 0, early)
        wait_all(push_a, p.shards)

        lines_to_rows(p, held_a, oh_t, mask, left, sq)
        rows_to_mixed(p, sq, y_inv, mixed)
        mixed_to_field(p, mixed, x_inv, x_fwd, pot_dv, field_p, spectrum, None)
        push_b = over(chunk_b, held_b, 1, True)
        spectrum_to_lines(p, spectrum, y_fwd, oh_t, rows_s, sq, left, chunk_b, held_b, push_b)
        convert(p, beta_hbm, staged, beta_sem, beta, early, middle)
        widen(p, vloc_r, pot_v)
        build_pair(p, dij_r, type_r, pair)
        wait_all(push_psi, groups)
        wait_all(push_b, p.shards)

        from_lines(p, held_b, joined, z_fwd, image)
        intersect(p, groups, gath, image, part)
        push_i = over(part, sums_i, 2, False)
        start_all(push_i, p.shards)
        sums_i[me] = part[...]
        convert(p, beta_hbm, staged, beta_sem, beta, middle, n_chunks)
        wait_all(push_i, p.shards)
        part[...] = total_of(sums_i, p.shards)
        stats = right_side(p, groups, gath, image, part, diag, rhs)
        to_lines(
            p, lambda b: jnp.concatenate([rhs[0, b], rhs[1, b]], axis=0), z_inv, chunk_a, False
        )
        stack_vector(p, rhs, stacked)
        push_c = over(chunk_a, held_c, 3, True)
        start_all(push_c, p.shards)
        held_c[me] = chunk_a[me]
        pay_stats(p, stats, pay_a)
        project(p, beta, stacked, acc, pay_a)
        push_pa = over(pay_a, sums_a, 4, False)
        start_all(push_pa, p.shards)
        sums_a[me] = pay_a[...]
        wait_all(push_c, p.shards)

        lines_to_rows(p, held_c, oh_t, mask, left, sq)
        rows_to_mixed(p, sq, y_inv, mixed)
        mixed_to_field(p, mixed, x_inv, x_fwd, pot_v, field_0, spectrum, stat)
        for b in range(p.bands):
            pay_b[b : b + 1, :] = everywhere(stat[b])
        push_pb = over(pay_b, sums_b, 5, False)
        start_all(push_pb, p.shards)
        sums_b[me] = pay_b[...]
        push_d = over(chunk_b, held_d, 6, True)
        spectrum_to_lines(p, spectrum, y_fwd, oh_t, rows_s, sq, left, chunk_b, held_d, push_d)
        wait_all(push_pa, p.shards)
        total = total_of(sums_a, p.shards)
        made, energy = couple(p, total, pair)
        build_coefs(p, made, coefs)
        back_project(p, beta, coefs, res)
        wait_all(push_pb, p.shards)
        planes = total_of(sums_b, p.shards)
        norm0, alpha0 = [], []
        for b in range(p.bands):
            norm0.append(total[2 * p.bands + b : 2 * p.bands + b + 1])
            curve = total[3 * p.bands + b : 3 * p.bands + b + 1] + planes[b : b + 1] + energy[b]
            alpha0.append(norm0[b] / curve)
        wait_all(push_d, p.shards)
        from_lines(p, held_d, joined, z_fwd, image)
        stats = fresh(p, rhs, image, res, diag, alpha0, res)
        to_lines(
            p, lambda b: jnp.concatenate([res[0, b], res[1, b]], axis=0), z_inv, chunk_a, False
        )
        stack_vector(p, res, stacked)
        push_e = over(chunk_a, held_e, 7, True)
        start_all(push_e, p.shards)
        held_e[me] = chunk_a[me]
        pay_stats(p, stats, pay_c)
        project(p, beta, stacked, acc, pay_c)
        push_pc = over(pay_c, sums_c, 8, False)
        start_all(push_pc, p.shards)
        sums_c[me] = pay_c[...]
        wait_all(push_e, p.shards)

        lines_to_rows(p, held_e, oh_t, mask, left, sq)
        rows_to_mixed(p, sq, y_inv, mixed)
        mixed_to_field(p, mixed, x_inv, None, pot_v, field_1, None, stat)
        for b in range(p.bands):
            pay_d[b : b + 1, :] = everywhere(stat[b])
        push_pd = over(pay_d, sums_d, 9, False)
        start_all(push_pd, p.shards)
        sums_d[me] = pay_d[...]
        wait_all(push_pc, p.shards)
        total = total_of(sums_c, p.shards)
        made, energy = couple(p, total, pair)
        wait_all(push_pd, p.shards)
        planes = total_of(sums_d, p.shards)
        keep, alpha1 = [], []
        for b in range(p.bands):
            norm1 = total[2 * p.bands + b : 2 * p.bands + b + 1]
            curve = total[3 * p.bands + b : 3 * p.bands + b + 1] + planes[b : b + 1] + energy[b]
            ratio = norm1 / norm0[b]
            alpha = norm1 / (curve - ratio * norm1 / alpha0[b])
            alpha1.append(alpha)
            keep.append(alpha0[b] + alpha * ratio)

        def plane(zp):
            made = 0.0
            for b in range(p.bands):
                at = aligned(b * p.planes + zp, p.grid)
                k2 = jnp.concatenate([keep[b], keep[b]], axis=1)
                a2 = jnp.concatenate([alpha1[b], alpha1[b]], axis=1)
                made = made + field_p[at, :] * (k2 * field_0[at, :] + a2 * field_1[at, :])
            return 4.0 * (made[:, :LANES] + made[:, LANES:])

        lane = lax.broadcasted_iota(jnp.int32, (1, LANES), 1)
        if dense:

            def four(i, carry):
                last = plane(4 * i + 3)
                for k in range(3):
                    moved = pltpu.roll(last, p.grid - k * rest, 1)
                    dens_f[3 * i + k] = jnp.where(lane < p.grid, plane(4 * i + k), moved)
                return carry

            lax.fori_loop(0, p.planes // 4, four, 0)
        else:

            def single(i, carry):
                dens_f[i] = plane(i)
                return carry

            lax.fori_loop(0, p.planes, single, 0)

        if coded:
            for g in range(groups):
                for at in range(thick):
                    value = dens_f[at, g * wide_y : (g + 1) * wide_y, :]
                    top = jnp.max(jnp.abs(value), axis=0, keepdims=True)
                    up = jnp.where(top > 1e-30, TOP / top, 0.0)
                    dens_q[at * wide_y : (at + 1) * wide_y, :] = jnp.round(value * up)
                    scale_send[g, at : at + 1, :] = top * (1.0 / TOP)
                dens_send[g] = dens_q[...].astype(jnp.int16)
        else:
            for g in range(groups):
                for at in range(thick):
                    to = pl.ds(at * wide_y, wide_y)
                    dens_send[g, to, :] = dens_f[at, g * wide_y : (g + 1) * wide_y, :]

        push_z = pusher("band", groups, dens_send, dens_got, band_sends, band_recvs, 1, True)
        start_all(push_z, groups)
        answers(p, keep, alpha1, rhs, res, image)
        resp_copy = pltpu.make_async_copy(image, resp_o, out_sem.at[0])
        if coded:
            push_s = pusher("band", groups, scale_send, scale_got, band_sends, band_recvs, 2, True)
            start_all(push_s, groups)
        resp_copy.start()
        if coded:
            wait_all(push_s, groups)
        wait_all(push_z, groups)
        if coded:
            base = pl.ds(pl.multiple_of(mine_band * wide_y, 8), wide_y)
            total = [dens_f[at, base, :] for at in range(thick)]
            for hop in range(1, groups):
                src = lax.rem(mine_band + hop, groups)
                dens_q[...] = dens_got[src].astype(f32)
                for at in range(thick):
                    total[at] = total[at] + (
                        dens_q[at * wide_y : (at + 1) * wide_y, :] * scale_got[src, at : at + 1, :]
                    )
        else:
            dens_got[mine_band] = dens_send[mine_band]
            total = []
            for at in range(thick):
                to = pl.ds(at * wide_y, wide_y)
                value = dens_got[0, to, :]
                for g in range(1, groups):
                    value = value + dens_got[g, to, :]
                total.append(value)
        if dense:
            for i in range(p.planes // 4):
                last = jnp.zeros((wide_y, LANES), f32)
                for k in range(3):
                    value = total[3 * i + k]
                    dens_sum[pl.ds((4 * i + k) * wide_y, wide_y), :] = value
                    moved = pltpu.roll(value, LANES - p.grid + k * rest, 1)
                    inside = (lane >= k * rest) & (lane < (k + 1) * rest)
                    last = jnp.where(inside, moved, last)
                dens_sum[pl.ds((4 * i + 3) * wide_y, wide_y), :] = last
        else:
            for at in range(p.planes):
                dens_sum[pl.ds(at * wide_y, wide_y), :] = total[at]
        narrow(p, wide_y, dens_sum, dens_r)
        resp_copy.wait()

    small = (p.shards, payload, LANES)
    tiny = (p.shards, few, LANES)
    scratch = [
        pltpu.VMEM((8, p.sticks), jnp.int32),
        pltpu.VMEM((p.planes * p.pot_step, LANES), f32),
        pltpu.VMEM((p.planes * p.pot_step, LANES), f32),
        pltpu.VMEM((p.count, p.count), f32),
        pltpu.VMEM((p.wide, p.sticks), bf16),
        pltpu.VMEM((p.groups, 16, p.sticks), bf16),
        pltpu.VMEM((2, many_rows, p.sticks), bf16),
        pltpu.VMEM(
            (p.tiles, max(p.groups * p.row_step, p.rows * p.group_step), LANES), f32
        ),
        pltpu.VMEM((2, cells, 2 * LANES), bf16),
        pltpu.VMEM((cells, 2 * LANES), f32),
        pltpu.VMEM((cells, 2 * LANES), f32),
        pltpu.VMEM((cells, 2 * LANES), f32),
        pltpu.VMEM((cells, 2 * LANES), f32),
        pltpu.VMEM(chunk, f32),
        pltpu.VMEM(chunk, f32),
        pltpu.VMEM(chunk, f32),
        pltpu.VMEM(chunk, f32),
        pltpu.VMEM(chunk, f32),
        pltpu.VMEM(chunk, f32),
        pltpu.VMEM(chunk, f32),
        pltpu.VMEM((groups,) + mine, bf16),
        pltpu.VMEM((p.shards * p.q, p.own), f32),
        pltpu.VMEM(mine, f32),
        pltpu.VMEM(mine, f32),
        pltpu.VMEM(mine, f32),
        pltpu.VMEM((p.bands, p.grid, p.own), f32),
        pltpu.VMEM((p.bands, 8, LANES), f32),
        pltpu.VMEM((inters, LANES), f32),
        pltpu.VMEM((p.shards, inters, LANES), f32),
        pltpu.VMEM((payload, LANES), f32),
        pltpu.VMEM(small, f32),
        pltpu.VMEM((few, LANES), f32),
        pltpu.VMEM(tiny, f32),
        pltpu.VMEM((payload, LANES), f32),
        pltpu.VMEM(small, f32),
        pltpu.VMEM((few, LANES), f32),
        pltpu.VMEM(tiny, f32),
        pltpu.VMEM((SLOTS, 2, JB, p.grid, p.own), f32),
        pltpu.VMEM((2, 2, p.count, p.grid, p.own), bf16),
        pltpu.VMEM((p.grid // TALL, 4 * p.bands * TALL, p.own), bf16),
        pltpu.VMEM((2, p.count, 8, 4 * p.bands * TALL), f32),
        pltpu.VMEM((2, 2 * p.bands * TALL, 2 * p.count * TALL), bf16),
        pltpu.VMEM((thick, p.grid, LANES), f32),
        pltpu.VMEM((dense_rows, LANES), f32),
        pltpu.VMEM((groups, dense_rows, LANES), jnp.int16 if coded else f32),
        pltpu.VMEM((groups, dense_rows, LANES), jnp.int16 if coded else f32),
        pltpu.VMEM((groups, -(-thick // 8) * 8, LANES), f32),
        pltpu.VMEM((groups, -(-thick // 8) * 8, LANES), f32),
        pltpu.VMEM((p.planes * wide_y, LANES), f32),
        pltpu.SemaphoreType.DMA((SLOTS,)),
        pltpu.SemaphoreType.DMA((10, p.shards - 1)),
        pltpu.SemaphoreType.DMA((10, p.shards - 1)),
        pltpu.SemaphoreType.DMA((3, groups - 1)),
        pltpu.SemaphoreType.DMA((3, groups - 1)),
        pltpu.SemaphoreType.DMA((1,)),
    ]
    hbm = pl.BlockSpec(memory_space=pl.ANY)
    smem = pl.BlockSpec(memory_space=pltpu.SMEM)
    return pl.pallas_call(
        kernel,
        out_shape=[
            spec_of(mine), spec_of((p.planes, wide_y * p.grid)),
        ],
        in_specs=[VMEM] * 3 + [hbm, VMEM] + [smem] * 3 + [VMEM] * 6,
        out_specs=[hbm, VMEM],
        scratch_shapes=scratch,
        compiler_params=pltpu.CompilerParams(
            collective_id=0, has_side_effects=True, vmem_limit_bytes=67_043_328
        ),
        name="response",
    )(
        psi, dv, vloc, beta_array, xy, shift, dij, atom_type,
        p.z_inv, p.z_fwd, p.y_inv, p.x_inv, p.x_fwd, p.y_fwd,
    )


def per_device(groups, shards, psi, vloc, dv, beta, dij, atom_type, stick_xy, band_shift):
    _, bands, grid, own = psi.shape
    planes = vloc.shape[0]
    sticks = stick_xy.shape[0]
    count = beta.shape[1]
    p = Plan(bands, grid, own, planes, shards, sticks, count)
    xy = stick_xy.reshape(sticks // LANES, LANES)
    return settle(*program(p, groups, psi, dv, vloc, beta, xy, band_shift, dij, atom_type))


def solution(mesh):
    placed = (
        P(None, "band", None, "ga"),
        P("ga", None),
        P("ga", None),
        P(None, None, None, "ga"),
        P(),
        P(),
        P(),
        P("band"),
    )
    groups, shards = mesh.shape["band"], mesh.shape["ga"]

    def body(*args):
        return per_device(groups, shards, *args)

    return jax.shard_map(
        body,
        mesh=mesh,
        in_specs=placed,
        out_specs=(P(None, "band", None, "ga"), P("ga", "band")),
        check_vma=False,
    )
```

```python
import math

import jax
import jax.numpy as jnp
import ml_dtypes
import numpy as np
from jax import lax
from jax.experimental import pallas as pl
from jax.experimental.pallas import tpu as pltpu
from jax.sharding import PartitionSpec as P

LANES = 128
PER = 4
TALL = 16
f32, bf16 = jnp.float32, jnp.bfloat16
VMEM = pl.BlockSpec(memory_space=pltpu.VMEM)


def frequency(index, grid):
    return (index + grid // 2) % grid - grid // 2


def phase(rows, cols, grid, sign):
    angle = 2.0 * math.pi * ((rows[:, None] * cols[None, :]) % grid) / grid
    return np.exp(1j * sign * angle) / math.sqrt(grid)


def parts_of(table):
    return np.stack(
        [np.stack([table.real, -table.imag], 1), np.stack([table.imag, table.real], 1)]
    )


def halves_of(table):
    table = table.astype(np.float32)
    hi = table.astype(ml_dtypes.bfloat16)
    lo = (table - hi.astype(np.float32)).astype(ml_dtypes.bfloat16)
    return hi, lo


class Plan:
    def __init__(self, bands, grid, own, planes, shards, sticks, count):
        self.bands, self.grid, self.own, self.planes = bands, grid, own, planes
        self.shards, self.sticks, self.count = shards, sticks, count
        self.vector = count * 4 // 8 // TALL * TALL
        self.matrix = count - self.vector
        self.side = 2 * (grid // 3)
        self.q = 2 * planes
        self.rows = -(-bands * self.q // 16) * 16
        self.images = bands * planes
        self.groups = self.side // PER
        self.fold = LANES // self.side
        self.tiles = PER // self.fold
        self.wide = PER * self.side
        self.row_step = self.rows + 8
        self.group_step = self.groups + 8
        self.pot_step = grid + 8
        side, fold, tiles, groups = self.side, self.fold, self.tiles, self.groups
        cells = np.arange(grid)
        freqs = np.arange(side) - grid // 3
        z = parts_of(phase(cells, cells, grid, 1.0))
        z = z.reshape(2, shards, planes, 2 * grid).transpose(1, 0, 2, 3)
        self.z_inv = np.stack(halves_of(z.reshape(shards * self.q, 2 * grid)))
        z = parts_of(phase(cells, cells, grid, -1.0))
        z = z.reshape(2, grid, 2, shards, planes).transpose(0, 1, 3, 2, 4)
        self.z_fwd = np.stack(halves_of(z.reshape(2 * grid, shards * self.q)))
        y = parts_of(phase(cells, freqs, grid, 1.0))
        y = y.reshape(2, grid, 2, groups, tiles, fold).transpose(0, 5, 1, 2, 4, 3)
        hi, lo = halves_of(y.reshape(2 * fold * grid, 2 * tiles * groups))
        self.y_inv = np.concatenate([hi, hi, lo], axis=1)
        x = parts_of(phase(freqs, cells, grid, 1.0).T).transpose(2, 3, 0, 1)
        x = np.repeat(x[:, None], fold, axis=1)
        x = np.pad(x, ((0, 0),) * 4 + ((0, LANES - grid),))
        self.x_inv = np.stack(halves_of(x.reshape(2 * LANES, 2 * LANES)))
        x = parts_of(phase(cells, freqs, grid, -1.0).T).transpose(2, 3, 0, 1)
        x = np.repeat(x[:, :, :, None], fold, axis=3)
        x = np.pad(x, ((0, 0), (0, LANES - grid)) + ((0, 0),) * 3)
        self.x_fwd = np.stack(halves_of(x.reshape(2 * LANES, 2 * LANES)))
        y = parts_of(phase(freqs, cells, grid, -1.0))
        y = y.reshape(2, groups, tiles, fold, 2 * grid).transpose(0, 3, 2, 1, 4)
        self.y_fwd = np.stack(halves_of(y.reshape(2 * side, 2 * grid)))


def dot(a, b):
    return jnp.dot(a, b, preferred_element_type=f32)


def dot_t(a, b):
    return lax.dot_general(a, b, (((1,), (1,)), ((), ())), preferred_element_type=f32)


def split(x):
    hi = x.astype(bf16)
    return hi, (x - hi.astype(f32)).astype(bf16)


def split3(x):
    hi = x.astype(bf16)
    rest = x - hi.astype(f32)
    mid = rest.astype(bf16)
    return hi, mid, (rest - mid.astype(f32)).astype(bf16)


def aligned(at, size):
    return pl.ds(pl.multiple_of(at * size, math.gcd(size, LANES)), size)


def spec_of(shape, dtype=f32):
    return jax.ShapeDtypeStruct(shape, dtype)


def lines_to_rows(p, held, oh_t, mask, left, sq):
    def spread(src, carry):
        at = aligned(src, p.own)
        hi, lo = split(held[src])
        for g in range(p.groups):
            keep = mask[g, :, at]
            for r in range(0, p.rows, 16):
                to = pl.ds(g * p.rows + r, 16)
                left[0, to, at] = hi[r : r + 16] * keep
                left[1, to, at] = lo[r : r + 16] * keep
        return carry

    lax.fori_loop(0, p.shards, spread, 0)
    many = p.groups * p.rows
    made = dot_t(left[...].reshape(2 * many, p.sticks), oh_t[...])
    made = made[:many] + made[many:]
    for g in range(p.groups):
        for t in range(p.tiles):
            sq[t, pl.ds(g * p.row_step, p.rows), :] = made[
                g * p.rows : (g + 1) * p.rows, t * LANES : (t + 1) * LANES
            ]


def rows_to_mixed(p, sq, y_inv, mixed):
    low = lax.broadcasted_iota(jnp.int32, (1, 2 * LANES), 1) % LANES < p.side

    def pair(at, carry):
        for b in range(p.bands):
            tiles = []
            for k in range(2):
                pieces = []
                for c in range(2):
                    n = b * p.q + c * p.planes + 2 * at + k
                    for t in range(p.tiles):
                        pieces.append(sq[t, pl.ds(n, p.groups, stride=p.row_step), :])
                tiles.append(jnp.concatenate(pieces, axis=0))
            hi, lo = split(jnp.concatenate(tiles, axis=1))
            out = dot(y_inv[...], jnp.concatenate([hi, lo, hi], axis=0))
            both = [
                jnp.where(
                    low,
                    out[2 * c * p.grid : (2 * c + 1) * p.grid],
                    out[(2 * c + 1) * p.grid : (2 * c + 2) * p.grid],
                )
                for c in range(2)
            ]
            for k in range(2):
                lane = slice(k * LANES, (k + 1) * LANES)
                hi, lo = split(jnp.concatenate([both[0][:, lane], both[1][:, lane]], axis=1))
                to = aligned(b * p.planes + 2 * at + k, p.grid)
                mixed[0, to, :] = hi
                mixed[1, to, :] = lo
        return carry

    lax.fori_loop(0, p.planes // 2, pair, 0, unroll=3)


def mixed_to_field(p, mixed, x_inv, x_fwd, pot, field, spectrum, stat):
    size = p.planes * p.grid

    def block(b, carry):
        to = aligned(b, size)
        hi, lo = mixed[0, to, :], mixed[1, to, :]
        field[to, :] = dot(hi, x_inv[0]) + dot(lo, x_inv[0]) + dot(hi, x_inv[1])
        return carry

    lax.fori_loop(0, p.bands, block, 0)
    if stat is not None:
        stat[...] = jnp.zeros_like(stat)

    def scaled(at, carry):
        to = aligned(at, p.grid)
        one = field[to, :]
        rows = pl.ds(pl.multiple_of(lax.rem(at, p.planes) * p.pot_step, 8), p.grid)
        wide = pot[rows, :]
        used = one * jnp.concatenate([wide, wide], axis=1)
        if spectrum is not None:
            hi, lo = split(used)
            mixed[0, to, :] = hi
            mixed[1, to, :] = lo
        if stat is not None:
            made = jnp.sum((used * one).reshape(p.grid // 8, 8, 2 * LANES), axis=0)
            b = at // p.planes
            stat[b] = stat[b] + made[:, :LANES] + made[:, LANES:]
        return carry

    lax.fori_loop(0, p.images, scaled, 0)
    if spectrum is not None:

        def forth(b, carry):
            to = aligned(b, size)
            hi, lo = mixed[0, to, :], mixed[1, to, :]
            spectrum[to, :] = dot(hi, x_fwd[0]) + dot(lo, x_fwd[0]) + dot(hi, x_fwd[1])
            return carry

        lax.fori_loop(0, p.bands, forth, 0)


def spectrum_to_lines(p, spectrum, y_fwd, oh_t, rows_of, sq, left, lines, held, push):
    low = lax.broadcasted_iota(jnp.int32, (1, 2 * LANES), 1) % LANES < p.side
    half = p.side // p.fold

    def pair(at, carry):
        for b in range(p.bands):
            tiles = []
            for k in range(2):
                one = spectrum[aligned(b * p.planes + 2 * at + k, p.grid), :]
                tiles.append(jnp.concatenate([one[:, :LANES], one[:, LANES:]], axis=0))
            hi, lo = split(jnp.concatenate(tiles, axis=1))
            both = dot(y_fwd[...].reshape(4 * p.side, 2 * p.grid), hi)
            out = both[: 2 * p.side] + both[2 * p.side :] + dot(y_fwd[0], lo)
            for c in range(2):
                from_ = c * p.side
                both = jnp.where(
                    low, out[from_ : from_ + half], out[from_ + half : from_ + 2 * half]
                )
                for k in range(2):
                    n = b * p.q + c * p.planes + 2 * at + k
                    to = pl.ds(pl.multiple_of(n * p.group_step, 8), p.groups)
                    for t in range(p.tiles):
                        sq[t, to, :] = both[
                            t * p.groups : (t + 1) * p.groups, k * LANES : (k + 1) * LANES
                        ]
        return carry

    lax.fori_loop(0, p.planes // 2, pair, 0, unroll=3)
    for g in range(p.groups):
        to = pl.ds(g * p.rows, p.rows)
        for t in range(p.tiles):
            hi, lo = split(sq[t, pl.ds(g, p.rows, stride=p.group_step), :])
            left[0, to, t * LANES : (t + 1) * LANES] = hi
            left[1, to, t * LANES : (t + 1) * LANES] = lo

    def gather(dest):
        at = aligned(dest, p.own)
        weights = oh_t[:, at]
        got = dot(left[0, :, : p.wide], weights) + dot(left[1, :, : p.wide], weights)
        kind = rows_of[0:1, at]
        kept = got[: p.rows]
        for g in range(1, p.groups):
            kept = jnp.where(kind == g, got[g * p.rows : (g + 1) * p.rows], kept)
        return kept

    me = lax.axis_index("ga")

    def each(hop, carry):
        dest = lax.rem(me + hop, p.shards)
        lines[dest] = gather(dest)

        @pl.when(hop > 1)
        def _():
            push(hop - 1).start()

        return carry

    lax.fori_loop(1, p.shards, each, 0)
    held[me] = gather(me)
    push(p.shards - 1).start()


def greet(axis, count):
    me = lax.axis_index(axis)
    barrier = pltpu.get_barrier_semaphore()
    for hop in range(1, count):
        peer = lax.rem(me + hop, count)
        pl.semaphore_signal(
            barrier, inc=1, device_id={axis: peer}, device_id_type=pl.DeviceIdType.MESH
        )


def pusher(axis, count, source, held, sends, recvs, which, scatter):
    me = lax.axis_index(axis)

    def push(hop):
        peer = lax.rem(me + hop, count)
        return pltpu.make_async_remote_copy(
            src_ref=source.at[peer] if scatter else source,
            dst_ref=held.at[me],
            send_sem=sends.at[which, hop - 1],
            recv_sem=recvs.at[which, hop - 1],
            device_id={axis: peer},
            device_id_type=pl.DeviceIdType.MESH,
        )

    return push


def start_all(push, count):
    for hop in range(1, count):
        push(hop).start()


def wait_all(push, count):
    for hop in range(1, count):
        push(hop).wait()


def total_of(sums, count):
    total = sums[0]
    for at in range(1, count):
        total = total + sums[at]
    return total


def to_lines(p, value_of, z_inv, chunks, exact):
    for b in range(p.bands):
        value = value_of(b)
        if exact:
            out = dot(z_inv[0], value) + dot(z_inv[1], value)
        else:
            hi, lo = split(value)
            out = dot(z_inv[0], hi) + dot(z_inv[0], lo) + dot(z_inv[1], hi)
        for d in range(p.shards):
            chunks[d, b * p.q : (b + 1) * p.q, :] = out[d * p.q : (d + 1) * p.q]


def from_lines(p, held, joined, z_fwd, result):
    for b in range(p.bands):
        for src in range(p.shards):
            joined[src * p.q : (src + 1) * p.q, :] = held[src, b * p.q : (b + 1) * p.q, :]
        hi, lo = split(joined[...])
        out = dot(z_fwd[0], hi) + dot(z_fwd[0], lo) + dot(z_fwd[1], hi)
        result[0, b] = out[: p.grid]
        result[1, b] = out[p.grid :]


JB = 4
SLOTS = 4


def fetch(p, beta_hbm, staged, sem, at):
    return pltpu.make_async_copy(
        beta_hbm.at[:, pl.ds(at * JB, JB)], staged.at[at % SLOTS], sem.at[at % SLOTS]
    )


def convert(p, beta_hbm, staged, sem, beta, first, last):
    chunks = p.matrix // JB
    for at in range(first, last):
        fetch(p, beta_hbm, staged, sem, at).wait()
        slot = at % SLOTS

        def one(j, carry, at=at, slot=slot):
            for c in range(2):
                hi, lo = split(staged[slot, c, j])
                beta[0, c, at * JB + j] = hi
                beta[1, c, at * JB + j] = lo
            return carry

        lax.fori_loop(0, JB, one, 0)
        if at + SLOTS < chunks:
            fetch(p, beta_hbm, staged, sem, at + SLOTS).start()


def stack_vector(p, vec, stacked):
    for zt in range(p.grid // TALL):
        for b in range(p.bands):
            for c in range(2):
                hi, lo = split(vec[c, b, zt * TALL : (zt + 1) * TALL, :])
                at = (2 * b + c) * 2 * TALL
                stacked[zt, at : at + TALL, :] = hi
                stacked[zt, at + TALL : at + 2 * TALL, :] = lo


def project(p, beta, beta_f, vec, stacked, acc, acc_f, pay):
    cols = 4 * p.bands * TALL
    many = 2 * p.bands
    keep = (
        lax.broadcasted_iota(jnp.int32, (TALL, cols), 0)
        == lax.broadcasted_iota(jnp.int32, (TALL, cols), 1) % TALL
    )
    acc[...] = jnp.zeros_like(acc)
    acc_f[...] = jnp.zeros_like(acc_f)

    def tile(zt, carry):
        z = aligned(zt, TALL)
        right = stacked[zt]
        for c in range(2):
            hi = beta[0, c, :, z, :].reshape(p.matrix * TALL, p.own)
            lo = beta[1, c, :, z, :].reshape(p.matrix * TALL, p.own)
            out = (dot_t(hi, right) + dot_t(lo, right)).reshape(p.matrix, TALL, cols)
            out = jnp.where(keep[None], out, 0.0)
            acc[c] += out[:, :8] + out[:, 8:]
        for first in range(0, p.vector, 4):
            sums = [[acc_f[n, first + j] for n in range(many)] for j in range(4)]
            for part in range(TALL // 8):
                rows = pl.ds(pl.multiple_of(zt * TALL + part * 8, 8), 8)
                for lane in range(0, p.own, LANES):
                    cut = pl.ds(lane, LANES)
                    v_re = [vec[0, b, rows, cut] for b in range(p.bands)]
                    v_im = [vec[1, b, rows, cut] for b in range(p.bands)]
                    for j in range(4):
                        b_re = beta_f[0, first + j, rows, cut]
                        b_im = beta_f[1, first + j, rows, cut]
                        for b in range(p.bands):
                            sums[j][2 * b] = sums[j][2 * b] + (b_re * v_re[b] + b_im * v_im[b])
                            sums[j][2 * b + 1] = sums[j][2 * b + 1] + (
                                b_re * v_im[b] - b_im * v_re[b]
                            )
            for j in range(4):
                for n in range(many):
                    acc_f[n, first + j] = sums[j][n]
        return carry

    lax.fori_loop(0, p.grid // TALL, tile, 0)
    row = lax.broadcasted_iota(jnp.int32, (8, cols), 0)
    kind = lax.broadcasted_iota(jnp.int32, (8, cols), 1) // (2 * TALL)
    same = (row // 2 == kind // 2) & (row < many)
    plain = jnp.where(same & (row % 2 == kind % 2), 1.0, 0.0).astype(bf16)
    cross = jnp.where(
        same & (row % 2 != kind % 2), jnp.where(row % 2 == 0, 1.0, -1.0), 0.0
    ).astype(bf16)
    made = 0.0
    empty = jnp.zeros((p.vector, cols), f32)
    for c, pick in ((0, plain), (1, cross)):
        for piece in split3(jnp.concatenate([jnp.sum(acc[c], axis=1), empty], axis=0)):
            made = made + dot_t(pick, piece)
    empty = jnp.zeros((p.matrix, LANES), f32)
    for n in range(many):
        mine = jnp.where(lax.broadcasted_iota(jnp.int32, (8, LANES), 0) == n, 1.0, 0.0)
        for piece in split3(jnp.concatenate([empty, jnp.sum(acc_f[n], axis=1)], axis=0)):
            made = made + dot_t(mine.astype(bf16), piece)
    pay[0:many, :] = made[:many]


def couple(p, total, pair):
    hi, mid, lo = split3(total)
    p_hi, p_mid, p_lo = split3(pair[...])
    made = (
        dot_t(hi, p_hi) + dot_t(hi, p_mid) + dot_t(mid, p_hi)
        + dot_t(hi, p_lo) + dot_t(mid, p_mid) + dot_t(lo, p_hi)
    )
    product = jnp.sum(made * total, axis=1, keepdims=True)
    energy = [product[2 * b : 2 * b + 1] + product[2 * b + 1 : 2 * b + 2] for b in range(p.bands)]
    return made, energy


def build_coefs(p, made, coefs, coefs_f):
    blocks = p.matrix // TALL
    wide = TALL * TALL
    lane = lax.broadcasted_iota(jnp.int32, (TALL, wide), 1) // TALL
    source = lax.broadcasted_iota(jnp.int32, (TALL, wide), 0)
    repeat = jnp.where(lane == source, 1.0, 0.0).astype(bf16)
    keep = (
        lax.broadcasted_iota(jnp.int32, (TALL, wide), 0)
        == lax.broadcasted_iota(jnp.int32, (TALL, wide), 1) % TALL
    )
    ones = jnp.ones((p.count, LANES), bf16)
    chosen = (
        lax.broadcasted_iota(jnp.int32, (p.vector, p.count), 0) + p.matrix
        == lax.broadcasted_iota(jnp.int32, (p.vector, p.count), 1)
    )
    for n in range(2 * p.bands):
        hi, mid, lo = split3(jnp.where(chosen, made[n : n + 1], 0.0))
        coefs_f[n] = dot(hi, ones) + dot(mid, ones) + dot(lo, ones)
    hi, mid, lo = split3(made)
    for jb in range(blocks):
        cut = slice(jb * TALL, (jb + 1) * TALL)
        full = dot(hi[:, cut], repeat) + dot(mid[:, cut], repeat) + dot(lo[:, cut], repeat)
        for b in range(p.bands):
            re, im = full[2 * b : 2 * b + 1], full[2 * b + 1 : 2 * b + 2]
            for part, rows in ((0, (re, im)), (1, (-im, re))):
                for c in range(2):
                    one, two = split(jnp.where(keep, rows[c], 0.0))
                    to = slice((2 * b + c) * TALL, (2 * b + c + 1) * TALL)
                    at = slice((2 * jb + part) * wide, (2 * jb + part + 1) * wide)
                    coefs[0, to, at] = one
                    coefs[1, to, at] = two


def back_project(p, beta, beta_f, coefs, coefs_f, back):
    blocks = p.matrix // TALL
    wide = TALL * TALL
    many = 2 * p.bands * TALL

    def tile(zt, carry):
        z = aligned(zt, TALL)
        made = jnp.zeros((many, p.own), f32)
        places = [
            (part, pl.ds(pl.multiple_of(zt * TALL + part * 8, 8), 8), lane)
            for part in range(TALL // 8)
            for lane in range(0, p.own, LANES)
        ]
        sums = [[0.0] * (2 * p.bands) for _ in places]
        for jb in range(blocks):
            for part in range(2):
                js = slice(jb * TALL, (jb + 1) * TALL)
                hi = beta[0, part, js, z, :].reshape(wide, p.own)
                lo = beta[1, part, js, z, :].reshape(wide, p.own)
                at = slice((2 * jb + part) * wide, (2 * jb + part + 1) * wide)
                both = dot(coefs[:, :, at].reshape(2 * many, wide), hi)
                made = made + both[:many] + both[many:] + dot(coefs[0, :, at], lo)
            for j in range(p.vector * jb // blocks, p.vector * (jb + 1) // blocks):
                rows_c = [coefs_f[n, j : j + 1, :] for n in range(2 * p.bands)]
                for mine, (part, rows, lane) in zip(sums, places):
                    b_re = beta_f[0, j, rows, pl.ds(lane, LANES)]
                    b_im = beta_f[1, j, rows, pl.ds(lane, LANES)]
                    for b in range(p.bands):
                        c_re, c_im = rows_c[2 * b], rows_c[2 * b + 1]
                        mine[2 * b] = mine[2 * b] + (b_re * c_re - b_im * c_im)
                        mine[2 * b + 1] = mine[2 * b + 1] + (b_re * c_im + b_im * c_re)
        for mine, (part, rows, lane) in zip(sums, places):
            for b in range(p.bands):
                for c in range(2):
                    at = (2 * b + c) * TALL + part * 8
                    back[c, b, rows, pl.ds(lane, LANES)] = (
                        made[at : at + 8, lane : lane + LANES] + mine[2 * b + c]
                    )
        return carry

    lax.fori_loop(0, p.grid // TALL, tile, 0)


TOP = 32767.0


def tables(p, xy_r, shift_r, rows_s, oh_t, mask, diag):
    radius = p.grid // 3

    def centred(k):
        return jnp.where(k < p.grid // 2, k, k - p.grid)

    def table(at, carry):
        cut = aligned(at, LANES)
        xy = xy_r[pl.ds(at, 1), :]
        y = ((xy.astype(f32) + 0.5) * (1.0 / p.grid)).astype(jnp.int32)
        fy, fx = centred(y), centred(xy - y * p.grid)
        group = (fy + radius) // PER
        slot = (fy + radius - group * PER) * p.side + fx + radius
        rows_s[0:1, cut] = group
        rows_s[1:2, cut] = fy * fy + fx * fx
        rows = lax.broadcasted_iota(jnp.int32, (p.wide, LANES), 0)
        oh_t[:, cut] = jnp.where(rows == slot, 1.0, 0.0).astype(bf16)
        kind = jnp.broadcast_to(group, (16, LANES))
        for g in range(p.groups):
            mask[g, :, cut] = jnp.where(kind == g, 1.0, 0.0).astype(bf16)
        return carry

    lax.fori_loop(0, p.sticks // LANES, table, 0)
    me = lax.axis_index("ga")
    flat = rows_s[1:2, pl.ds(pl.multiple_of(me * p.own, LANES), p.own)]
    z = centred(lax.broadcasted_iota(jnp.int32, (p.grid, p.own), 0))
    kinetic = (z * z + flat).astype(f32) * (4.0 / (p.grid * p.grid))
    for b in range(p.bands):
        diag[b] = kinetic + shift_r[b]


def widen(p, raw, pot):
    lane = lax.broadcasted_iota(jnp.int32, (1, LANES), 1)
    for y in range(p.grid):
        tile, off = divmod(y * p.grid, LANES)
        value = raw[:, tile * LANES : (tile + 1) * LANES]
        if off:
            value = pltpu.roll(value, LANES - off, 1)
        if off + p.grid > LANES:
            more = raw[:, (tile + 1) * LANES : (tile + 2) * LANES]
            value = jnp.where(lane < LANES - off, value, pltpu.roll(more, LANES - off, 1))
        pot[pl.ds(y, p.planes, stride=p.pot_step), :] = value


def narrow(p, wide_y, rows, out):
    lane = lax.broadcasted_iota(jnp.int32, (1, LANES), 1)
    made = None
    for y in range(wide_y):
        tile, off = divmod(y * p.grid, LANES)
        value = rows[pl.ds(y, p.planes, stride=wide_y), :]
        if off:
            value = pltpu.roll(value, off, 1)
        made = value if off == 0 else jnp.where(lane < off, made, value)
        if off + p.grid >= LANES:
            out[:, tile * LANES : (tile + 1) * LANES] = made
            made = value
    if wide_y * p.grid % LANES:
        tile = wide_y * p.grid // LANES
        out[:, tile * LANES :] = made[:, : wide_y * p.grid - tile * LANES]


def build_pair(p, dij_r, type_r, pair):
    kinds, per, _ = dij_r.shape
    shape = (8, p.count)
    row = lax.broadcasted_iota(jnp.int32, shape, 0)
    col = lax.broadcasted_iota(jnp.int32, shape, 1)
    for first in range(0, p.count, 8):
        kind = jnp.zeros(shape, jnp.int32)
        for a in range(first // per, (first + 8) // per):
            kind = jnp.where((row + first) // per == a, type_r[a], kind)
        value = jnp.zeros(shape, f32)
        for t in range(kinds):
            for i in range(per):
                here = (kind == t) & (row % per == i)
                for k in range(per):
                    value = jnp.where(here & (col % per == k), dij_r[t, i, k], value)
        value = jnp.where((row + first) // per == col // per, value, 0.0)
        pair[pl.ds(first, 8), :] = value


def spread_rows(pay, part):
    rows = part.shape[0]
    here = lax.broadcasted_iota(jnp.int32, (rows, rows), 0) == lax.broadcasted_iota(
        jnp.int32, (rows, rows), 1
    )
    ones = jnp.ones((rows, LANES), bf16)
    made = 0.0
    for piece in split3(jnp.where(here, pay[0:1], 0.0)):
        made = made + dot(piece, ones)
    part[...] = made


def intersect(p, groups, gath, image, part, pay):
    many = groups * p.bands
    inv_norm = 1.0 / (2.0 * p.grid * p.sticks)
    for n in range(p.bands):

        def overlap(t, acc, n=n):
            z = aligned(t, TALL)
            acc = list(acc)
            for lane in range(0, p.own, LANES):
                cut = pl.ds(lane, LANES)
                i_re, i_im = image[0, n, z, cut], image[1, n, z, cut]
                for m in range(many):
                    p_re = gath[m // p.bands, 0, m % p.bands, z, cut].astype(f32)
                    p_im = gath[m // p.bands, 1, m % p.bands, z, cut].astype(f32)
                    re = p_re * i_re + p_im * i_im
                    im = p_re * i_im - p_im * i_re
                    acc[2 * m] = acc[2 * m] + (re[:8] + re[8:])
                    acc[2 * m + 1] = acc[2 * m + 1] + (im[:8] + im[8:])
            return tuple(acc)

        zero = jnp.zeros((8, LANES), f32)
        acc = lax.fori_loop(0, p.grid // TALL, overlap, (zero,) * (2 * many))
        for m in range(2 * many):
            part[pl.ds(n * 2 * many + m, 1), :] = jnp.sum(acc[m], axis=0, keepdims=True)
    ones = jnp.ones((8, LANES), bf16)
    made = 0.0
    for piece in split3(part[...]):
        made = made + dot_t(ones, piece)
    pay[...] = made * inv_norm


def right_side(p, groups, gath, image, inter, diag, rhs):
    many = groups * p.bands
    stats = []
    for n in range(p.bands):

        def right(t, acc, n=n):
            z = aligned(t, TALL)
            norm, curve = acc
            for lane in range(0, p.own, LANES):
                cut = pl.ds(lane, LANES)
                re, im = -image[0, n, z, cut], -image[1, n, z, cut]
                for m in range(many):
                    p_re = gath[m // p.bands, 0, m % p.bands, z, cut].astype(f32)
                    p_im = gath[m // p.bands, 1, m % p.bands, z, cut].astype(f32)
                    row = n * 2 * many + 2 * m
                    c_re = inter[row : row + 1, :]
                    c_im = inter[row + 1 : row + 2, :]
                    re = re + (c_re * p_re - c_im * p_im)
                    im = im + (c_im * p_re + c_re * p_im)
                rhs[0, n, z, cut] = re
                rhs[1, n, z, cut] = im
                square = re * re + im * im
                norm = norm + square
                curve = curve + square * diag[n, z, cut]
            return norm, curve

        zero = jnp.zeros((TALL, LANES), f32)
        norm, curve = lax.fori_loop(0, p.grid // TALL, right, (zero, zero))
        stats.append((norm, curve))
    return stats


def fresh(p, rhs, image, back, diag, alpha, res):
    stats = []
    for b in range(p.bands):

        def one(t, acc, b=b):
            z = aligned(t, 8)
            norm, curve = acc
            for lane in range(0, p.own, LANES):
                cut = pl.ds(lane, LANES)
                scale = diag[b, z, cut]
                square = 0.0
                for c in range(2):
                    r = rhs[c, b, z, cut]
                    made = scale * r + image[c, b, z, cut] + back[c, b, z, cut]
                    new = r - alpha[b] * made
                    res[c, b, z, cut] = new
                    square = square + new * new
                norm = norm + square
                curve = curve + square * scale
            return norm, curve

        zero = jnp.zeros((8, LANES), f32)
        stats.append(lax.fori_loop(0, p.grid // 8, one, (zero, zero)))
    return stats


def answers(p, keep, alpha, rhs, res, out):
    for b in range(p.bands):

        def answer(t, carry, b=b):
            z = aligned(t, 8)
            for lane_at in range(0, p.own, LANES):
                cut = pl.ds(lane_at, LANES)
                for c in range(2):
                    out[c, b, z, cut] = keep[b] * rhs[c, b, z, cut] + alpha[b] * res[c, b, z, cut]
            return carry

        lax.fori_loop(0, p.grid // 8, answer, 0)


def settle(*arrays):
    def kernel(*refs):
        for source, target in zip(refs[: len(arrays)], refs[len(arrays) :]):
            target[...] = source[...]

    return pl.pallas_call(
        kernel,
        out_shape=[spec_of(x.shape) for x in arrays],
        in_specs=[VMEM] * len(arrays),
        out_specs=[VMEM] * len(arrays),
        name="settle",
    )(*arrays)


def everywhere(x):
    x = jnp.sum(x, axis=0, keepdims=True)
    return jnp.broadcast_to(jnp.sum(x, axis=1, keepdims=True), x.shape)


def pay_stats(p, stats, pay):
    for b in range(p.bands):
        at = 2 * p.bands + b
        pay[at : at + 1, :] = everywhere(stats[b][0])
        at = 3 * p.bands + b
        pay[at : at + 1, :] = everywhere(stats[b][1])


def program(p, groups, psi, dv, vloc, beta_array, xy, shift, dij, atom_type):
    payload = -(-4 * p.bands // 8) * 8
    few = -(-p.bands // 8) * 8
    many = groups * p.bands
    inters = p.bands * many * 2
    wide_y = p.grid // groups
    dense = p.planes % 4 == 0 and LANES - p.grid == p.grid // 3
    thick = p.planes * 3 // 4 if dense else p.planes
    rest = LANES - p.grid
    coded = dense and wide_y % 8 == 0
    dense_rows = -(-thick * wide_y // 16) * 16
    chunk = (p.shards, p.rows, p.own)
    mine = (2, p.bands, p.grid, p.own)
    cells = p.images * p.grid
    many_rows = p.groups * p.rows
    n_chunks = p.matrix // JB

    def kernel(
        psi_h, dv_h, vloc_h, beta_hbm, xy_h, shift_r, dij_r, type_r,
        z_inv_h, z_fwd_h, y_inv_h, x_inv_h, x_fwd_h, y_fwd_h,
        resp_o, dens_r,
        rows_s, pot_dv, pot_v, pair, oh_t, mask, left, sq, mixed, spectrum, field_p, field_0, field_1,
        chunk_a, chunk_b, held_a, held_b, held_c, held_d, held_e,
        gath, joined, image, rhs, res, diag, stat,
        part, pay_i, sums_i, pay_a, sums_a, pay_b, sums_b, pay_c, sums_c, pay_d, sums_d,
        staged, beta, beta_f, stacked, acc, acc_f, coefs, coefs_f,
        dens_f, dens_q, dens_send, dens_got, scale_send, scale_got, dens_sum,
        beta_sem, sends, recvs, band_sends, band_recvs, out_sem,
        psi_r, dv_r, vloc_r, xy_r, z_inv, z_fwd, y_inv, x_inv, x_fwd, y_fwd, in_sem,
    ):
        me = lax.axis_index("ga")
        mine_band = lax.axis_index("band")

        def over(source, held, which, scatter):
            return pusher("ga", p.shards, source, held, sends, recvs, which, scatter)

        greet("ga", p.shards)
        greet("band", groups)
        loads = [
            pltpu.make_async_copy(source, target, in_sem.at[i])
            for i, (source, target) in enumerate(
                (
                    (psi_h, psi_r), (z_inv_h, z_inv), (xy_h, xy_r), (dv_h, dv_r),
                    (y_inv_h, y_inv), (x_inv_h, x_inv), (x_fwd_h, x_fwd), (y_fwd_h, y_fwd),
                    (z_fwd_h, z_fwd), (vloc_h, vloc_r),
                )
            )
        ]
        for load in loads:
            load.start()
        for at in range(SLOTS):
            fetch(p, beta_hbm, staged, beta_sem, at).start()
        loads[0].wait()
        loads[1].wait()
        to_lines(
            p, lambda b: jnp.concatenate([psi_r[0, b], psi_r[1, b]], axis=0), z_inv, chunk_a, True
        )
        pl.semaphore_wait(pltpu.get_barrier_semaphore(), p.shards + groups - 2)
        push_a = over(chunk_a, held_a, 0, True)
        start_all(push_a, p.shards)
        push_psi = pusher("band", groups, psi_r, gath, band_sends, band_recvs, 0, False)
        start_all(push_psi, groups)
        held_a[me] = chunk_a[me]
        gath[mine_band] = psi_r[...]
        for load in loads[2:]:
            load.wait()
        tables(p, xy_r, shift_r, rows_s, oh_t, mask, diag)
        widen(p, dv_r, pot_dv)

        early, middle = n_chunks * 7 // 8, n_chunks
        convert(p, beta_hbm, staged, beta_sem, beta, 0, early)
        rest_copy = pltpu.make_async_copy(
            beta_hbm.at[:, pl.ds(p.matrix, p.vector)], beta_f, out_sem.at[1]
        )
        rest_copy.start()
        wait_all(push_a, p.shards)

        lines_to_rows(p, held_a, oh_t, mask, left, sq)
        rows_to_mixed(p, sq, y_inv, mixed)
        mixed_to_field(p, mixed, x_inv, x_fwd, pot_dv, field_p, spectrum, None)
        push_b = over(chunk_b, held_b, 1, True)
        spectrum_to_lines(p, spectrum, y_fwd, oh_t, rows_s, sq, left, chunk_b, held_b, push_b)
        convert(p, beta_hbm, staged, beta_sem, beta, early, middle)
        widen(p, vloc_r, pot_v)
        build_pair(p, dij_r, type_r, pair)
        wait_all(push_psi, groups)
        wait_all(push_b, p.shards)

        from_lines(p, held_b, joined, z_fwd, image)
        intersect(p, groups, gath, image, part, pay_i)
        push_i = over(pay_i, sums_i, 2, False)
        start_all(push_i, p.shards)
        sums_i[me] = pay_i[...]
        convert(p, beta_hbm, staged, beta_sem, beta, middle, n_chunks)
        rest_copy.wait()
        wait_all(push_i, p.shards)
        spread_rows(total_of(sums_i, p.shards), part)
        stats = right_side(p, groups, gath, image, part, diag, rhs)
        to_lines(
            p, lambda b: jnp.concatenate([rhs[0, b], rhs[1, b]], axis=0), z_inv, chunk_a, False
        )
        stack_vector(p, rhs, stacked)
        push_c = over(chunk_a, held_c, 3, True)
        start_all(push_c, p.shards)
        held_c[me] = chunk_a[me]
        pay_stats(p, stats, pay_a)
        project(p, beta, beta_f, rhs, stacked, acc, acc_f, pay_a)
        push_pa = over(pay_a, sums_a, 4, False)
        start_all(push_pa, p.shards)
        sums_a[me] = pay_a[...]
        wait_all(push_c, p.shards)

        lines_to_rows(p, held_c, oh_t, mask, left, sq)
        rows_to_mixed(p, sq, y_inv, mixed)
        mixed_to_field(p, mixed, x_inv, x_fwd, pot_v, field_0, spectrum, stat)
        for b in range(p.bands):
            pay_b[b : b + 1, :] = everywhere(stat[b])
        push_pb = over(pay_b, sums_b, 5, False)
        start_all(push_pb, p.shards)
        sums_b[me] = pay_b[...]
        push_d = over(chunk_b, held_d, 6, True)
        spectrum_to_lines(p, spectrum, y_fwd, oh_t, rows_s, sq, left, chunk_b, held_d, push_d)
        wait_all(push_pa, p.shards)
        total = total_of(sums_a, p.shards)
        made, energy = couple(p, total, pair)
        build_coefs(p, made, coefs, coefs_f)
        back_project(p, beta, beta_f, coefs, coefs_f, res)
        wait_all(push_pb, p.shards)
        planes = total_of(sums_b, p.shards)
        norm0, alpha0 = [], []
        for b in range(p.bands):
            norm0.append(total[2 * p.bands + b : 2 * p.bands + b + 1])
            curve = total[3 * p.bands + b : 3 * p.bands + b + 1] + planes[b : b + 1] + energy[b]
            alpha0.append(norm0[b] / curve)
        wait_all(push_d, p.shards)
        from_lines(p, held_d, joined, z_fwd, image)
        stats = fresh(p, rhs, image, res, diag, alpha0, res)
        to_lines(
            p, lambda b: jnp.concatenate([res[0, b], res[1, b]], axis=0), z_inv, chunk_a, False
        )
        stack_vector(p, res, stacked)
        push_e = over(chunk_a, held_e, 7, True)
        start_all(push_e, p.shards)
        held_e[me] = chunk_a[me]
        pay_stats(p, stats, pay_c)
        project(p, beta, beta_f, res, stacked, acc, acc_f, pay_c)
        push_pc = over(pay_c, sums_c, 8, False)
        start_all(push_pc, p.shards)
        sums_c[me] = pay_c[...]
        wait_all(push_e, p.shards)

        lines_to_rows(p, held_e, oh_t, mask, left, sq)
        rows_to_mixed(p, sq, y_inv, mixed)
        mixed_to_field(p, mixed, x_inv, None, pot_v, field_1, None, stat)
        for b in range(p.bands):
            pay_d[b : b + 1, :] = everywhere(stat[b])
        push_pd = over(pay_d, sums_d, 9, False)
        start_all(push_pd, p.shards)
        sums_d[me] = pay_d[...]
        wait_all(push_pc, p.shards)
        total = total_of(sums_c, p.shards)
        made, energy = couple(p, total, pair)
        wait_all(push_pd, p.shards)
        planes = total_of(sums_d, p.shards)
        keep, alpha1 = [], []
        for b in range(p.bands):
            norm1 = total[2 * p.bands + b : 2 * p.bands + b + 1]
            curve = total[3 * p.bands + b : 3 * p.bands + b + 1] + planes[b : b + 1] + energy[b]
            ratio = norm1 / norm0[b]
            alpha = norm1 / (curve - ratio * norm1 / alpha0[b])
            alpha1.append(alpha)
            keep.append(alpha0[b] + alpha * ratio)

        def plane(zp):
            made = 0.0
            for b in range(p.bands):
                at = aligned(b * p.planes + zp, p.grid)
                k2 = jnp.concatenate([keep[b], keep[b]], axis=1)
                a2 = jnp.concatenate([alpha1[b], alpha1[b]], axis=1)
                made = made + field_p[at, :] * (k2 * field_0[at, :] + a2 * field_1[at, :])
            return 4.0 * (made[:, :LANES] + made[:, LANES:])

        lane = lax.broadcasted_iota(jnp.int32, (1, LANES), 1)
        if dense:

            def four(i, carry):
                last = plane(4 * i + 3)
                for k in range(3):
                    moved = pltpu.roll(last, p.grid - k * rest, 1)
                    dens_f[3 * i + k] = jnp.where(lane < p.grid, plane(4 * i + k), moved)
                return carry

            lax.fori_loop(0, p.planes // 4, four, 0)
        else:

            def single(i, carry):
                dens_f[i] = plane(i)
                return carry

            lax.fori_loop(0, p.planes, single, 0)

        if coded:
            for g in range(groups):
                for at in range(thick):
                    value = dens_f[at, g * wide_y : (g + 1) * wide_y, :]
                    top = jnp.max(jnp.abs(value), axis=0, keepdims=True)
                    up = jnp.where(top > 1e-30, TOP / top, 0.0)
                    dens_q[at * wide_y : (at + 1) * wide_y, :] = jnp.round(value * up)
                    scale_send[g, at : at + 1, :] = top * (1.0 / TOP)
                dens_send[g] = dens_q[...].astype(jnp.int16)
        else:
            for g in range(groups):
                for at in range(thick):
                    to = pl.ds(at * wide_y, wide_y)
                    dens_send[g, to, :] = dens_f[at, g * wide_y : (g + 1) * wide_y, :]

        push_z = pusher("band", groups, dens_send, dens_got, band_sends, band_recvs, 1, True)
        start_all(push_z, groups)
        answers(p, keep, alpha1, rhs, res, image)
        resp_copy = pltpu.make_async_copy(image, resp_o, out_sem.at[0])
        if coded:
            push_s = pusher("band", groups, scale_send, scale_got, band_sends, band_recvs, 2, True)
            start_all(push_s, groups)
        resp_copy.start()
        if coded:
            wait_all(push_s, groups)
        wait_all(push_z, groups)
        if coded:
            base = pl.ds(pl.multiple_of(mine_band * wide_y, 8), wide_y)
            total = [dens_f[at, base, :] for at in range(thick)]
            for hop in range(1, groups):
                src = lax.rem(mine_band + hop, groups)
                dens_q[...] = dens_got[src].astype(f32)
                for at in range(thick):
                    total[at] = total[at] + (
                        dens_q[at * wide_y : (at + 1) * wide_y, :] * scale_got[src, at : at + 1, :]
                    )
        else:
            dens_got[mine_band] = dens_send[mine_band]
            total = []
            for at in range(thick):
                to = pl.ds(at * wide_y, wide_y)
                value = dens_got[0, to, :]
                for g in range(1, groups):
                    value = value + dens_got[g, to, :]
                total.append(value)
        if dense:
            for i in range(p.planes // 4):
                last = jnp.zeros((wide_y, LANES), f32)
                for k in range(3):
                    value = total[3 * i + k]
                    dens_sum[pl.ds((4 * i + k) * wide_y, wide_y), :] = value
                    moved = pltpu.roll(value, LANES - p.grid + k * rest, 1)
                    inside = (lane >= k * rest) & (lane < (k + 1) * rest)
                    last = jnp.where(inside, moved, last)
                dens_sum[pl.ds((4 * i + 3) * wide_y, wide_y), :] = last
        else:
            for at in range(p.planes):
                dens_sum[pl.ds(at * wide_y, wide_y), :] = total[at]
        narrow(p, wide_y, dens_sum, dens_r)
        resp_copy.wait()

    small = (p.shards, payload, LANES)
    tiny = (p.shards, few, LANES)
    scratch = [
        pltpu.VMEM((8, p.sticks), jnp.int32),
        pltpu.VMEM((p.planes * p.pot_step, LANES), f32),
        pltpu.VMEM((p.planes * p.pot_step, LANES), f32),
        pltpu.VMEM((p.count, p.count), f32),
        pltpu.VMEM((p.wide, p.sticks), bf16),
        pltpu.VMEM((p.groups, 16, p.sticks), bf16),
        pltpu.VMEM((2, many_rows, p.sticks), bf16),
        pltpu.VMEM(
            (p.tiles, max(p.groups * p.row_step, p.rows * p.group_step), LANES), f32
        ),
        pltpu.VMEM((2, cells, 2 * LANES), bf16),
        pltpu.VMEM((cells, 2 * LANES), f32),
        pltpu.VMEM((cells, 2 * LANES), f32),
        pltpu.VMEM((cells, 2 * LANES), f32),
        pltpu.VMEM((cells, 2 * LANES), f32),
        pltpu.VMEM(chunk, f32),
        pltpu.VMEM(chunk, f32),
        pltpu.VMEM(chunk, f32),
        pltpu.VMEM(chunk, f32),
        pltpu.VMEM(chunk, f32),
        pltpu.VMEM(chunk, f32),
        pltpu.VMEM(chunk, f32),
        pltpu.VMEM((groups,) + mine, bf16),
        pltpu.VMEM((p.shards * p.q, p.own), f32),
        pltpu.VMEM(mine, f32),
        pltpu.VMEM(mine, f32),
        pltpu.VMEM(mine, f32),
        pltpu.VMEM((p.bands, p.grid, p.own), f32),
        pltpu.VMEM((p.bands, 8, LANES), f32),
        pltpu.VMEM((inters, LANES), f32),
        pltpu.VMEM((8, inters), f32),
        pltpu.VMEM((p.shards, 8, inters), f32),
        pltpu.VMEM((payload, LANES), f32),
        pltpu.VMEM(small, f32),
        pltpu.VMEM((few, LANES), f32),
        pltpu.VMEM(tiny, f32),
        pltpu.VMEM((payload, LANES), f32),
        pltpu.VMEM(small, f32),
        pltpu.VMEM((few, LANES), f32),
        pltpu.VMEM(tiny, f32),
        pltpu.VMEM((SLOTS, 2, JB, p.grid, p.own), f32),
        pltpu.VMEM((2, 2, p.matrix, p.grid, p.own), bf16),
        pltpu.VMEM((2, p.vector, p.grid, p.own), f32),
        pltpu.VMEM((p.grid // TALL, 4 * p.bands * TALL, p.own), bf16),
        pltpu.VMEM((2, p.matrix, 8, 4 * p.bands * TALL), f32),
        pltpu.VMEM((2 * p.bands, p.vector, 8, LANES), f32),
        pltpu.VMEM((2, 2 * p.bands * TALL, 2 * p.matrix * TALL), bf16),
        pltpu.VMEM((2 * p.bands, p.vector, LANES), f32),
        pltpu.VMEM((thick, p.grid, LANES), f32),
        pltpu.VMEM((dense_rows, LANES), f32),
        pltpu.VMEM((groups, dense_rows, LANES), jnp.int16 if coded else f32),
        pltpu.VMEM((groups, dense_rows, LANES), jnp.int16 if coded else f32),
        pltpu.VMEM((groups, -(-thick // 8) * 8, LANES), f32),
        pltpu.VMEM((groups, -(-thick // 8) * 8, LANES), f32),
        pltpu.VMEM((p.planes * wide_y, LANES), f32),
        pltpu.SemaphoreType.DMA((SLOTS,)),
        pltpu.SemaphoreType.DMA((10, p.shards - 1)),
        pltpu.SemaphoreType.DMA((10, p.shards - 1)),
        pltpu.SemaphoreType.DMA((3, groups - 1)),
        pltpu.SemaphoreType.DMA((3, groups - 1)),
        pltpu.SemaphoreType.DMA((2,)),
        pltpu.VMEM(mine, bf16),
        pltpu.VMEM(dv.shape, f32),
        pltpu.VMEM(vloc.shape, f32),
        pltpu.VMEM(xy.shape, jnp.int32),
    ]
    scratch += [
        pltpu.VMEM(table.shape, bf16)
        for table in (p.z_inv, p.z_fwd, p.y_inv, p.x_inv, p.x_fwd, p.y_fwd)
    ]
    scratch.append(pltpu.SemaphoreType.DMA((10,)))

    hbm = pl.BlockSpec(memory_space=pl.ANY)
    smem = pl.BlockSpec(memory_space=pltpu.SMEM)
    return pl.pallas_call(
        kernel,
        out_shape=[
            spec_of(mine), spec_of((p.planes, wide_y * p.grid)),
        ],
        in_specs=[hbm] * 5 + [smem] * 3 + [hbm] * 6,
        out_specs=[hbm, VMEM],
        scratch_shapes=scratch,
        compiler_params=pltpu.CompilerParams(
            collective_id=0, has_side_effects=True, vmem_limit_bytes=67_043_328
        ),
        name="response",
    )(
        psi, dv, vloc, beta_array, xy, shift, dij, atom_type,
        p.z_inv, p.z_fwd, p.y_inv, p.x_inv, p.x_fwd, p.y_fwd,
    )


def per_device(groups, shards, psi, vloc, dv, beta, dij, atom_type, stick_xy, band_shift):
    _, bands, grid, own = psi.shape
    planes = vloc.shape[0]
    sticks = stick_xy.shape[0]
    count = beta.shape[1]
    p = Plan(bands, grid, own, planes, shards, sticks, count)
    xy = stick_xy.reshape(sticks // LANES, LANES)
    return settle(*program(p, groups, psi, dv, vloc, beta, xy, band_shift, dij, atom_type))


def solution(mesh):
    placed = (
        P(None, "band", None, "ga"),
        P("ga", None),
        P("ga", None),
        P(None, None, None, "ga"),
        P(),
        P(),
        P(),
        P("band"),
    )
    groups, shards = mesh.shape["band"], mesh.shape["ga"]

    def body(*args):
        return per_device(groups, shards, *args)

    return jax.shard_map(
        body,
        mesh=mesh,
        in_specs=placed,
        out_specs=(P(None, "band", None, "ga"), P("ga", "band")),
        check_vma=False,
    )
```

```python
import math

import jax
import jax.numpy as jnp
import ml_dtypes
import numpy as np
from jax import lax
from jax.experimental import pallas as pl
from jax.experimental.pallas import tpu as pltpu
from jax.sharding import PartitionSpec as P

LANES = 128
PER = 4
TALL = 16
f32, bf16 = jnp.float32, jnp.bfloat16
VMEM = pl.BlockSpec(memory_space=pltpu.VMEM)


def frequency(index, grid):
    return (index + grid // 2) % grid - grid // 2


def phase(rows, cols, grid, sign):
    angle = 2.0 * math.pi * ((rows[:, None] * cols[None, :]) % grid) / grid
    return np.exp(1j * sign * angle) / math.sqrt(grid)


def parts_of(table):
    return np.stack(
        [np.stack([table.real, -table.imag], 1), np.stack([table.imag, table.real], 1)]
    )


def halves_of(table):
    table = table.astype(np.float32)
    hi = table.astype(ml_dtypes.bfloat16)
    lo = (table - hi.astype(np.float32)).astype(ml_dtypes.bfloat16)
    return hi, lo


class Plan:
    def __init__(self, bands, grid, own, planes, shards, sticks, count):
        self.bands, self.grid, self.own, self.planes = bands, grid, own, planes
        self.shards, self.sticks, self.count = shards, sticks, count
        self.vector = count * 4 // 8 // TALL * TALL
        self.matrix = count - self.vector
        self.side = 2 * (grid // 3)
        self.q = 2 * planes
        self.rows = -(-bands * self.q // 16) * 16
        self.images = bands * planes
        self.groups = self.side // PER
        self.fold = LANES // self.side
        self.tiles = PER // self.fold
        self.wide = PER * self.side
        self.row_step = self.rows + 8
        self.group_step = self.groups + 8
        self.pot_step = grid + 8
        side, fold, tiles, groups = self.side, self.fold, self.tiles, self.groups
        cells = np.arange(grid)
        freqs = np.arange(side) - grid // 3
        z = parts_of(phase(cells, cells, grid, 1.0))
        z = z.reshape(2, shards, planes, 2 * grid).transpose(1, 0, 2, 3)
        self.z_inv = np.stack(halves_of(z.reshape(shards * self.q, 2 * grid)))
        z = parts_of(phase(cells, cells, grid, -1.0))
        z = z.reshape(2, grid, 2, shards, planes).transpose(0, 1, 3, 2, 4)
        self.z_fwd = np.stack(halves_of(z.reshape(2 * grid, shards * self.q)))
        y = parts_of(phase(cells, freqs, grid, 1.0))
        y = y.reshape(2, grid, 2, groups, tiles, fold).transpose(0, 5, 1, 2, 4, 3)
        hi, lo = halves_of(y.reshape(2 * fold * grid, 2 * tiles * groups))
        self.y_inv = np.concatenate([hi, hi, lo], axis=1)
        x = parts_of(phase(freqs, cells, grid, 1.0).T).transpose(2, 3, 0, 1)
        x = np.repeat(x[:, None], fold, axis=1)
        x = np.pad(x, ((0, 0),) * 4 + ((0, LANES - grid),))
        self.x_inv = np.stack(halves_of(x.reshape(2 * LANES, 2 * LANES)))
        x = parts_of(phase(cells, freqs, grid, -1.0).T).transpose(2, 3, 0, 1)
        x = np.repeat(x[:, :, :, None], fold, axis=3)
        x = np.pad(x, ((0, 0), (0, LANES - grid)) + ((0, 0),) * 3)
        self.x_fwd = np.stack(halves_of(x.reshape(2 * LANES, 2 * LANES)))
        y = parts_of(phase(freqs, cells, grid, -1.0))
        y = y.reshape(2, groups, tiles, fold, 2 * grid).transpose(0, 3, 2, 1, 4)
        self.y_fwd = np.stack(halves_of(y.reshape(2 * side, 2 * grid)))


def dot(a, b):
    return jnp.dot(a, b, preferred_element_type=f32)


def dot_t(a, b):
    return lax.dot_general(a, b, (((1,), (1,)), ((), ())), preferred_element_type=f32)


def split(x):
    hi = x.astype(bf16)
    return hi, (x - hi.astype(f32)).astype(bf16)


def split3(x):
    hi = x.astype(bf16)
    rest = x - hi.astype(f32)
    mid = rest.astype(bf16)
    return hi, mid, (rest - mid.astype(f32)).astype(bf16)


def aligned(at, size):
    return pl.ds(pl.multiple_of(at * size, math.gcd(size, LANES)), size)


def spec_of(shape, dtype=f32):
    return jax.ShapeDtypeStruct(shape, dtype)


def lines_to_rows(p, held, oh_t, mask, left, sq):
    def spread(src, carry):
        at = aligned(src, p.own)
        hi, lo = split(held[src])
        for g in range(p.groups):
            keep = mask[g, :, at]
            for r in range(0, p.rows, 16):
                to = pl.ds(g * p.rows + r, 16)
                left[0, to, at] = hi[r : r + 16] * keep
                left[1, to, at] = lo[r : r + 16] * keep
        return carry

    lax.fori_loop(0, p.shards, spread, 0)
    many = p.groups * p.rows
    made = dot_t(left[...].reshape(2 * many, p.sticks), oh_t[...])
    made = made[:many] + made[many:]
    for g in range(p.groups):
        for t in range(p.tiles):
            sq[t, pl.ds(g * p.row_step, p.rows), :] = made[
                g * p.rows : (g + 1) * p.rows, t * LANES : (t + 1) * LANES
            ]


def rows_to_mixed(p, sq, y_inv, mixed):
    low = lax.broadcasted_iota(jnp.int32, (1, 2 * LANES), 1) % LANES < p.side

    def pair(at, carry):
        for b in range(p.bands):
            tiles = []
            for k in range(2):
                pieces = []
                for c in range(2):
                    n = b * p.q + c * p.planes + 2 * at + k
                    for t in range(p.tiles):
                        pieces.append(sq[t, pl.ds(n, p.groups, stride=p.row_step), :])
                tiles.append(jnp.concatenate(pieces, axis=0))
            hi, lo = split(jnp.concatenate(tiles, axis=1))
            out = dot(y_inv[...], jnp.concatenate([hi, lo, hi], axis=0))
            both = [
                jnp.where(
                    low,
                    out[2 * c * p.grid : (2 * c + 1) * p.grid],
                    out[(2 * c + 1) * p.grid : (2 * c + 2) * p.grid],
                )
                for c in range(2)
            ]
            for k in range(2):
                lane = slice(k * LANES, (k + 1) * LANES)
                hi, lo = split(jnp.concatenate([both[0][:, lane], both[1][:, lane]], axis=1))
                to = aligned(b * p.planes + 2 * at + k, p.grid)
                mixed[0, to, :] = hi
                mixed[1, to, :] = lo
        return carry

    lax.fori_loop(0, p.planes // 2, pair, 0, unroll=3)


def mixed_to_field(p, mixed, x_inv, x_fwd, pot, field, spectrum, stat):
    size = p.planes * p.grid

    def block(b, carry):
        to = aligned(b, size)
        hi, lo = mixed[0, to, :], mixed[1, to, :]
        field[to, :] = dot(hi, x_inv[0]) + dot(lo, x_inv[0]) + dot(hi, x_inv[1])
        return carry

    lax.fori_loop(0, p.bands, block, 0)
    if stat is not None:
        stat[...] = jnp.zeros_like(stat)

    def scaled(at, carry):
        to = aligned(at, p.grid)
        one = field[to, :]
        rows = pl.ds(pl.multiple_of(lax.rem(at, p.planes) * p.pot_step, 8), p.grid)
        wide = pot[rows, :]
        used = one * jnp.concatenate([wide, wide], axis=1)
        if spectrum is not None:
            hi, lo = split(used)
            mixed[0, to, :] = hi
            mixed[1, to, :] = lo
        if stat is not None:
            made = jnp.sum((used * one).reshape(p.grid // 8, 8, 2 * LANES), axis=0)
            b = at // p.planes
            stat[b] = stat[b] + made[:, :LANES] + made[:, LANES:]
        return carry

    lax.fori_loop(0, p.images, scaled, 0, unroll=2)
    if spectrum is not None:

        def forth(b, carry):
            to = aligned(b, size)
            hi, lo = mixed[0, to, :], mixed[1, to, :]
            spectrum[to, :] = dot(hi, x_fwd[0]) + dot(lo, x_fwd[0]) + dot(hi, x_fwd[1])
            return carry

        lax.fori_loop(0, p.bands, forth, 0)


def spectrum_to_lines(p, spectrum, y_fwd, oh_t, rows_of, sq, left, lines, held, push):
    low = lax.broadcasted_iota(jnp.int32, (1, 2 * LANES), 1) % LANES < p.side
    half = p.side // p.fold

    def pair(at, carry):
        for b in range(p.bands):
            tiles = []
            for k in range(2):
                one = spectrum[aligned(b * p.planes + 2 * at + k, p.grid), :]
                tiles.append(jnp.concatenate([one[:, :LANES], one[:, LANES:]], axis=0))
            hi, lo = split(jnp.concatenate(tiles, axis=1))
            both = dot(y_fwd[...].reshape(4 * p.side, 2 * p.grid), hi)
            out = both[: 2 * p.side] + both[2 * p.side :] + dot(y_fwd[0], lo)
            for c in range(2):
                from_ = c * p.side
                both = jnp.where(
                    low, out[from_ : from_ + half], out[from_ + half : from_ + 2 * half]
                )
                for k in range(2):
                    n = b * p.q + c * p.planes + 2 * at + k
                    to = pl.ds(pl.multiple_of(n * p.group_step, 8), p.groups)
                    for t in range(p.tiles):
                        sq[t, to, :] = both[
                            t * p.groups : (t + 1) * p.groups, k * LANES : (k + 1) * LANES
                        ]
        return carry

    lax.fori_loop(0, p.planes // 2, pair, 0, unroll=3)
    for g in range(p.groups):
        to = pl.ds(g * p.rows, p.rows)
        for t in range(p.tiles):
            hi, lo = split(sq[t, pl.ds(g, p.rows, stride=p.group_step), :])
            left[0, to, t * LANES : (t + 1) * LANES] = hi
            left[1, to, t * LANES : (t + 1) * LANES] = lo

    def gather(dest):
        at = aligned(dest, p.own)
        weights = oh_t[:, at]
        got = dot(left[0, :, : p.wide], weights) + dot(left[1, :, : p.wide], weights)
        kind = rows_of[0:1, at]
        kept = got[: p.rows]
        for g in range(1, p.groups):
            kept = jnp.where(kind == g, got[g * p.rows : (g + 1) * p.rows], kept)
        return kept

    me = lax.axis_index("ga")

    def each(hop, carry):
        dest = lax.rem(me + hop, p.shards)
        lines[dest] = gather(dest)

        @pl.when(hop > 1)
        def _():
            push(hop - 1).start()

        return carry

    lax.fori_loop(1, p.shards, each, 0)
    held[me] = gather(me)
    push(p.shards - 1).start()


def greet(axis, count):
    me = lax.axis_index(axis)
    barrier = pltpu.get_barrier_semaphore()
    for hop in range(1, count):
        peer = lax.rem(me + hop, count)
        pl.semaphore_signal(
            barrier, inc=1, device_id={axis: peer}, device_id_type=pl.DeviceIdType.MESH
        )


def pusher(axis, count, source, held, sends, recvs, which, scatter):
    me = lax.axis_index(axis)

    def push(hop):
        peer = lax.rem(me + hop, count)
        return pltpu.make_async_remote_copy(
            src_ref=source.at[peer] if scatter else source,
            dst_ref=held.at[me],
            send_sem=sends.at[which, hop - 1],
            recv_sem=recvs.at[which, hop - 1],
            device_id={axis: peer},
            device_id_type=pl.DeviceIdType.MESH,
        )

    return push


def start_all(push, count):
    for hop in range(1, count):
        push(hop).start()


def wait_all(push, count):
    for hop in range(1, count):
        push(hop).wait()


def total_of(sums, count):
    total = sums[0]
    for at in range(1, count):
        total = total + sums[at]
    return total


def to_lines(p, value_of, z_inv, chunks, exact):
    for b in range(p.bands):
        value = value_of(b)
        if exact:
            out = dot(z_inv[0], value) + dot(z_inv[1], value)
        else:
            hi, lo = split(value)
            out = dot(z_inv[0], hi) + dot(z_inv[0], lo) + dot(z_inv[1], hi)
        for d in range(p.shards):
            chunks[d, b * p.q : (b + 1) * p.q, :] = out[d * p.q : (d + 1) * p.q]


def from_lines(p, held, joined, z_fwd, result):
    for b in range(p.bands):
        for src in range(p.shards):
            joined[src * p.q : (src + 1) * p.q, :] = held[src, b * p.q : (b + 1) * p.q, :]
        hi, lo = split(joined[...])
        out = dot(z_fwd[0], hi) + dot(z_fwd[0], lo) + dot(z_fwd[1], hi)
        result[0, b] = out[: p.grid]
        result[1, b] = out[p.grid :]


JB = 4
SLOTS = 4


def fetch(p, beta_hbm, staged, sem, at):
    return pltpu.make_async_copy(
        beta_hbm.at[:, pl.ds(at * JB, JB)], staged.at[at % SLOTS], sem.at[at % SLOTS]
    )


def convert(p, beta_hbm, staged, sem, beta, first, last):
    chunks = p.matrix // JB
    for at in range(first, last):
        fetch(p, beta_hbm, staged, sem, at).wait()
        slot = at % SLOTS

        def one(j, carry, at=at, slot=slot):
            for c in range(2):
                hi, lo = split(staged[slot, c, j])
                beta[0, c, at * JB + j] = hi
                beta[1, c, at * JB + j] = lo
            return carry

        lax.fori_loop(0, JB, one, 0)
        if at + SLOTS < chunks:
            fetch(p, beta_hbm, staged, sem, at + SLOTS).start()


def stack_vector(p, vec, stacked):
    for zt in range(p.grid // TALL):
        for b in range(p.bands):
            for c in range(2):
                hi, lo = split(vec[c, b, zt * TALL : (zt + 1) * TALL, :])
                at = (2 * b + c) * 2 * TALL
                stacked[zt, at : at + TALL, :] = hi
                stacked[zt, at + TALL : at + 2 * TALL, :] = lo


def project(p, beta, beta_f, vec, stacked, acc, acc_f, pay):
    cols = 4 * p.bands * TALL
    many = 2 * p.bands
    keep = (
        lax.broadcasted_iota(jnp.int32, (TALL, cols), 0)
        == lax.broadcasted_iota(jnp.int32, (TALL, cols), 1) % TALL
    )
    acc[...] = jnp.zeros_like(acc)
    acc_f[...] = jnp.zeros_like(acc_f)

    def tile(zt, carry):
        z = aligned(zt, TALL)
        right = stacked[zt]
        for c in range(2):
            hi = beta[0, c, :, z, :].reshape(p.matrix * TALL, p.own)
            lo = beta[1, c, :, z, :].reshape(p.matrix * TALL, p.own)
            out = (dot_t(hi, right) + dot_t(lo, right)).reshape(p.matrix, TALL, cols)
            out = jnp.where(keep[None], out, 0.0)
            acc[c] += out[:, :8] + out[:, 8:]
        for first in range(0, p.vector, 4):
            sums = [[acc_f[n, first + j] for n in range(many)] for j in range(4)]
            for part in range(TALL // 8):
                rows = pl.ds(pl.multiple_of(zt * TALL + part * 8, 8), 8)
                for lane in range(0, p.own, LANES):
                    cut = pl.ds(lane, LANES)
                    v_re = [vec[0, b, rows, cut] for b in range(p.bands)]
                    v_im = [vec[1, b, rows, cut] for b in range(p.bands)]
                    for j in range(4):
                        b_re = beta_f[0, first + j, rows, cut]
                        b_im = beta_f[1, first + j, rows, cut]
                        for b in range(p.bands):
                            sums[j][2 * b] = sums[j][2 * b] + (b_re * v_re[b] + b_im * v_im[b])
                            sums[j][2 * b + 1] = sums[j][2 * b + 1] + (
                                b_re * v_im[b] - b_im * v_re[b]
                            )
            for j in range(4):
                for n in range(many):
                    acc_f[n, first + j] = sums[j][n]
        return carry

    lax.fori_loop(0, p.grid // TALL, tile, 0)
    row = lax.broadcasted_iota(jnp.int32, (8, cols), 0)
    kind = lax.broadcasted_iota(jnp.int32, (8, cols), 1) // (2 * TALL)
    same = (row // 2 == kind // 2) & (row < many)
    plain = jnp.where(same & (row % 2 == kind % 2), 1.0, 0.0).astype(bf16)
    cross = jnp.where(
        same & (row % 2 != kind % 2), jnp.where(row % 2 == 0, 1.0, -1.0), 0.0
    ).astype(bf16)
    made = 0.0
    empty = jnp.zeros((p.vector, cols), f32)
    for c, pick in ((0, plain), (1, cross)):
        for piece in split3(jnp.concatenate([jnp.sum(acc[c], axis=1), empty], axis=0)):
            made = made + dot_t(pick, piece)
    empty = jnp.zeros((p.matrix, LANES), f32)
    for n in range(many):
        mine = jnp.where(lax.broadcasted_iota(jnp.int32, (8, LANES), 0) == n, 1.0, 0.0)
        for piece in split3(jnp.concatenate([empty, jnp.sum(acc_f[n], axis=1)], axis=0)):
            made = made + dot_t(mine.astype(bf16), piece)
    pay[0:many, :] = made[:many]


def couple(p, total, pair):
    hi, mid, lo = split3(total)
    p_hi, p_mid, p_lo = split3(pair[...])
    made = (
        dot_t(hi, p_hi) + dot_t(hi, p_mid) + dot_t(mid, p_hi)
        + dot_t(hi, p_lo) + dot_t(mid, p_mid) + dot_t(lo, p_hi)
    )
    product = jnp.sum(made * total, axis=1, keepdims=True)
    energy = [product[2 * b : 2 * b + 1] + product[2 * b + 1 : 2 * b + 2] for b in range(p.bands)]
    return made, energy


def build_coefs(p, made, coefs, coefs_f):
    blocks = p.matrix // TALL
    wide = TALL * TALL
    lane = lax.broadcasted_iota(jnp.int32, (TALL, wide), 1) // TALL
    source = lax.broadcasted_iota(jnp.int32, (TALL, wide), 0)
    repeat = jnp.where(lane == source, 1.0, 0.0).astype(bf16)
    keep = (
        lax.broadcasted_iota(jnp.int32, (TALL, wide), 0)
        == lax.broadcasted_iota(jnp.int32, (TALL, wide), 1) % TALL
    )
    ones = jnp.ones((p.count, LANES), bf16)
    chosen = (
        lax.broadcasted_iota(jnp.int32, (p.vector, p.count), 0) + p.matrix
        == lax.broadcasted_iota(jnp.int32, (p.vector, p.count), 1)
    )
    for n in range(2 * p.bands):
        hi, mid, lo = split3(jnp.where(chosen, made[n : n + 1], 0.0))
        coefs_f[n] = dot(hi, ones) + dot(mid, ones) + dot(lo, ones)
    hi, mid, lo = split3(made)
    for jb in range(blocks):
        cut = slice(jb * TALL, (jb + 1) * TALL)
        full = dot(hi[:, cut], repeat) + dot(mid[:, cut], repeat) + dot(lo[:, cut], repeat)
        for b in range(p.bands):
            re, im = full[2 * b : 2 * b + 1], full[2 * b + 1 : 2 * b + 2]
            for part, rows in ((0, (re, im)), (1, (-im, re))):
                for c in range(2):
                    one, two = split(jnp.where(keep, rows[c], 0.0))
                    to = slice((2 * b + c) * TALL, (2 * b + c + 1) * TALL)
                    at = slice((2 * jb + part) * wide, (2 * jb + part + 1) * wide)
                    coefs[0, to, at] = one
                    coefs[1, to, at] = two


def back_project(p, beta, beta_f, coefs, coefs_f, back):
    blocks = p.matrix // TALL
    wide = TALL * TALL
    many = 2 * p.bands * TALL

    def tile(zt, carry):
        z = aligned(zt, TALL)
        made = jnp.zeros((many, p.own), f32)
        places = [
            (part, pl.ds(pl.multiple_of(zt * TALL + part * 8, 8), 8), lane)
            for part in range(TALL // 8)
            for lane in range(0, p.own, LANES)
        ]
        sums = [[0.0] * (2 * p.bands) for _ in places]
        for jb in range(blocks):
            for part in range(2):
                js = slice(jb * TALL, (jb + 1) * TALL)
                hi = beta[0, part, js, z, :].reshape(wide, p.own)
                lo = beta[1, part, js, z, :].reshape(wide, p.own)
                at = slice((2 * jb + part) * wide, (2 * jb + part + 1) * wide)
                both = dot(coefs[:, :, at].reshape(2 * many, wide), hi)
                made = made + both[:many] + both[many:] + dot(coefs[0, :, at], lo)
            for j in range(p.vector * jb // blocks, p.vector * (jb + 1) // blocks):
                rows_c = [coefs_f[n, j : j + 1, :] for n in range(2 * p.bands)]
                for mine, (part, rows, lane) in zip(sums, places):
                    b_re = beta_f[0, j, rows, pl.ds(lane, LANES)]
                    b_im = beta_f[1, j, rows, pl.ds(lane, LANES)]
                    for b in range(p.bands):
                        c_re, c_im = rows_c[2 * b], rows_c[2 * b + 1]
                        mine[2 * b] = mine[2 * b] + (b_re * c_re - b_im * c_im)
                        mine[2 * b + 1] = mine[2 * b + 1] + (b_re * c_im + b_im * c_re)
        for mine, (part, rows, lane) in zip(sums, places):
            for b in range(p.bands):
                for c in range(2):
                    at = (2 * b + c) * TALL + part * 8
                    back[c, b, rows, pl.ds(lane, LANES)] = (
                        made[at : at + 8, lane : lane + LANES] + mine[2 * b + c]
                    )
        return carry

    lax.fori_loop(0, p.grid // TALL, tile, 0)


TOP = 32767.0


def tables(p, xy_r, shift_r, rows_s, oh_t, mask, diag):
    radius = p.grid // 3

    def centred(k):
        return jnp.where(k < p.grid // 2, k, k - p.grid)

    def table(at, carry):
        cut = aligned(at, LANES)
        xy = xy_r[pl.ds(at, 1), :]
        y = ((xy.astype(f32) + 0.5) * (1.0 / p.grid)).astype(jnp.int32)
        fy, fx = centred(y), centred(xy - y * p.grid)
        group = (fy + radius) // PER
        slot = (fy + radius - group * PER) * p.side + fx + radius
        rows_s[0:1, cut] = group
        rows_s[1:2, cut] = fy * fy + fx * fx
        rows = lax.broadcasted_iota(jnp.int32, (p.wide, LANES), 0)
        oh_t[:, cut] = jnp.where(rows == slot, 1.0, 0.0).astype(bf16)
        kind = jnp.broadcast_to(group, (16, LANES))
        for g in range(p.groups):
            mask[g, :, cut] = jnp.where(kind == g, 1.0, 0.0).astype(bf16)
        return carry

    lax.fori_loop(0, p.sticks // LANES, table, 0)
    me = lax.axis_index("ga")
    flat = rows_s[1:2, pl.ds(pl.multiple_of(me * p.own, LANES), p.own)]
    z = centred(lax.broadcasted_iota(jnp.int32, (p.grid, p.own), 0))
    kinetic = (z * z + flat).astype(f32) * (4.0 / (p.grid * p.grid))
    for b in range(p.bands):
        diag[b] = kinetic + shift_r[b]


def widen(p, raw, pot):
    lane = lax.broadcasted_iota(jnp.int32, (1, LANES), 1)
    for y in range(p.grid):
        tile, off = divmod(y * p.grid, LANES)
        value = raw[:, tile * LANES : (tile + 1) * LANES]
        if off:
            value = pltpu.roll(value, LANES - off, 1)
        if off + p.grid > LANES:
            more = raw[:, (tile + 1) * LANES : (tile + 2) * LANES]
            value = jnp.where(lane < LANES - off, value, pltpu.roll(more, LANES - off, 1))
        pot[pl.ds(y, p.planes, stride=p.pot_step), :] = value


def narrow(p, wide_y, rows, out):
    lane = lax.broadcasted_iota(jnp.int32, (1, LANES), 1)
    made = None
    for y in range(wide_y):
        tile, off = divmod(y * p.grid, LANES)
        value = rows[pl.ds(y, p.planes, stride=wide_y), :]
        if off:
            value = pltpu.roll(value, off, 1)
        made = value if off == 0 else jnp.where(lane < off, made, value)
        if off + p.grid >= LANES:
            out[:, tile * LANES : (tile + 1) * LANES] = made
            made = value
    if wide_y * p.grid % LANES:
        tile = wide_y * p.grid // LANES
        out[:, tile * LANES :] = made[:, : wide_y * p.grid - tile * LANES]


def build_pair(p, dij_r, type_r, pair):
    kinds, per, _ = dij_r.shape
    shape = (8, p.count)
    row = lax.broadcasted_iota(jnp.int32, shape, 0)
    col = lax.broadcasted_iota(jnp.int32, shape, 1)
    for first in range(0, p.count, 8):
        kind = jnp.zeros(shape, jnp.int32)
        for a in range(first // per, (first + 8) // per):
            kind = jnp.where((row + first) // per == a, type_r[a], kind)
        value = jnp.zeros(shape, f32)
        for t in range(kinds):
            for i in range(per):
                here = (kind == t) & (row % per == i)
                for k in range(per):
                    value = jnp.where(here & (col % per == k), dij_r[t, i, k], value)
        value = jnp.where((row + first) // per == col // per, value, 0.0)
        pair[pl.ds(first, 8), :] = value


def spread_rows(pay, part):
    rows = part.shape[0]
    here = lax.broadcasted_iota(jnp.int32, (rows, rows), 0) == lax.broadcasted_iota(
        jnp.int32, (rows, rows), 1
    )
    ones = jnp.ones((rows, LANES), bf16)
    made = 0.0
    for piece in split3(jnp.where(here, pay[0:1], 0.0)):
        made = made + dot(piece, ones)
    part[...] = made


def intersect(p, groups, gath, image, part, pay):
    many = groups * p.bands
    inv_norm = 1.0 / (2.0 * p.grid * p.sticks)
    for n in range(p.bands):

        def overlap(t, acc, n=n):
            z = aligned(t, TALL)
            acc = list(acc)
            for lane in range(0, p.own, LANES):
                cut = pl.ds(lane, LANES)
                i_re, i_im = image[0, n, z, cut], image[1, n, z, cut]
                for m in range(many):
                    p_re = gath[m // p.bands, 0, m % p.bands, z, cut].astype(f32)
                    p_im = gath[m // p.bands, 1, m % p.bands, z, cut].astype(f32)
                    re = p_re * i_re + p_im * i_im
                    im = p_re * i_im - p_im * i_re
                    acc[2 * m] = acc[2 * m] + (re[:8] + re[8:])
                    acc[2 * m + 1] = acc[2 * m + 1] + (im[:8] + im[8:])
            return tuple(acc)

        zero = jnp.zeros((8, LANES), f32)
        acc = lax.fori_loop(0, p.grid // TALL, overlap, (zero,) * (2 * many))
        for m in range(2 * many):
            part[pl.ds(n * 2 * many + m, 1), :] = jnp.sum(acc[m], axis=0, keepdims=True)
    ones = jnp.ones((8, LANES), bf16)
    made = 0.0
    for piece in split3(part[...]):
        made = made + dot_t(ones, piece)
    pay[...] = made * inv_norm


def right_side(p, groups, gath, image, inter, diag, rhs):
    many = groups * p.bands
    stats = []
    for n in range(p.bands):

        def right(t, acc, n=n):
            z = aligned(t, TALL)
            norm, curve = acc
            for lane in range(0, p.own, LANES):
                cut = pl.ds(lane, LANES)
                re, im = -image[0, n, z, cut], -image[1, n, z, cut]
                for m in range(many):
                    p_re = gath[m // p.bands, 0, m % p.bands, z, cut].astype(f32)
                    p_im = gath[m // p.bands, 1, m % p.bands, z, cut].astype(f32)
                    row = n * 2 * many + 2 * m
                    c_re = inter[row : row + 1, :]
                    c_im = inter[row + 1 : row + 2, :]
                    re = re + (c_re * p_re - c_im * p_im)
                    im = im + (c_im * p_re + c_re * p_im)
                rhs[0, n, z, cut] = re
                rhs[1, n, z, cut] = im
                square = re * re + im * im
                norm = norm + square
                curve = curve + square * diag[n, z, cut]
            return norm, curve

        zero = jnp.zeros((TALL, LANES), f32)
        norm, curve = lax.fori_loop(0, p.grid // TALL, right, (zero, zero))
        stats.append((norm, curve))
    return stats


def fresh(p, rhs, image, back, diag, alpha, res):
    stats = []
    for b in range(p.bands):

        def one(t, acc, b=b):
            z = aligned(t, 8)
            norm, curve = acc
            for lane in range(0, p.own, LANES):
                cut = pl.ds(lane, LANES)
                scale = diag[b, z, cut]
                square = 0.0
                for c in range(2):
                    r = rhs[c, b, z, cut]
                    made = scale * r + image[c, b, z, cut] + back[c, b, z, cut]
                    new = r - alpha[b] * made
                    res[c, b, z, cut] = new
                    square = square + new * new
                norm = norm + square
                curve = curve + square * scale
            return norm, curve

        zero = jnp.zeros((8, LANES), f32)
        stats.append(lax.fori_loop(0, p.grid // 8, one, (zero, zero)))
    return stats


def answers(p, keep, alpha, rhs, res, out):
    for b in range(p.bands):

        def answer(t, carry, b=b):
            z = aligned(t, 8)
            for lane_at in range(0, p.own, LANES):
                cut = pl.ds(lane_at, LANES)
                for c in range(2):
                    out[c, b, z, cut] = keep[b] * rhs[c, b, z, cut] + alpha[b] * res[c, b, z, cut]
            return carry

        lax.fori_loop(0, p.grid // 8, answer, 0)


def settle(*arrays):
    def kernel(*refs):
        for source, target in zip(refs[: len(arrays)], refs[len(arrays) :]):
            target[...] = source[...]

    return pl.pallas_call(
        kernel,
        out_shape=[spec_of(x.shape) for x in arrays],
        in_specs=[VMEM] * len(arrays),
        out_specs=[VMEM] * len(arrays),
        name="settle",
    )(*arrays)


def everywhere(x):
    x = jnp.sum(x, axis=0, keepdims=True)
    return jnp.broadcast_to(jnp.sum(x, axis=1, keepdims=True), x.shape)


def pay_stats(p, stats, pay):
    for b in range(p.bands):
        at = 2 * p.bands + b
        pay[at : at + 1, :] = everywhere(stats[b][0])
        at = 3 * p.bands + b
        pay[at : at + 1, :] = everywhere(stats[b][1])


def program(p, groups, psi, dv, vloc, beta_array, xy, shift, dij, atom_type):
    payload = -(-4 * p.bands // 8) * 8
    few = -(-p.bands // 8) * 8
    many = groups * p.bands
    inters = p.bands * many * 2
    wide_y = p.grid // groups
    dense = p.planes % 4 == 0 and LANES - p.grid == p.grid // 3
    thick = p.planes * 3 // 4 if dense else p.planes
    rest = LANES - p.grid
    coded = dense and wide_y % 8 == 0
    dense_rows = -(-thick * wide_y // 16) * 16
    chunk = (p.shards, p.rows, p.own)
    mine = (2, p.bands, p.grid, p.own)
    cells = p.images * p.grid
    many_rows = p.groups * p.rows
    n_chunks = p.matrix // JB

    def kernel(
        psi_h, dv_h, vloc_h, beta_hbm, xy_h, shift_r, dij_r, type_r,
        z_inv_h, z_fwd_h, y_inv_h, x_inv_h, x_fwd_h, y_fwd_h,
        resp_o, dens_r,
        rows_s, pot_dv, pot_v, pair, oh_t, mask, left, sq, mixed, spectrum, field_p, field_0, field_1,
        chunk_a, chunk_b, held_a, held_b, held_c, held_d, held_e,
        gath, joined, image, rhs, res, diag, stat,
        part, pay_i, sums_i, pay_a, sums_a, pay_b, sums_b, pay_c, sums_c, pay_d, sums_d,
        staged, beta, beta_f, stacked, acc, acc_f, coefs, coefs_f,
        dens_f, dens_q, dens_send, dens_got, scale_send, scale_got, dens_sum,
        beta_sem, sends, recvs, band_sends, band_recvs, out_sem,
        psi_r, dv_r, vloc_r, xy_r, z_inv, z_fwd, y_inv, x_inv, x_fwd, y_fwd, in_sem,
    ):
        me = lax.axis_index("ga")
        mine_band = lax.axis_index("band")

        def over(source, held, which, scatter):
            return pusher("ga", p.shards, source, held, sends, recvs, which, scatter)

        greet("ga", p.shards)
        greet("band", groups)
        loads = [
            pltpu.make_async_copy(source, target, in_sem.at[i])
            for i, (source, target) in enumerate(
                (
                    (psi_h, psi_r), (z_inv_h, z_inv), (xy_h, xy_r), (dv_h, dv_r),
                    (y_inv_h, y_inv), (x_inv_h, x_inv), (x_fwd_h, x_fwd), (y_fwd_h, y_fwd),
                    (z_fwd_h, z_fwd), (vloc_h, vloc_r),
                )
            )
        ]
        for load in loads:
            load.start()
        for at in range(SLOTS):
            fetch(p, beta_hbm, staged, beta_sem, at).start()
        loads[0].wait()
        loads[1].wait()
        to_lines(
            p, lambda b: jnp.concatenate([psi_r[0, b], psi_r[1, b]], axis=0), z_inv, chunk_a, True
        )
        pl.semaphore_wait(pltpu.get_barrier_semaphore(), p.shards + groups - 2)
        push_a = over(chunk_a, held_a, 0, True)
        start_all(push_a, p.shards)
        push_psi = pusher("band", groups, psi_r, gath, band_sends, band_recvs, 0, False)
        start_all(push_psi, groups)
        held_a[me] = chunk_a[me]
        gath[mine_band] = psi_r[...]
        for load in loads[2:]:
            load.wait()
        tables(p, xy_r, shift_r, rows_s, oh_t, mask, diag)
        widen(p, dv_r, pot_dv)

        early, middle = n_chunks * 7 // 8, n_chunks
        convert(p, beta_hbm, staged, beta_sem, beta, 0, early)
        rest_copy = pltpu.make_async_copy(
            beta_hbm.at[:, pl.ds(p.matrix, p.vector)], beta_f, out_sem.at[1]
        )
        rest_copy.start()
        wait_all(push_a, p.shards)

        lines_to_rows(p, held_a, oh_t, mask, left, sq)
        rows_to_mixed(p, sq, y_inv, mixed)
        mixed_to_field(p, mixed, x_inv, x_fwd, pot_dv, field_p, spectrum, None)
        push_b = over(chunk_b, held_b, 1, True)
        spectrum_to_lines(p, spectrum, y_fwd, oh_t, rows_s, sq, left, chunk_b, held_b, push_b)
        convert(p, beta_hbm, staged, beta_sem, beta, early, middle)
        widen(p, vloc_r, pot_v)
        build_pair(p, dij_r, type_r, pair)
        wait_all(push_psi, groups)
        wait_all(push_b, p.shards)

        from_lines(p, held_b, joined, z_fwd, image)
        intersect(p, groups, gath, image, part, pay_i)
        push_i = over(pay_i, sums_i, 2, False)
        start_all(push_i, p.shards)
        sums_i[me] = pay_i[...]
        convert(p, beta_hbm, staged, beta_sem, beta, middle, n_chunks)
        rest_copy.wait()
        wait_all(push_i, p.shards)
        spread_rows(total_of(sums_i, p.shards), part)
        stats = right_side(p, groups, gath, image, part, diag, rhs)
        to_lines(
            p, lambda b: jnp.concatenate([rhs[0, b], rhs[1, b]], axis=0), z_inv, chunk_a, False
        )
        stack_vector(p, rhs, stacked)
        push_c = over(chunk_a, held_c, 3, True)
        start_all(push_c, p.shards)
        held_c[me] = chunk_a[me]
        pay_stats(p, stats, pay_a)
        project(p, beta, beta_f, rhs, stacked, acc, acc_f, pay_a)
        push_pa = over(pay_a, sums_a, 4, False)
        start_all(push_pa, p.shards)
        sums_a[me] = pay_a[...]
        wait_all(push_c, p.shards)

        lines_to_rows(p, held_c, oh_t, mask, left, sq)
        rows_to_mixed(p, sq, y_inv, mixed)
        mixed_to_field(p, mixed, x_inv, x_fwd, pot_v, field_0, spectrum, stat)
        for b in range(p.bands):
            pay_b[b : b + 1, :] = everywhere(stat[b])
        push_pb = over(pay_b, sums_b, 5, False)
        start_all(push_pb, p.shards)
        sums_b[me] = pay_b[...]
        push_d = over(chunk_b, held_d, 6, True)
        spectrum_to_lines(p, spectrum, y_fwd, oh_t, rows_s, sq, left, chunk_b, held_d, push_d)
        wait_all(push_pa, p.shards)
        total = total_of(sums_a, p.shards)
        made, energy = couple(p, total, pair)
        build_coefs(p, made, coefs, coefs_f)
        back_project(p, beta, beta_f, coefs, coefs_f, res)
        wait_all(push_pb, p.shards)
        planes = total_of(sums_b, p.shards)
        norm0, alpha0 = [], []
        for b in range(p.bands):
            norm0.append(total[2 * p.bands + b : 2 * p.bands + b + 1])
            curve = total[3 * p.bands + b : 3 * p.bands + b + 1] + planes[b : b + 1] + energy[b]
            alpha0.append(norm0[b] / curve)
        wait_all(push_d, p.shards)
        from_lines(p, held_d, joined, z_fwd, image)
        stats = fresh(p, rhs, image, res, diag, alpha0, res)
        to_lines(
            p, lambda b: jnp.concatenate([res[0, b], res[1, b]], axis=0), z_inv, chunk_a, False
        )
        stack_vector(p, res, stacked)
        push_e = over(chunk_a, held_e, 7, True)
        start_all(push_e, p.shards)
        held_e[me] = chunk_a[me]
        pay_stats(p, stats, pay_c)
        project(p, beta, beta_f, res, stacked, acc, acc_f, pay_c)
        push_pc = over(pay_c, sums_c, 8, False)
        start_all(push_pc, p.shards)
        sums_c[me] = pay_c[...]
        wait_all(push_e, p.shards)

        lines_to_rows(p, held_e, oh_t, mask, left, sq)
        rows_to_mixed(p, sq, y_inv, mixed)
        mixed_to_field(p, mixed, x_inv, None, pot_v, field_1, None, stat)
        for b in range(p.bands):
            pay_d[b : b + 1, :] = everywhere(stat[b])
        push_pd = over(pay_d, sums_d, 9, False)
        start_all(push_pd, p.shards)
        sums_d[me] = pay_d[...]

        def products(at, carry):
            to = aligned(at, p.grid)
            one = field_p[to, :]
            first, second = one * field_0[to, :], one * field_1[to, :]
            spectrum[to, :LANES] = first[:, :LANES] + first[:, LANES:]
            spectrum[to, LANES:] = second[:, :LANES] + second[:, LANES:]
            return carry

        lax.fori_loop(0, p.images, products, 0)
        wait_all(push_pc, p.shards)
        total = total_of(sums_c, p.shards)
        made, energy = couple(p, total, pair)
        wait_all(push_pd, p.shards)
        planes = total_of(sums_d, p.shards)
        keep, alpha1 = [], []
        for b in range(p.bands):
            norm1 = total[2 * p.bands + b : 2 * p.bands + b + 1]
            curve = total[3 * p.bands + b : 3 * p.bands + b + 1] + planes[b : b + 1] + energy[b]
            ratio = norm1 / norm0[b]
            alpha = norm1 / (curve - ratio * norm1 / alpha0[b])
            alpha1.append(alpha)
            keep.append(alpha0[b] + alpha * ratio)

        def plane(zp):
            made = 0.0
            for b in range(p.bands):
                at = aligned(b * p.planes + zp, p.grid)
                made = made + (keep[b] * spectrum[at, :LANES] + alpha1[b] * spectrum[at, LANES:])
            return 4.0 * made

        lane = lax.broadcasted_iota(jnp.int32, (1, LANES), 1)
        if dense:

            def four(i, carry):
                last = plane(4 * i + 3)
                for k in range(3):
                    moved = pltpu.roll(last, p.grid - k * rest, 1)
                    dens_f[3 * i + k] = jnp.where(lane < p.grid, plane(4 * i + k), moved)
                return carry

            lax.fori_loop(0, p.planes // 4, four, 0)
        else:

            def single(i, carry):
                dens_f[i] = plane(i)
                return carry

            lax.fori_loop(0, p.planes, single, 0)

        if coded:
            for g in range(groups):
                for at in range(thick):
                    value = dens_f[at, g * wide_y : (g + 1) * wide_y, :]
                    top = jnp.max(jnp.abs(value), axis=0, keepdims=True)
                    up = jnp.where(top > 1e-30, TOP / top, 0.0)
                    dens_q[at * wide_y : (at + 1) * wide_y, :] = jnp.round(value * up)
                    scale_send[g, at : at + 1, :] = top * (1.0 / TOP)
                dens_send[g] = dens_q[...].astype(jnp.int16)
        else:
            for g in range(groups):
                for at in range(thick):
                    to = pl.ds(at * wide_y, wide_y)
                    dens_send[g, to, :] = dens_f[at, g * wide_y : (g + 1) * wide_y, :]

        push_z = pusher("band", groups, dens_send, dens_got, band_sends, band_recvs, 1, True)
        start_all(push_z, groups)
        answers(p, keep, alpha1, rhs, res, image)
        resp_copy = pltpu.make_async_copy(image, resp_o, out_sem.at[0])
        if coded:
            push_s = pusher("band", groups, scale_send, scale_got, band_sends, band_recvs, 2, True)
            start_all(push_s, groups)
        resp_copy.start()
        if coded:
            wait_all(push_s, groups)
        wait_all(push_z, groups)
        if coded:
            base = pl.ds(pl.multiple_of(mine_band * wide_y, 8), wide_y)
            total = [dens_f[at, base, :] for at in range(thick)]
            for hop in range(1, groups):
                src = lax.rem(mine_band + hop, groups)
                dens_q[...] = dens_got[src].astype(f32)
                for at in range(thick):
                    total[at] = total[at] + (
                        dens_q[at * wide_y : (at + 1) * wide_y, :] * scale_got[src, at : at + 1, :]
                    )
        else:
            dens_got[mine_band] = dens_send[mine_band]
            total = []
            for at in range(thick):
                to = pl.ds(at * wide_y, wide_y)
                value = dens_got[0, to, :]
                for g in range(1, groups):
                    value = value + dens_got[g, to, :]
                total.append(value)
        if dense:
            for i in range(p.planes // 4):
                last = jnp.zeros((wide_y, LANES), f32)
                for k in range(3):
                    value = total[3 * i + k]
                    dens_sum[pl.ds((4 * i + k) * wide_y, wide_y), :] = value
                    moved = pltpu.roll(value, LANES - p.grid + k * rest, 1)
                    inside = (lane >= k * rest) & (lane < (k + 1) * rest)
                    last = jnp.where(inside, moved, last)
                dens_sum[pl.ds((4 * i + 3) * wide_y, wide_y), :] = last
        else:
            for at in range(p.planes):
                dens_sum[pl.ds(at * wide_y, wide_y), :] = total[at]
        narrow(p, wide_y, dens_sum, dens_r)
        resp_copy.wait()

    small = (p.shards, payload, LANES)
    tiny = (p.shards, few, LANES)
    scratch = [
        pltpu.VMEM((8, p.sticks), jnp.int32),
        pltpu.VMEM((p.planes * p.pot_step, LANES), f32),
        pltpu.VMEM((p.planes * p.pot_step, LANES), f32),
        pltpu.VMEM((p.count, p.count), f32),
        pltpu.VMEM((p.wide, p.sticks), bf16),
        pltpu.VMEM((p.groups, 16, p.sticks), bf16),
        pltpu.VMEM((2, many_rows, p.sticks), bf16),
        pltpu.VMEM(
            (p.tiles, max(p.groups * p.row_step, p.rows * p.group_step), LANES), f32
        ),
        pltpu.VMEM((2, cells, 2 * LANES), bf16),
        pltpu.VMEM((cells, 2 * LANES), f32),
        pltpu.VMEM((cells, 2 * LANES), f32),
        pltpu.VMEM((cells, 2 * LANES), f32),
        pltpu.VMEM((cells, 2 * LANES), f32),
        pltpu.VMEM(chunk, f32),
        pltpu.VMEM(chunk, f32),
        pltpu.VMEM(chunk, f32),
        pltpu.VMEM(chunk, f32),
        pltpu.VMEM(chunk, f32),
        pltpu.VMEM(chunk, f32),
        pltpu.VMEM(chunk, f32),
        pltpu.VMEM((groups,) + mine, bf16),
        pltpu.VMEM((p.shards * p.q, p.own), f32),
        pltpu.VMEM(mine, f32),
        pltpu.VMEM(mine, f32),
        pltpu.VMEM(mine, f32),
        pltpu.VMEM((p.bands, p.grid, p.own), f32),
        pltpu.VMEM((p.bands, 8, LANES), f32),
        pltpu.VMEM((inters, LANES), f32),
        pltpu.VMEM((8, inters), f32),
        pltpu.VMEM((p.shards, 8, inters), f32),
        pltpu.VMEM((payload, LANES), f32),
        pltpu.VMEM(small, f32),
        pltpu.VMEM((few, LANES), f32),
        pltpu.VMEM(tiny, f32),
        pltpu.VMEM((payload, LANES), f32),
        pltpu.VMEM(small, f32),
        pltpu.VMEM((few, LANES), f32),
        pltpu.VMEM(tiny, f32),
        pltpu.VMEM((SLOTS, 2, JB, p.grid, p.own), f32),
        pltpu.VMEM((2, 2, p.matrix, p.grid, p.own), bf16),
        pltpu.VMEM((2, p.vector, p.grid, p.own), f32),
        pltpu.VMEM((p.grid // TALL, 4 * p.bands * TALL, p.own), bf16),
        pltpu.VMEM((2, p.matrix, 8, 4 * p.bands * TALL), f32),
        pltpu.VMEM((2 * p.bands, p.vector, 8, LANES), f32),
        pltpu.VMEM((2, 2 * p.bands * TALL, 2 * p.matrix * TALL), bf16),
        pltpu.VMEM((2 * p.bands, p.vector, LANES), f32),
        pltpu.VMEM((thick, p.grid, LANES), f32),
        pltpu.VMEM((dense_rows, LANES), f32),
        pltpu.VMEM((groups, dense_rows, LANES), jnp.int16 if coded else f32),
        pltpu.VMEM((groups, dense_rows, LANES), jnp.int16 if coded else f32),
        pltpu.VMEM((groups, -(-thick // 8) * 8, LANES), f32),
        pltpu.VMEM((groups, -(-thick // 8) * 8, LANES), f32),
        pltpu.VMEM((p.planes * wide_y, LANES), f32),
        pltpu.SemaphoreType.DMA((SLOTS,)),
        pltpu.SemaphoreType.DMA((10, p.shards - 1)),
        pltpu.SemaphoreType.DMA((10, p.shards - 1)),
        pltpu.SemaphoreType.DMA((3, groups - 1)),
        pltpu.SemaphoreType.DMA((3, groups - 1)),
        pltpu.SemaphoreType.DMA((2,)),
        pltpu.VMEM(mine, bf16),
        pltpu.VMEM(dv.shape, f32),
        pltpu.VMEM(vloc.shape, f32),
        pltpu.VMEM(xy.shape, jnp.int32),
    ]
    scratch += [
        pltpu.VMEM(table.shape, bf16)
        for table in (p.z_inv, p.z_fwd, p.y_inv, p.x_inv, p.x_fwd, p.y_fwd)
    ]
    scratch.append(pltpu.SemaphoreType.DMA((10,)))

    hbm = pl.BlockSpec(memory_space=pl.ANY)
    smem = pl.BlockSpec(memory_space=pltpu.SMEM)
    return pl.pallas_call(
        kernel,
        out_shape=[
            spec_of(mine), spec_of((p.planes, wide_y * p.grid)),
        ],
        in_specs=[hbm] * 5 + [smem] * 3 + [hbm] * 6,
        out_specs=[hbm, VMEM],
        scratch_shapes=scratch,
        compiler_params=pltpu.CompilerParams(
            collective_id=0, has_side_effects=True, vmem_limit_bytes=67_043_328
        ),
        name="response",
    )(
        psi, dv, vloc, beta_array, xy, shift, dij, atom_type,
        p.z_inv, p.z_fwd, p.y_inv, p.x_inv, p.x_fwd, p.y_fwd,
    )


def per_device(groups, shards, psi, vloc, dv, beta, dij, atom_type, stick_xy, band_shift):
    _, bands, grid, own = psi.shape
    planes = vloc.shape[0]
    sticks = stick_xy.shape[0]
    count = beta.shape[1]
    p = Plan(bands, grid, own, planes, shards, sticks, count)
    xy = stick_xy.reshape(sticks // LANES, LANES)
    return settle(*program(p, groups, psi, dv, vloc, beta, xy, band_shift, dij, atom_type))


def solution(mesh):
    placed = (
        P(None, "band", None, "ga"),
        P("ga", None),
        P("ga", None),
        P(None, None, None, "ga"),
        P(),
        P(),
        P(),
        P("band"),
    )
    groups, shards = mesh.shape["band"], mesh.shape["ga"]

    def body(*args):
        return per_device(groups, shards, *args)

    return jax.shard_map(
        body,
        mesh=mesh,
        in_specs=placed,
        out_specs=(P(None, "band", None, "ga"), P("ga", "band")),
        check_vma=False,
    )
```
